32 devices in a mesh: gx: 2 (over y), gy: 4 (over x, core), gz: 4 (over z).
Axes of the slice: x: 2, y: 2, z: 4, core: 2. Of those that a mesh axis runs over, the one named last changes fastest.
Arguments:
- right_side: float32 [16, 256, 512], P('gx', 'gy', 'gz'), may hold values from -4 to 4
- start: float32 [16, 256, 512], P('gx', 'gy', 'gz'), may hold values from -6 to 6
Outputs:
- solution: float32 [16, 256, 512], P('gx', 'gy', 'gz')
The draws below stay inside these ranges and needn't reach their ends.
All inputs are finite; a program needn't handle non-finite values.
Results may differ from the reference program's by a relative error of at most 0.0003.
Values sent between devices are 32-bit elements; how exact they have to be, the bound alone decides.
A program may use at most 128 MiB of HBM per device.

```python
import jax
import jax.numpy as jnp
from jax import lax

LEVELS = 4
SWEEPS = 2
CSWEEPS = 8
NX = 16
NY = 256
NZ = 512


def draw_right_side(key, part):
    values = jnp.clip(jax.random.normal(key, (NX, NY, NZ), jnp.float32), -4.0, 4.0)
    return values


def steps_of(key, shape, pieces, low, top_value):
    def one(axis_at, shards_of):
        draws = jax.random.uniform(jax.random.fold_in(jax.random.fold_in(key, 6), axis_at), (shards_of,), jnp.float32, low / len(pieces), top_value / len(pieces))
        return jnp.repeat(jnp.exp(draws), shape[axis_at] // shards_of).reshape((-1,) + (1,) * (len(shape) - axis_at - 1))

    factor_of = one(*pieces[0])
    for cut in pieces[1:]:
        factor_of = factor_of * one(*cut)
    return factor_of


def scatter_about(own_key, shape, deviation, reach, pieces=(), held_as=jnp.bfloat16):
    factor_of = steps_of(own_key, shape, pieces, -0.22, 0.18) if pieces else 1.0
    entries = jax.random.normal(own_key, shape, jnp.float32) * deviation * factor_of
    return jnp.minimum(jnp.maximum(entries, -reach), reach).astype(held_as)


def setup_inputs(seed: int = 0) -> dict:
    streams_of = jax.random.split(jax.random.key(seed), 3)
    right_side = draw_right_side(jax.random.fold_in(streams_of[2], 71), 0)
    start = scatter_about(streams_of[1], (NX, NY, NZ), 1.0, 6.0, ((0, 2), (1, 4), (2, 4)), jnp.float32)
    return {"right_side": right_side, "start": start}


def neighbours(padded):
    total = padded[2:, 1:-1, 1:-1] + padded[:-2, 1:-1, 1:-1]
    total = total + padded[1:-1, 2:, 1:-1] + padded[1:-1, :-2, 1:-1]
    return total + padded[1:-1, 1:-1, 2:] + padded[1:-1, 1:-1, :-2]


def parity(dims):
    first = lax.broadcasted_iota(jnp.int32, dims, 0)
    second = lax.broadcasted_iota(jnp.int32, dims, 1)
    third = lax.broadcasted_iota(jnp.int32, dims, 2)
    return (first + second + third) % 2


def smooth(correction, source, factor, colours, count):
    for pass_index in range(count):
        for colour in (0, 1):
            beside_all = neighbours(jnp.pad(correction, 1))
            correction = jnp.where(colours == colour, (factor * source + beside_all) / 6.0, correction)
    return correction


def restrict(residual):
    sx, sy, sz = residual.shape
    return residual.reshape(sx // 2, 2, sy // 2, 2, sz // 2, 2).mean(axis=(1, 3, 5))


def prolong(coarse):
    return jnp.repeat(jnp.repeat(jnp.repeat(coarse, 2, axis=0), 2, axis=1), 2, axis=2)


def reference(right_side, start):
    stored = []
    correction = start
    source = right_side
    for depth in range(LEVELS - 1):
        factor = 4.0 ** depth
        if depth > 0:
            correction = jnp.zeros_like(source)
        colours = parity(source.shape)
        correction = smooth(correction, source, factor, colours, SWEEPS)
        residual = source - (6.0 * correction - neighbours(jnp.pad(correction, 1))) / factor
        stored.append((correction, source, colours))
        source = restrict(residual)
    correction = smooth(jnp.zeros_like(source), source, 4.0 ** (LEVELS - 1), parity(source.shape), CSWEEPS)
    for depth in reversed(range(LEVELS - 1)):
        fine_value, fine_source, colours = stored[depth]
        correction = smooth(fine_value + prolong(correction), fine_source, 4.0 ** depth, colours, SWEEPS)
    return correction
```

```python
import functools

import jax
import jax.numpy as jnp
from jax import lax
from jax.experimental import pallas as pl
from jax.experimental.pallas import tpu as pltpu
from jax.sharding import PartitionSpec as P

MESH = pl.DeviceIdType.MESH
SIXTH = 1.0 / 6.0
PAD = 8
TOP = 16
LANES = 128
HALO = 3
CSWEEPS = 8
REACH2 = 42
EDGE = ((0, 1, 4), (0, 2, 2), (1, 1, 3), (1, 2, 1), (2, 1, 2))
FACE = 5
RHS1 = 5
COR1 = 6
COR0 = 4


def dot(a, b):
    return jnp.dot(a, b, precision=lax.Precision.HIGHEST, preferred_element_type=jnp.float32)


def iota(shape, axis):
    return lax.broadcasted_iota(jnp.int32, shape, axis)


def turn(v, shift):
    shift %= v.shape[1]
    return pltpu.roll(v, shift, axis=1) if shift else v


def evens(rows, lanes, add=0):
    shape = (rows // 8, 8, lanes)
    return ((iota(shape, 1) + iota(shape, 2) + add) & 1).reshape(rows, lanes) == 0


def both(*terms):
    out = True
    for term in terms:
        if term is True:
            continue
        out = term if out is True else out & term
    return out


def when(condition, action):
    if condition is True:
        action()
    else:
        pl.when(condition)(action)


class Side:
    def __init__(self, hop, up, send, recv, peer):
        self.hop, self.up, self.send, self.recv, self.peer = hop, up, send, recv, peer
        self.dynamic = not isinstance(up, bool)

    def pick(self, a, b):
        if self.dynamic:
            return jnp.where(self.up, a, b)
        return a if self.up else b

    def source(self, c, n, count):
        return self.pick(c + n - count, c)

    def target(self, c, n, count):
        return self.pick(c - count, c + n)

    def landing(self, c, n, k):
        if self.dynamic:
            return jnp.where(self.up, c + n + k - 1, c - k)
        return c - k if self.up else c + n + k - 1

    def outward(self, c, n, k):
        return self.pick(c + n - k, c + k - 1)

    def base(self, c, n):
        if self.dynamic:
            return jnp.where(self.up, c + n, c - n)
        return c - self.hop * n if self.up else c + self.hop * n

    def send_shift(self):
        return self.pick(0, 1)

    def recv_shift(self):
        return jnp.where(self.up, 1, 0) if self.dynamic else (0 if self.up else 1)


class Mail:
    def __init__(self, sems):
        self.sems, self.count, self.items = sems, 0, []

    def add(self, src, dst, send, recv, peer):
        at = self.count
        self.count += 1
        copy = pltpu.make_async_remote_copy(
            src_ref=src,
            dst_ref=dst,
            send_sem=self.sems.at[0, at],
            recv_sem=self.sems.at[1, at],
            device_id=peer,
            device_id_type=MESH,
        )
        self.items.append((copy, send, recv))
        when(send, copy.start)

    def wait(self):
        for copy, send, recv in self.items:
            when(send, copy.wait_send)
            when(recv, copy.wait_recv)


def kernel(
    sizes, rhs_hbm, start_hbm, out_ref,
    rhs, start, a0, r0, f0, s0, merged_out, merged_in, zsend, zrecv, esend, erecv,
    a1, r1, b1, f1, s1, w0, w1, tiles_out, tiles_in, ysides, xysides, zout, zin,
    n_out, n_in, ny_in, nxy_in, nz_out, nz_in, g_out, g_in,
    b2r, b2b, r2, v2, pack, slots, w2, b3r, b3b, r3, v3,
    in_sems, relay, sems, gather_sems,
):
    gx, gy, gz = sizes
    count = gx * gy * gz
    mx, my, mz = lax.axis_index("gx"), lax.axis_index("gy"), lax.axis_index("gz")
    lx, ly, lz = start.shape
    n0, n1 = lx // 2, lx // 4
    hy, hz = ly // 2, lz // 2
    qy, qz = hy // 2, hz // 2
    left = (LANES - hz) // 2
    c = HALO
    y2, z2 = gy * qy, gz * qz
    p2, p3 = gx * lx // 8, gx * lx // 16
    y3, z3 = y2 // 2, z2 // 2
    z3p = r3.shape[2]
    groups0, groups1 = ly // 8, hy // 8

    copies = [
        pltpu.make_async_copy(start_hbm, start, in_sems.at[0]),
        pltpu.make_async_copy(rhs_hbm, rhs, in_sems.at[1]),
    ]
    for copy in copies:
        copy.start()

    if gx == 1:
        near, sides1 = [], []
    elif gx == 2:
        near = sides1 = [Side(1, mx == 0, True, True, 1 - mx)]
    else:
        def side(hop, up):
            if up:
                return Side(hop, True, mx + hop < gx, mx >= hop, mx + hop)
            return Side(hop, False, mx >= hop, mx + hop < gx, mx - hop)

        near = [side(1, True), side(1, False)]
        sides1 = near + [side(2, True), side(2, False)]

    def along(at, size, step):
        if step == 0:
            return True, True, at
        if step > 0:
            return at + 1 < size, at >= 1, at + 1
        return at >= 1, at + 1 < size, at - 1

    def to(side, dy, dz):
        sx, rx, px = (True, True, mx) if side is None else (side.send, side.recv, side.peer)
        sy, ry, py = along(my, gy, dy)
        sz, rz, pz = along(mz, gz, dz)
        return both(sx, sy, sz), both(rx, ry, rz), (px, py, pz)

    faces = [to(s, 0, 0) for s in near]
    faces += [to(None, d, 0) for d in (1, -1)] + [to(None, 0, d) for d in (1, -1)]

    def signal_faces(sem):
        for send, _, peer in faces:
            when(send, lambda peer=peer: pl.semaphore_signal(sem, inc=1, device_id=peer, device_id_type=MESH))

    heard = sum([(1 if recv is True else jnp.where(recv, 1, 0)) for _, recv, _ in faces])

    for ref in (zrecv, erecv, merged_in):
        ref[...] = jnp.zeros_like(ref)
    rows0 = a0.shape[3]
    for q in range(3):
        for i in range(a0.shape[1]):
            if i < c or i >= c + n0:
                a0[q, i, 0] = jnp.zeros((rows0, LANES), jnp.float32)
            else:
                a0[q, i, 0, 0:TOP] = jnp.zeros((TOP, LANES), jnp.float32)
                a0[q, i, 0, TOP + ly:] = jnp.zeros((rows0 - TOP - ly, LANES), jnp.float32)
    barrier = pltpu.get_barrier_semaphore()
    signal_faces(barrier)

    for ref in (ysides, xysides, tiles_in, zin, n_in, ny_in, nxy_in, nz_in, g_in, slots):
        ref[...] = jnp.zeros_like(ref)
    for q in range(3):
        for i in range(a0.shape[1]):
            a0[q, i, 1] = jnp.zeros((rows0, LANES), jnp.float32)
    for ref in (r0, f0):
        ref[...] = jnp.zeros_like(ref)

    def mask(shape, row0, lane_of, bounds):
        y = iota(shape, 0) + row0
        z = lane_of(iota(shape, 1))
        inside = (y >= 0) & (y < bounds[0]) & (z >= 0) & (z < bounds[1])
        return jnp.where(inside, SIXTH, 0.0)

    fine = (gy * ly, gz * lz)
    s0[0] = mask(s0.shape[1:], my * ly - PAD, lambda k: mz * lz + k, fine)
    s0[1] = mask(s0.shape[1:], my * ly - PAD, lambda k: mz * lz + jnp.where(k < 64, k + lz, k - LANES), fine)
    s1[0] = mask(s1.shape[1:], my * hy - PAD, lambda k: mz * hz + k - left, (gy * hy, gz * hz))

    own = slice(TOP, TOP + ly)
    even = evens(ly, LANES)
    for copy in copies:
        copy.wait()
    for i in range(n0):
        a0[0, c + i, 0, own] = jnp.where(even, start[2 * i + 1], start[2 * i])
        a0[1, c + i, 0, own] = jnp.where(even, rhs[2 * i], rhs[2 * i + 1])
        a0[2, c + i, 0, own] = jnp.where(even, rhs[2 * i + 1], rhs[2 * i])
    for s, side in enumerate(near):
        third = a0[0, side.outward(c, n0, 3), 0, own]
        second = a0[2, side.outward(c, n0, 2), 0, own]
        merged_out[s] = jnp.where(evens(ly, LANES, side.send_shift()), third, pltpu.roll(second, 1, axis=0))

    pl.semaphore_wait(barrier, heard)

    lane64 = iota((ly, LANES), 1)
    lane8 = iota((8, LANES), 1)
    ydirs = zdirs = (1, -1)
    mail = Mail(sems.at[0])
    for s, side in enumerate(near):
        where = to(side, 0, 0)
        src, dst = side.source(c, n0, 2), side.target(c, n0, 2)
        mail.add(a0.at[0:2, pl.ds(src, 2), 0, own], a0.at[0:2, pl.ds(dst, 2), 0, own], *where)
        src, dst = side.source(c, n0, 1), side.target(c, n0, 1)
        mail.add(a0.at[2, pl.ds(src, 1), 0, own], a0.at[2, pl.ds(dst, 1), 0, own], *where)
        mail.add(merged_out.at[s], merged_in.at[s], *where)

    def strip(d, rows):
        return (TOP + rows - 8, TOP - 8) if d > 0 else (TOP, TOP + rows)

    for d in ydirs:
        src, dst = strip(d, ly)
        mail.add(
            a0.at[0:3, pl.ds(c, n0), 0, pl.ds(src, 8)], a0.at[0:3, pl.ds(c, n0), 0, pl.ds(dst, 8)], *to(None, d, 0)
        )
    signal_faces(relay.at[0])

    slots0 = [(q, i) for i in range(n0) for q in range(3)]
    for zi, d in enumerate(zdirs):
        packed = jnp.zeros((ly, LANES), jnp.float32)
        for t, (q, i) in enumerate(slots0):
            v = a0[q, c + i, 0, own]
            first = lz - FACE if d > 0 else 0
            here = (lane64 >= FACE * t) & (lane64 < FACE * (t + 1))
            packed = jnp.where(here, turn(v, FACE * t - first), packed)
        zsend[zi] = packed
    for zi, d in enumerate(zdirs):
        mail.add(zsend.at[zi], zrecv.at[zi, pl.ds(8, ly)], *to(None, 0, d))

    width = sum(w for _, _, w in EDGE)
    starts = [sum(w for _, _, w in EDGE[:t]) for t in range(len(EDGE))]
    for s, side in enumerate(near):
        for zi, d in enumerate(zdirs):
            packed = jnp.zeros((8, LANES), jnp.float32)
            for (q, k, w), at in zip(EDGE, starts):
                v = a0[q, side.outward(c, n0, k), 0, own]
                for g in range(groups0):
                    lo = width * g + at
                    first = lz - w if d > 0 else 0
                    here = (lane8 >= lo) & (lane8 < lo + w)
                    packed = jnp.where(here, turn(v[8 * g:8 * g + 8], lo - first), packed)
            esend[s, zi] = packed
    pl.semaphore_wait(relay.at[0], heard)
    signal_faces(relay.at[1])
    for s, side in enumerate(near):
        p_src, p_dst = side.source(c, n0, 2), side.target(c, n0, 2)
        for d in ydirs:
            src, dst = strip(d, ly)
            mail.add(
                a0.at[0:3, pl.ds(p_src, 2), 0, pl.ds(src, 8)],
                a0.at[0:3, pl.ds(p_dst, 2), 0, pl.ds(dst, 8)],
                *to(side, d, 0),
            )
    for zi, dz in enumerate(zdirs):
        for d in ydirs:
            src, dst = strip(d, ly)
            mail.add(
                zsend.at[zi, pl.ds(src - TOP, 8)], zrecv.at[zi, pl.ds(dst - 8, 8)], *to(None, d, dz)
            )
        for s, side in enumerate(near):
            mail.add(esend.at[s, zi], erecv.at[s, zi, 1], *to(side, 0, dz))
    rounds = relay.shape[0]
    pl.semaphore_wait(relay.at[1], heard)
    for zi, dz in enumerate(zdirs):
        for s, side in enumerate(near):
            for d in ydirs:
                mail.add(esend.at[s, zi], erecv.at[s, zi, 0 if d > 0 else 2], *to(side, d, dz))
    for r in range(2, rounds):
        signal_faces(relay.at[r])
        pl.semaphore_wait(relay.at[r], heard)
    mail.wait()

    for s, side in enumerate(near):
        v = merged_in[s]
        a0[0, side.landing(c, n0, 3), 0, own] = v
        a0[2, side.landing(c, n0, 2), 0, own] = pltpu.roll(v, ly - 1, axis=0)
    rows_h = ly + 16
    lane_h = iota((rows_h, LANES), 1)
    for t, (q, i) in enumerate(slots0):
        low = turn(zrecv[0], LANES - FACE - FACE * t)
        high = turn(zrecv[1], -FACE * t)
        a0[q, c + i, 1, PAD:PAD + rows_h] = jnp.where(
            lane_h >= LANES - FACE, low, jnp.where(lane_h < FACE, high, 0.0)
        )
    for s, side in enumerate(near):
        for (q, k, w), at in zip(EDGE, starts):
            pair = side.landing(c, n0, k)
            for g in range(groups0 + 2):
                which, group = (0, groups0 - 1) if g == 0 else ((2, 0) if g > groups0 else (1, g - 1))
                lo = width * group + at
                low = turn(erecv[s, 0, which], LANES - w - lo)
                high = turn(erecv[s, 1, which], -lo)
                a0[q, pair, 1, PAD + 8 * g:PAD + 8 * g + 8] = jnp.where(
                    lane8 >= LANES - w, low, jnp.where(lane8 < w, high, 0.0)
                )

    def span(n, k):
        if gx == 1:
            return c, n
        k = min(k, n * (gx - 1), HALO)
        if gx == 2:
            return jnp.where(mx == 0, c, c - k), n + k
        return c - k, n + 2 * k

    def inside(n, i):
        if gx <= 2:
            return None
        at = mx * n + i - c
        return jnp.where((at >= 0) & (at < gx * n), 1.0, 0.0)

    def neighbours(src, i, planes, red, chess, lo, hi, tiles):
        prev, cur, nxt = planes
        low = [turn(t, 1) for t in cur]
        high = [turn(t, -1) for t in cur]
        if len(cur) == 2:
            lane = iota(cur[0].shape, 1)
            low = [jnp.where(lane == 0, low[1 - g], low[g]) for g in range(tiles)]
            high = [jnp.where(lane == LANES - 1, high[1 - g], high[g]) for g in range(tiles)]
        out = []
        for g in range(tiles):
            beside = jnp.where(chess, prev[g], nxt[g]) if red else jnp.where(chess, nxt[g], prev[g])
            total = (cur[g] + beside) + (src[i, g, lo - 1:hi - 1] + src[i, g, lo + 1:hi + 1])
            out.append(total + (low[g] + high[g]))
        return out

    def relax(dst, src, rhs_of, scale, n, k, red, factor, tiles=None, emit=None):
        first, length = span(n, k)
        held = src.shape[1]
        rows = src.shape[2]
        lo, hi = (TOP, rows - TOP) if emit else (PAD, rows - PAD)
        tiles = tiles or held
        chess = evens(hi - lo, LANES)
        planes = [[src[first + j - 1, g, lo:hi] for g in range(held)] for j in range(length + 2)]
        for j in range(length):
            i = first + j
            totals = neighbours(src, i, planes[j:j + 3], red, chess, lo, hi, tiles)
            factor_x = inside(n, i)
            for g in range(tiles):
                b = rhs_of(i, g, lo, hi)
                if factor != 1.0:
                    b = b * factor
                value = (b + totals[g]) * scale[g, lo - PAD:hi - PAD]
                if factor_x is not None:
                    value = value * factor_x
                if emit:
                    emit(j, planes[j + 1][g], value)
                else:
                    dst[i, g, lo:hi] = value

    def residual(red_ref, black_ref, red_rhs, black_rhs, n, j, factor):
        rows = red_ref.shape[2]
        lo, hi = TOP, rows - TOP
        chess = evens(hi - lo, LANES)
        i = c + j
        held = red_ref.shape[1]

        def load(ref):
            return [[ref[i + d, g, lo:hi] for g in range(held if d == 0 else 1)] for d in (-1, 0, 1)]

        red, black = load(red_ref), load(black_ref)
        from_black = neighbours(black_ref, i, black, True, chess, lo, hi, 1)[0]
        from_red = neighbours(red_ref, i, red, False, chess, lo, hi, 1)[0]
        out = red_rhs(i, 0, lo, hi) - (6.0 * red[1][0] - from_black) * (1.0 / factor)
        return out + (black_rhs(i, 0, lo, hi) - (6.0 * black[1][0] - from_red) * (1.0 / factor))

    black0 = a0.at[0]
    rhs0 = [lambda i, g, lo, hi, q=q: a0[q, i, g, lo:hi] for q in (1, 2)]
    for step in range(4):
        k = (4 - step + 1) // 2
        if step % 2 == 0:
            relax(r0, black0, rhs0[0], s0, n0, k, True, 1.0)
        else:
            relax(black0, r0, rhs0[1], s0, n0, k, False, 1.0)
    for j in range(n0):
        w0[j * ly:(j + 1) * ly, :] = residual(r0, black0, rhs0[0], rhs0[1], n0, j, 1.0)
    r = w0[pl.ds(0, n0 * hy, stride=2), :] + w0[pl.ds(1, n0 * hy, stride=2), :]
    source, target = iota((LANES, LANES), 0), iota((LANES, LANES), 1)
    fold = jnp.where(lax.rem(target - left + LANES, hz) == source // 2, 0.125, 0.0)
    r = dot(r, fold)

    own1 = slice(TOP, TOP + hy)
    lane32 = iota((hy, LANES), 1)
    mid = (lane32 >= left) & (lane32 < left + hz)
    chess1 = evens(hy, LANES)
    for j in range(n1):
        one, two = r[2 * j * hy:(2 * j + 1) * hy], r[(2 * j + 1) * hy:(2 * j + 2) * hy]
        red = jnp.where(chess1, one, two)
        black = jnp.where(chess1, two, one)
        tiles_out[j] = jnp.where(mid, red, black)
        a1[0, c + j, 0, own1] = jnp.where(mid, red, 0.0)
        a1[1, c + j, 0, own1] = jnp.where(mid, black, 0.0)

    def pack_edges(read, items, w):
        for d in zdirs:
            first = left + hz - w if d > 0 else left
            packed = jnp.zeros((8, LANES), jnp.float32)
            for t in range(items * groups1):
                here = (lane8 >= w * t) & (lane8 < w * (t + 1))
                packed = jnp.where(here, turn(read(t), w * t - first), packed)
            yield packed

    def post1(mail, out, into, y_in, xy_in, z_out, z_in):
        for s, side in enumerate(sides1):
            mail.add(out, into.at[s], *to(side, 0, 0))
        for yi, d in enumerate(ydirs):
            src = hy - 8 if d > 0 else 0
            mail.add(out.at[:, pl.ds(src, 8)], y_in.at[yi], *to(None, d, 0))
        for s, side in enumerate(sides1):
            for yi, d in enumerate(ydirs):
                src = hy - 8 if d > 0 else 0
                mail.add(out.at[:, pl.ds(src, 8)], xy_in.at[s, yi], *to(side, d, 0))
        for zi, dz in enumerate(zdirs):
            for s, side in enumerate([None] + sides1):
                for yi, d in enumerate((1, 0, -1)):
                    mail.add(z_out.at[zi], z_in.at[zi, s, yi], *to(side, d, dz))

    def regions1():
        yield from ((None, None, j, c + j) for j in range(n1))
        for s, side in enumerate(sides1):
            for j in range(n1):
                at = side.base(c, n1) + j
                if side.dynamic or 0 <= at < 2 * c + n1:
                    yield (s, side, j, at)

    def row_groups():
        yield 0, groups1 - 1, None, 0
        for g in range(groups1):
            yield 1, g, g, None
        yield 2, 0, None, 1

    lane_l = lane8
    mid8 = (lane_l >= left) & (lane_l < left + hz)

    def edges(z_in, s, which, lo, w):
        at = 0 if s is None else s + 1
        low = turn(z_in[0, at, which], left - w - lo)
        high = turn(z_in[1, at, which], left + hz - lo)
        return jnp.where(lane_l < left, low, high)

    items = 2 * n1
    order1 = [(g, q, j) for g in range(groups1) for j in range(n1) for q in range(2)]
    tile_of = lambda t: a1[order1[t][1], c + order1[t][2], 0, TOP + 8 * order1[t][0]:TOP + 8 * order1[t][0] + 8]
    for zi, packed in enumerate(pack_edges(tile_of, items, RHS1)):
        zout[zi] = packed
    mail = Mail(sems.at[1])
    post1(mail, tiles_out, tiles_in, ysides, xysides, zout, zin)
    for ref in (a1, r1, b1, f1):
        for i in range(ref.shape[-4]):
            halo_pair = i < c or i >= c + n1
            lead = (slice(None),) if len(ref.shape) == 5 else ()
            if halo_pair or ref is not a1:
                at = lead + (i,)
                ref[at] = jnp.zeros(ref[at].shape, jnp.float32)
            else:
                for rows in (slice(0, TOP), slice(TOP + hy, None)):
                    at = lead + (i, slice(None), rows)
                    ref[at] = jnp.zeros(ref[at].shape, jnp.float32)
    for ref in (b2r, b2b, r2, v2, b3r, b3b, r3, v3):
        ref[...] = jnp.zeros_like(ref)
    mail.wait()

    near_lanes = (lane_l >= left - RHS1) & (lane_l < left + hz + RHS1)
    for s, side, j, at in regions1():
        for n, (which, group, rows, yi) in enumerate(row_groups()):
            if rows is None:
                base = ysides[yi, j] if s is None else xysides[s, yi, j]
            elif s is None:
                base = None
            else:
                base = tiles_in[s, j, 8 * rows:8 * rows + 8]
            for q in range(2):
                to_rows = slice(PAD + 8 * n, PAD + 8 * n + 8)
                lo = RHS1 * ((group * n1 + j) * 2 + q)
                if base is None:
                    middle = a1[q, at, 0, to_rows]
                else:
                    middle = base if q == 0 else turn(base, LANES - hz)
                outer = edges(zin, s, which, lo, RHS1)
                a1[q, at, 0, to_rows] = jnp.where(mid8, middle, jnp.where(near_lanes, outer, 0.0))

    rhs1 = [lambda i, g, lo, hi, q=q: a1[q, i, g, lo:hi] for q in (0, 1)]
    first, length = span(n1, 2)
    for j in range(length):
        i = first + j
        value = (a1[0, i, 0, PAD:-PAD] * 4.0) * s1[0]
        factor_x = inside(n1, i)
        r1[i, 0, PAD:-PAD] = value if factor_x is None else value * factor_x
    relax(b1, r1, rhs1[1], s1, n1, 2, False, 4.0)
    relax(r1, b1, rhs1[0], s1, n1, 1, True, 4.0)
    relax(b1, r1, rhs1[1], s1, n1, 1, False, 4.0)

    for j in range(n1):
        w1[j, 0:hy, :] = residual(r1, b1, rhs1[0], rhs1[1], n1, j, 4.0)
    r = jnp.concatenate(
        [w1[j, pl.ds(0, qy, stride=2), :] + w1[j, pl.ds(1, qy, stride=2), :] for j in range(n1)], axis=0
    )
    fold = jnp.where(
        (lax.rem(target, qz) == (source - left) // 2) & (source >= left) & (source < left + hz), 0.125, 0.0
    )
    r = dot(r, fold)
    block = lane8 // qz
    per_colour = qy // 8
    one = two = None
    for h in range(per_colour):
        p, q = r[8 * h:8 * h + 8], r[qy + 8 * h:qy + 8 * h + 8]
        here = lax.rem(block, per_colour) == h
        one = p if one is None else jnp.where(here, p, one)
        two = q if two is None else jnp.where(here, q, two)
    tile = jnp.where(evens(8, LANES) ^ (block >= per_colour), one, two)
    pack[...] = tile

    mine = (mx * gy + my) * gz + mz
    slots[mine] = tile

    dist = (-(-REACH2 // (lx // 4)), -(-REACH2 // qy), -(-REACH2 // qz))

    def coords(k):
        steps = (k // (gy * gz), k // gz % gy, k % gz)
        moved = [at + step for at, step in zip((mx, my, mz), steps)]
        at = tuple(jnp.where(v >= size, v - size, v) for v, size in zip(moved, sizes))
        close = True
        for a, b, size, reach in zip(at, (mx, my, mz), sizes, dist):
            if reach < size - 1:
                close = both(close, (a - b <= reach) & (b - a <= reach))
        return at, close

    def number(at):
        return (at[0] * gy + at[1]) * gz + at[2]

    def others(body):
        if count <= 64:
            for k in range(1, count):
                body(k)
        else:
            def step(k, carry):
                body(k)
                return carry

            lax.fori_loop(1, count, step, 0)

    def gather(k, arriving):
        at, close = coords(k)
        d = number(at)
        return pltpu.make_async_remote_copy(
            src_ref=pack,
            dst_ref=slots.at[d if arriving else mine],
            send_sem=gather_sems.at[0, d],
            recv_sem=gather_sems.at[1, d if arriving else mine],
            device_id=at,
            device_id_type=MESH,
        ), close

    def gather_start(k):
        copy, close = gather(k, False)
        when(close, copy.start)

    def gather_wait(k):
        copy, close = gather(k, True)

        def done():
            copy.wait_send()
            copy.wait_recv()

        when(close, done)

    others(gather_start)

    red_out = jnp.where(mid, b1[c, 0, own1], turn(b1[c + n1 - 1, 0, own1], LANES - hz))
    n_out[0] = red_out
    order_n = [(g, j) for g in range(groups1) for j in range(n1)]
    tile_n = lambda t: b1[c + order_n[t][1], 0, TOP + 8 * order_n[t][0]:TOP + 8 * order_n[t][0] + 8]
    for zi, packed in enumerate(pack_edges(tile_n, n1, COR1)):
        nz_out[zi] = packed
    mail1 = Mail(sems.at[2])
    post1(mail1, n_out, n_in, ny_in, nxy_in, nz_out, nz_in)

    for zi, d in enumerate(zdirs):
        packed = jnp.zeros((8, LANES), jnp.float32)
        for i in range(n0):
            v = a0[0, c + i, 0, own]
            for g in range(groups0):
                lo = COR0 * (g * n0 + i)
                first = lz - COR0 if d > 0 else 0
                here = (lane8 >= lo) & (lane8 < lo + COR0)
                packed = jnp.where(here, turn(v[8 * g:8 * g + 8], lo - first), packed)
        g_out[zi] = packed
    mail0 = Mail(sems.at[3])
    for side in near:
        src, dst = side.source(c, n0, 2), side.target(c, n0, 2)
        mail0.add(black0.at[pl.ds(src, 2), 0, own], f0.at[pl.ds(dst, 2), 0, own], *to(side, 0, 0))
        for d in ydirs:
            ysrc, ydst = strip(d, ly)
            mail0.add(
                black0.at[pl.ds(src, 2), 0, pl.ds(ysrc, 8)], f0.at[pl.ds(dst, 2), 0, pl.ds(ydst, 8)], *to(side, d, 0)
            )
    for d in ydirs:
        ysrc, ydst = strip(d, ly)
        mail0.add(
            black0.at[pl.ds(c, n0), 0, pl.ds(ysrc, 8)], f0.at[pl.ds(c, n0), 0, pl.ds(ydst, 8)], *to(None, d, 0)
        )
    for zi, dz in enumerate(zdirs):
        for s, side in enumerate([None] + near):
            for yi, d in enumerate((1, 0, -1)):
                mail0.add(g_out.at[zi], g_in.at[zi, s, yi], *to(side, d, dz))

    others(gather_wait)

    per = LANES // qz
    for k in range(gx * gy):
        cx, cy = k // gy, k % gy
        for g in range(gz // per):
            parts = [slots[k * gz + g * per + q] for q in range(per)]
            for h in range(per_colour):
                for colour, ref in ((0, b2r), (1, b2b)):
                    at = colour * per_colour + h
                    v = None
                    for q in range(per):
                        moved = turn(parts[q], (q - at) * qz)
                        here = (lane8 >= q * qz) & (lane8 < (q + 1) * qz)
                        v = moved if v is None else jnp.where(here, moved, v)
                    ref[1 + cx, PAD + cy * qy + 8 * h:PAD + cy * qy + 8 * h + 8, LANES * g:LANES * (g + 1)] = v

    def coarse_total(src, i, red, rows, full):
        width_z = src.shape[2]
        lo, hi = PAD, PAD + rows
        v = src[i, lo:hi]
        low, high = turn(v, 1), turn(v, -1)
        lane = iota(v.shape, 1)
        if full:
            low = jnp.where(lane == 0, 0.0, low)
            high = jnp.where(lane == width_z - 1, 0.0, high)
        chess = evens(rows, width_z)
        prev, nxt = src[i - 1, lo:hi], src[i + 1, lo:hi]
        beside = jnp.where(chess, prev, nxt) if red else jnp.where(chess, nxt, prev)
        total = (v + beside) + (src[i, lo - 1:hi - 1] + src[i, lo + 1:hi + 1])
        return v, total + (low + high)

    def coarse(dst, src, b, pairs, red, factor, rows, scale, full):
        for i in range(1, pairs + 1):
            _, total = coarse_total(src, i, red, rows, full)
            dst[i, PAD:PAD + rows] = (b[i, PAD:PAD + rows] * factor + total) * scale

    in2 = slice(PAD, PAD + y2)
    for i in range(1, p2 + 1):
        r2[i, in2] = (b2r[i, in2] * 16.0) * SIXTH
    coarse(v2, r2, b2b, p2, False, 16.0, y2, SIXTH, True)
    coarse(r2, v2, b2r, p2, True, 16.0, y2, SIXTH, True)
    coarse(v2, r2, b2b, p2, False, 16.0, y2, SIXTH, True)

    fold = jnp.where(iota((z2, z3p), 1) == iota((z2, z3p), 0) // 2, 0.125, 0.0)
    parts = []
    for i in range(1, p2 + 1):
        red, from_black = r2[i, in2], coarse_total(v2, i, True, y2, True)[1]
        black, from_red = v2[i, in2], coarse_total(r2, i, False, y2, True)[1]
        r = b2r[i, in2] - (6.0 * red - from_black) * 0.0625
        r = r + (b2b[i, in2] - (6.0 * black - from_red) * 0.0625)
        for g in range(z2 // LANES):
            w2[i - 1, g, 0:y2] = r[:, LANES * g:LANES * (g + 1)]
        parts.append(
            jnp.concatenate(
                [
                    w2[i - 1, g, pl.ds(0, y3, stride=2), :] + w2[i - 1, g, pl.ds(1, y3, stride=2), :]
                    for g in range(z2 // LANES)
                ],
                axis=1,
            )
        )
    r = dot(jnp.concatenate(parts, axis=0), fold)
    chess3 = evens(y3, z3p)
    in3 = slice(PAD, PAD + y3)
    for j in range(p3):
        one, two = r[2 * j * y3:(2 * j + 1) * y3], r[(2 * j + 1) * y3:(2 * j + 2) * y3]
        b3r[1 + j, in3] = jnp.where(chess3, one, two)
        b3b[1 + j, in3] = jnp.where(chess3, two, one)

    full3 = z3 == z3p
    scale3 = SIXTH if full3 else jnp.where(iota((y3, z3p), 1) < z3, SIXTH, 0.0)

    def sweep3(_, carry):
        coarse(r3, v3, b3r, p3, True, 64.0, y3, scale3, full3)
        coarse(v3, r3, b3b, p3, False, 64.0, y3, scale3, full3)
        return carry

    if p3 == 1:
        for _ in range(CSWEEPS):
            sweep3(0, 0)
    else:
        lax.fori_loop(0, CSWEEPS, sweep3, 0)

    def plane(red, black, chess, odd):
        return jnp.where(chess, black, red) if odd else jnp.where(chess, red, black)

    grow = jnp.where(iota((z3p, z2), 0) == iota((z3p, z2), 1) // 2, 1.0, 0.0)
    v = jnp.concatenate(
        [plane(r3[1 + i // 2, in3], v3[1 + i // 2, in3], chess3, i % 2) for i in range(p2)], axis=0
    )
    v = dot(v, grow)
    for i in range(p2):
        part = v[i * y3:(i + 1) * y3]
        for g in range(z2 // LANES):
            w2[i, g, pl.ds(0, y3, stride=2), :] = part[:, LANES * g:LANES * (g + 1)]
            w2[i, g, pl.ds(1, y3, stride=2), :] = part[:, LANES * g:LANES * (g + 1)]
    for i in range(p2):
        for g in range(z2 // LANES):
            lanes = slice(LANES * g, LANES * (g + 1))
            v2[1 + i, in2, lanes] = v2[1 + i, in2, lanes] + w2[i, g, 0:y2]
    for _ in range(2):
        coarse(r2, v2, b2r, p2, True, 16.0, y2, SIXTH, True)
        coarse(v2, r2, b2b, p2, False, 16.0, y2, SIXTH, True)

    mail1.wait()
    grow1 = jnp.where(
        iota((z2, LANES), 0) == mz * qz + (iota((z2, LANES), 1) - left + 2 * LANES) // 2 - LANES, 1.0, 0.0
    )
    rows1 = f1.shape[2]
    half1 = rows1 // 2
    rows2 = pl.ds(pl.multiple_of(my * qy, 8), half1)
    chess2 = evens(half1, z2)
    first, length = span(n1, HALO)
    begin = first - c + mx * n1
    shift = 0 if gx <= 2 else 1
    first_even = begin - shift
    tops = []
    for j in range(length):
        at = j + shift
        index = (first_even + (at - at % 2)) // 2 + 1
        if gx > 2:
            index = jnp.clip(index, 0, p2 + 1)
        tops.append(plane(r2[index, rows2], v2[index, rows2], chess2, at % 2))
    v = dot(jnp.concatenate(tops, axis=0), grow1)
    for j in range(length):
        part = v[j * half1:(j + 1) * half1]
        w1[j, pl.ds(0, half1, stride=2), :] = part
        w1[j, pl.ds(1, half1, stride=2), :] = part

    near_lanes = (lane_l >= left - COR1) & (lane_l < left + hz + COR1)
    for s, side, j, at in regions1():
        for n, (which, group, rows, yi) in enumerate(row_groups()):
            to_rows = slice(PAD + 8 * n, PAD + 8 * n + 8)
            if rows is None:
                base = ny_in[yi, 0] if s is None else nxy_in[s, yi, 0]
            elif s is None:
                base = None
            else:
                base = n_in[s, 0, 8 * rows:8 * rows + 8]
            if base is None:
                middle = b1[at, 0, to_rows]
            else:
                middle = base if j == 0 else turn(base, LANES - hz)
            outer = edges(nz_in, s, which, COR1 * (group * n1 + j), COR1)
            value = jnp.where(mid8, middle, jnp.where(near_lanes, outer, 0.0))
            f1[at, 0, to_rows] = value + w1[at - first, to_rows, :]

    for step in range(4):
        k = (5 - step + 1) // 2
        if step % 2 == 0:
            relax(r1, f1, rhs1[0], s1, n1, k, True, 4.0)
        else:
            relax(f1, r1, rhs1[1], s1, n1, k, False, 4.0)

    mail0.wait()
    grow0 = jnp.where(
        iota((LANES, 2 * LANES), 0) == (left + iota((LANES, 2 * LANES), 1) // 2) % LANES, 1.0, 0.0
    )
    half0 = rows0 // 2
    first, length = span(n0, 2)
    chess_h = evens(half0, LANES)
    tops = []
    for j in range(length):
        index = (first - c + j - j % 2) // 2 + c if gx <= 2 else (first - c + j) // 2 + c
        red, black = r1[index, 0, PAD:PAD + half0], f1[index, 0, PAD:PAD + half0]
        tops.append(plane(red, black, chess_h, j % 2))
    v = dot(jnp.concatenate(tops, axis=0), grow0)
    for j in range(length):
        for g in range(2):
            base = (2 * j + g) * rows0
            part = v[j * half0:(j + 1) * half0, LANES * g:LANES * (g + 1)]
            w0[pl.ds(base, half0, stride=2), :] = part
            w0[pl.ds(base + 1, half0, stride=2), :] = part

    for i in range(n0):
        at = c + i
        j = at - first
        lift = w0[pl.ds(pl.multiple_of(2 * j * rows0, 8) + TOP, ly), :]
        f0[at, 0, own] = black0[at, 0, own] + lift
        for rows in (slice(PAD, TOP), slice(TOP + ly, TOP + ly + 8)):
            lift = w0[pl.ds(pl.multiple_of(2 * j * rows0, 8) + rows.start, 8), :]
            f0[at, 0, rows] = f0[at, 0, rows] + lift
    for side in near:
        for k in (1, 2):
            at = side.landing(c, n0, k)
            j = at - first
            lift = w0[pl.ds(pl.multiple_of(2 * j * rows0, 8) + PAD, rows_h), :]
            f0[at, 0, PAD:PAD + rows_h] = f0[at, 0, PAD:PAD + rows_h] + lift
    for s, side in enumerate([None] + near):
        pairs = range(n0) if side is None else (1, 2)
        for k in pairs:
            if side is None:
                at, far = c + k, k
            else:
                at = side.landing(c, n0, k)
                far = None
            for n in range(groups0 + 2):
                which, group = (0, groups0 - 1) if n == 0 else ((2, 0) if n > groups0 else (1, n - 1))
                tiles = []
                for zi in range(2):
                    t = g_in[zi, s, which]
                    if far is not None:
                        lo = COR0 * (group * n0 + far)
                        tiles.append(turn(t, (LANES - COR0 if zi == 0 else 0) - lo))
                    elif side.dynamic:
                        spot = (LANES - COR0 if zi == 0 else 0)
                        a = turn(t, spot - COR0 * (group * n0 + k - 1))
                        b = turn(t, spot - COR0 * (group * n0 + n0 - k))
                        tiles.append(jnp.where(side.up, a, b))
                    else:
                        far_at = n0 - k if side.up else k - 1
                        tiles.append(turn(t, (LANES - COR0 if zi == 0 else 0) - COR0 * (group * n0 + far_at)))
                low, high = tiles
                value = jnp.where(lane8 >= LANES - COR0, low, jnp.where(lane8 < COR0, high, 0.0))
                j = at - first
                to_rows = slice(PAD + 8 * n, PAD + 8 * n + 8)
                lift = w0[pl.ds(pl.multiple_of((2 * j + 1) * rows0, 8) + PAD + 8 * n, 8), :]
                f0[at, 1, to_rows] = value + lift

    relax(r0, f0, rhs0[0], s0, n0, 2, True, 1.0)
    relax(f0, r0, rhs0[1], s0, n0, 1, False, 1.0)
    relax(r0, f0, rhs0[0], s0, n0, 1, True, 1.0)

    def emit(j, red, black):
        out_ref[2 * j] = jnp.where(even, red, black)
        out_ref[2 * j + 1] = jnp.where(even, black, red)

    relax(None, r0, rhs0[1], s0, n0, 0, False, 1.0, tiles=1, emit=emit)


def local(sizes, right_side, start):
    gx, gy, gz = sizes
    lx, ly, lz = start.shape
    f32 = jnp.float32
    count = gx * gy * gz
    near = {1: 0, 2: 1}.get(gx, 2)
    far = {1: 0, 2: 1}.get(gx, 4)
    n0, n1 = lx // 2, lx // 4
    m0, m1 = n0 + 2 * HALO, n1 + 2 * HALO
    r0, r1 = ly + 2 * TOP, ly // 2 + 2 * TOP
    hy = ly // 2
    y2, z2 = gy * ly // 4, gz * lz // 4
    p2, p3 = gx * lx // 8, gx * lx // 16
    y3, z3 = y2 // 2, z2 // 2
    z3p = -(-z3 // LANES) * LANES
    dx = min(gx - 1, -(-REACH2 // (lx // 4)))
    dy = min(gy - 1, -(-REACH2 // (ly // 4)))
    dz = min(gz - 1, -(-REACH2 // (lz // 4)))
    rounds = max(2, sum(max(0, d - 2) for d in (dx, dy, dz)) - 1)
    near_a, far_a = max(near, 1), max(far, 1)

    def vmem(*shape):
        return pltpu.VMEM(shape, f32)

    messages = 24 if gx <= 2 else 48
    return pl.pallas_call(
        functools.partial(kernel, sizes),
        out_shape=jax.ShapeDtypeStruct(start.shape, f32),
        in_specs=[pl.BlockSpec(memory_space=pl.ANY)] * 2,
        out_specs=pl.BlockSpec(memory_space=pltpu.VMEM),
        scratch_shapes=[
            vmem(lx, ly, lz),
            vmem(lx, ly, lz),
            vmem(3, m0, 2, r0, LANES),
            vmem(m0, 2, r0, LANES),
            vmem(m0, 2, r0, LANES),
            vmem(2, r0 - 2 * PAD, LANES),
            vmem(near_a, ly, LANES),
            vmem(near_a, ly, LANES),
            vmem(2, ly, LANES),
            vmem(2, ly + 16, LANES),
            vmem(near_a, 2, 8, LANES),
            vmem(near_a, 2, 3, 8, LANES),
            vmem(2, m1, 1, r1, LANES),
            vmem(m1, 1, r1, LANES),
            vmem(m1, 1, r1, LANES),
            vmem(m1, 1, r1, LANES),
            vmem(1, r1 - 2 * PAD, LANES),
            vmem(2 * m0 * r0, LANES),
            vmem(m1, r1, LANES),
            vmem(n1, hy, LANES),
            vmem(far_a, n1, hy, LANES),
            vmem(2, n1, 8, LANES),
            vmem(far_a, 2, n1, 8, LANES),
            vmem(2, 8, LANES),
            vmem(2, far + 1, 3, 8, LANES),
            vmem(1, hy, LANES),
            vmem(far_a, 1, hy, LANES),
            vmem(2, 1, 8, LANES),
            vmem(far_a, 2, 1, 8, LANES),
            vmem(2, 8, LANES),
            vmem(2, far + 1, 3, 8, LANES),
            vmem(2, 8, LANES),
            vmem(2, near + 1, 3, 8, LANES),
            vmem(p2 + 2, y2 + 2 * PAD, z2),
            vmem(p2 + 2, y2 + 2 * PAD, z2),
            vmem(p2 + 2, y2 + 2 * PAD, z2),
            vmem(p2 + 2, y2 + 2 * PAD, z2),
            vmem(8, LANES),
            vmem(count, 8, LANES),
            vmem(p2, z2 // LANES, y2, LANES),
            vmem(p3 + 2, y3 + 2 * PAD, z3p),
            vmem(p3 + 2, y3 + 2 * PAD, z3p),
            vmem(p3 + 2, y3 + 2 * PAD, z3p),
            vmem(p3 + 2, y3 + 2 * PAD, z3p),
            pltpu.SemaphoreType.DMA((2,)),
            pltpu.SemaphoreType.REGULAR((rounds,)),
            pltpu.SemaphoreType.DMA((4, 2, messages)),
            pltpu.SemaphoreType.DMA((2, count)),
        ],
        compiler_params=pltpu.CompilerParams(
            collective_id=0, has_side_effects=True, vmem_limit_bytes=48 * 1024 * 1024
        ),
    )(right_side, start)


def solution(mesh):
    sizes = (mesh.shape["gx"], mesh.shape["gy"], mesh.shape["gz"])
    spec = P("gx", "gy", "gz")
    return jax.shard_map(
        functools.partial(local, sizes), mesh=mesh, in_specs=(spec, spec), out_specs=spec, check_vma=False
    )
```

```python
import functools

import jax
import jax.numpy as jnp
from jax import lax
from jax.experimental import pallas as pl
from jax.experimental.pallas import tpu as pltpu
from jax.sharding import PartitionSpec as P

MESH = pl.DeviceIdType.MESH
SIXTH = 1.0 / 6.0
PAD = 8
TOP = 16
LANES = 128
HALO = 3
CSWEEPS = 8
REACH2 = 42
EDGE = ((0, 1, 4), (0, 2, 2), (1, 1, 3), (1, 2, 1), (2, 1, 2))
FACE = 5
RHS1 = 5
COR1 = 6
COR0 = 4
GRANT = 56150000


def dot(a, b):
    return jnp.dot(a, b, precision=lax.Precision.HIGHEST, preferred_element_type=jnp.float32)


def iota(shape, axis):
    return lax.broadcasted_iota(jnp.int32, shape, axis)


def turn(v, shift):
    shift %= v.shape[1]
    return pltpu.roll(v, shift, axis=1) if shift else v


def evens(rows, lanes, add=0):
    shape = (rows // 8, 8, lanes)
    return ((iota(shape, 1) + iota(shape, 2) + add) & 1).reshape(rows, lanes) == 0


def both(*terms):
    out = True
    for term in terms:
        if term is True:
            continue
        out = term if out is True else out & term
    return out


def when(condition, action):
    if condition is True:
        action()
    else:
        pl.when(condition)(action)


class Side:
    def __init__(self, hop, up, send, recv, peer):
        self.hop, self.up, self.send, self.recv, self.peer = hop, up, send, recv, peer
        self.dynamic = not isinstance(up, bool)

    def pick(self, a, b):
        if self.dynamic:
            return jnp.where(self.up, a, b)
        return a if self.up else b

    def source(self, c, n, count):
        return self.pick(c + n - count, c)

    def target(self, c, n, count):
        return self.pick(c - count, c + n)

    def landing(self, c, n, k):
        if self.dynamic:
            return jnp.where(self.up, c + n + k - 1, c - k)
        return c - k if self.up else c + n + k - 1

    def outward(self, c, n, k):
        return self.pick(c + n - k, c + k - 1)

    def base(self, c, n):
        if self.dynamic:
            return jnp.where(self.up, c + n, c - n)
        return c - self.hop * n if self.up else c + self.hop * n

    def send_shift(self):
        return self.pick(0, 1)

    def recv_shift(self):
        return jnp.where(self.up, 1, 0) if self.dynamic else (0 if self.up else 1)


class Mail:
    def __init__(self, sems):
        self.sems, self.count, self.items = sems, 0, []

    def add(self, src, dst, send, recv, peer, tag=None):
        at = self.count
        self.count += 1
        copy = pltpu.make_async_remote_copy(
            src_ref=src,
            dst_ref=dst,
            send_sem=self.sems.at[0, at],
            recv_sem=self.sems.at[1, at],
            device_id=peer,
            device_id_type=MESH,
        )
        self.items.append((tag, copy, send, recv))
        when(send, copy.start)

    def wait(self, tag=None):
        for item in list(self.items):
            name, copy, send, recv = item
            if tag is None or name == tag:
                when(send, copy.wait_send)
                when(recv, copy.wait_recv)
                self.items.remove(item)


def kernel(
    sizes, rhs_hbm, start_hbm, out_ref,
    rhs, start, a0, r0, f0, s0, merged_out, merged_in, zsend, zrecv, esend, erecv, yedge_out, yedge_in,
    a1, r1, b1, f1, s1, w0, w1, tiles_out, tiles_in, ysides, xysides, zout, zin,
    n_out, n_in, ny_in, nxy_in, nz_out, nz_in, g_out, g_in,
    b2r, b2b, r2, v2, pack, slots, w2, b3r, b3b, r3, v3,
    in_sems, relay, sems, gather_sems,
):
    gx, gy, gz = sizes
    count = gx * gy * gz
    mx, my, mz = lax.axis_index("gx"), lax.axis_index("gy"), lax.axis_index("gz")
    lx, ly, lz = start.shape
    n0, n1 = lx // 2, lx // 4
    hy, hz = ly // 2, lz // 2
    qy, qz = hy // 2, hz // 2
    left = (LANES - hz) // 2
    c = HALO
    y2, z2 = gy * qy, gz * qz
    p2, p3 = gx * lx // 8, gx * lx // 16
    y3, z3 = y2 // 2, z2 // 2
    z3p = r3.shape[2]
    groups0, groups1 = ly // 8, hy // 8

    copies = [
        pltpu.make_async_copy(start_hbm, start, in_sems.at[0]),
        pltpu.make_async_copy(rhs_hbm, rhs, in_sems.at[1]),
    ]
    for copy in copies:
        copy.start()

    if gx == 1:
        near, sides1 = [], []
    elif gx == 2:
        near = sides1 = [Side(1, mx == 0, True, True, 1 - mx)]
    else:
        def side(hop, up):
            if up:
                return Side(hop, True, mx + hop < gx, mx >= hop, mx + hop)
            return Side(hop, False, mx >= hop, mx + hop < gx, mx - hop)

        near = [side(1, True), side(1, False)]
        sides1 = near + [side(2, True), side(2, False)]

    def along(at, size, step):
        if step == 0:
            return True, True, at
        if step > 0:
            return at + 1 < size, at >= 1, at + 1
        return at >= 1, at + 1 < size, at - 1

    def to(side, dy, dz):
        sx, rx, px = (True, True, mx) if side is None else (side.send, side.recv, side.peer)
        sy, ry, py = along(my, gy, dy)
        sz, rz, pz = along(mz, gz, dz)
        return both(sx, sy, sz), both(rx, ry, rz), (px, py, pz)

    faces = [to(s, 0, 0) for s in near]
    faces += [to(None, d, 0) for d in (1, -1)] + [to(None, 0, d) for d in (1, -1)]

    def signal_faces(sem):
        for send, _, peer in faces:
            when(send, lambda peer=peer: pl.semaphore_signal(sem, inc=1, device_id=peer, device_id_type=MESH))

    heard = sum([(1 if recv is True else jnp.where(recv, 1, 0)) for _, recv, _ in faces])

    for ref in (zrecv, erecv, merged_in, yedge_in):
        ref[...] = jnp.zeros_like(ref)
    rows0 = a0.shape[3]
    for q in range(3):
        for i in range(a0.shape[1]):
            if i < c or i >= c + n0:
                a0[q, i, 0] = jnp.zeros((rows0, LANES), jnp.float32)
            else:
                a0[q, i, 0, 0:TOP] = jnp.zeros((TOP, LANES), jnp.float32)
                a0[q, i, 0, TOP + ly:] = jnp.zeros((rows0 - TOP - ly, LANES), jnp.float32)
    barrier = pltpu.get_barrier_semaphore()
    signal_faces(barrier)

    for ref in (ysides, xysides, tiles_in, zin, n_in, ny_in, nxy_in, nz_in, g_in, slots):
        ref[...] = jnp.zeros_like(ref)
    for q in range(3):
        for i in range(a0.shape[1]):
            a0[q, i, 1] = jnp.zeros((rows0, LANES), jnp.float32)
    for ref in (r0, f0):
        ref[...] = jnp.zeros_like(ref)

    def mask(shape, row0, lane_of, bounds):
        y = iota(shape, 0) + row0
        z = lane_of(iota(shape, 1))
        inside = (y >= 0) & (y < bounds[0]) & (z >= 0) & (z < bounds[1])
        return jnp.where(inside, SIXTH, 0.0)

    fine = (gy * ly, gz * lz)
    s0[0] = mask(s0.shape[1:], my * ly - PAD, lambda k: mz * lz + k, fine)
    s0[1] = mask(s0.shape[1:], my * ly - PAD, lambda k: mz * lz + jnp.where(k < 64, k + lz, k - LANES), fine)
    s1[0] = mask(s1.shape[1:], my * hy - PAD, lambda k: mz * hz + k - left, (gy * hy, gz * hz))

    own = slice(TOP, TOP + ly)
    even = evens(ly, LANES)
    for copy in copies:
        copy.wait()
    for i in range(n0):
        a0[0, c + i, 0, own] = jnp.where(even, start[2 * i + 1], start[2 * i])
        a0[1, c + i, 0, own] = jnp.where(even, rhs[2 * i], rhs[2 * i + 1])
        a0[2, c + i, 0, own] = jnp.where(even, rhs[2 * i + 1], rhs[2 * i])
    for s, side in enumerate(near):
        third = a0[0, side.outward(c, n0, 3), 0, own]
        second = a0[2, side.outward(c, n0, 2), 0, own]
        merged_out[s] = jnp.where(evens(ly, LANES, side.send_shift()), third, pltpu.roll(second, 1, axis=0))

    pl.semaphore_wait(barrier, heard)

    lane64 = iota((ly, LANES), 1)
    lane8 = iota((8, LANES), 1)
    ydirs = zdirs = (1, -1)
    mail = Mail(sems.at[0])
    for s, side in enumerate(near):
        where = to(side, 0, 0)
        src, dst = side.source(c, n0, 2), side.target(c, n0, 2)
        mail.add(a0.at[0:2, pl.ds(src, 2), 0, own], a0.at[0:2, pl.ds(dst, 2), 0, own], *where)
        src, dst = side.source(c, n0, 1), side.target(c, n0, 1)
        mail.add(a0.at[2, pl.ds(src, 1), 0, own], a0.at[2, pl.ds(dst, 1), 0, own], *where)
        mail.add(merged_out.at[s], merged_in.at[s], *where)

    def strip(d, rows):
        return (TOP + rows - 8, TOP - 8) if d > 0 else (TOP, TOP + rows)

    for d in ydirs:
        src, dst = strip(d, ly)
        mail.add(
            a0.at[0:3, pl.ds(c, n0), 0, pl.ds(src, 8)], a0.at[0:3, pl.ds(c, n0), 0, pl.ds(dst, 8)], *to(None, d, 0)
        )
    signal_faces(relay.at[0])

    slots0 = [(q, i) for i in range(n0) for q in range(3)]
    for zi, d in enumerate(zdirs):
        packed = jnp.zeros((ly, LANES), jnp.float32)
        for t, (q, i) in enumerate(slots0):
            v = a0[q, c + i, 0, own]
            first = lz - FACE if d > 0 else 0
            here = (lane64 >= FACE * t) & (lane64 < FACE * (t + 1))
            packed = jnp.where(here, turn(v, FACE * t - first), packed)
        zsend[zi] = packed
    for zi, d in enumerate(zdirs):
        mail.add(zsend.at[zi], zrecv.at[zi, pl.ds(8, ly)], *to(None, 0, d), "z")

    width = sum(w for _, _, w in EDGE)
    starts = [sum(w for _, _, w in EDGE[:t]) for t in range(len(EDGE))]
    for s, side in enumerate(near):
        for zi, d in enumerate(zdirs):
            packed = jnp.zeros((8, LANES), jnp.float32)
            for (q, k, w), at in zip(EDGE, starts):
                v = a0[q, side.outward(c, n0, k), 0, own]
                for g in range(groups0):
                    lo = width * g + at
                    first = lz - w if d > 0 else 0
                    here = (lane8 >= lo) & (lane8 < lo + w)
                    packed = jnp.where(here, turn(v[8 * g:8 * g + 8], lo - first), packed)
            esend[s, zi] = packed
        for yi, d in enumerate(ydirs):
            for (q, k, w), at in zip(EDGE, starts):
                first = TOP + ly - w if d > 0 else TOP
                yedge_out[s, yi, at:at + w] = a0[q, side.outward(c, n0, k), 0, first:first + w]
    pl.semaphore_wait(relay.at[0], heard)
    signal_faces(relay.at[1])
    for s, side in enumerate(near):
        for yi, d in enumerate(ydirs):
            mail.add(yedge_out.at[s, yi], yedge_in.at[s, yi], *to(side, d, 0), "y")
    for zi, dz in enumerate(zdirs):
        for d in ydirs:
            src, dst = strip(d, ly)
            mail.add(
                zsend.at[zi, pl.ds(src - TOP, 8)], zrecv.at[zi, pl.ds(dst - 8, 8)], *to(None, d, dz), "z"
            )
        for s, side in enumerate(near):
            mail.add(esend.at[s, zi], erecv.at[s, zi, 1], *to(side, 0, dz), "e")
    rounds = relay.shape[0]
    pl.semaphore_wait(relay.at[1], heard)
    for zi, dz in enumerate(zdirs):
        for s, side in enumerate(near):
            for d in ydirs:
                mail.add(esend.at[s, zi], erecv.at[s, zi, 0 if d > 0 else 2], *to(side, d, dz), "e")
    for r in range(2, rounds):
        signal_faces(relay.at[r])
        pl.semaphore_wait(relay.at[r], heard)
    mail.wait("z")
    rows_h = ly + 16
    lane_h = iota((rows_h, LANES), 1)
    for t, (q, i) in enumerate(slots0):
        low = turn(zrecv[0], LANES - FACE - FACE * t)
        high = turn(zrecv[1], -FACE * t)
        a0[q, c + i, 1, PAD:PAD + rows_h] = jnp.where(
            lane_h >= LANES - FACE, low, jnp.where(lane_h < FACE, high, 0.0)
        )
    mail.wait("e")
    for s, side in enumerate(near):
        for (q, k, w), at in zip(EDGE, starts):
            pair = side.landing(c, n0, k)
            for g in range(groups0 + 2):
                which, group = (0, groups0 - 1) if g == 0 else ((2, 0) if g > groups0 else (1, g - 1))
                lo = width * group + at
                low = turn(erecv[s, 0, which], LANES - w - lo)
                high = turn(erecv[s, 1, which], -lo)
                a0[q, pair, 1, PAD + 8 * g:PAD + 8 * g + 8] = jnp.where(
                    lane8 >= LANES - w, low, jnp.where(lane8 < w, high, 0.0)
                )

    mail.wait("y")
    for s, side in enumerate(near):
        for yi, d in enumerate(ydirs):
            for (q, k, w), at in zip(EDGE, starts):
                first = TOP - w if d > 0 else TOP + ly
                a0[q, side.landing(c, n0, k), 0, first:first + w] = yedge_in[s, yi, at:at + w]
    mail.wait()
    for s, side in enumerate(near):
        v = merged_in[s]
        a0[0, side.landing(c, n0, 3), 0, own] = v
        a0[2, side.landing(c, n0, 2), 0, own] = pltpu.roll(v, ly - 1, axis=0)

    def span(n, k):
        if gx == 1:
            return c, n
        k = min(k, n * (gx - 1), HALO)
        if gx == 2:
            return jnp.where(mx == 0, c, c - k), n + k
        return c - k, n + 2 * k

    def inside(n, i):
        if gx <= 2:
            return None
        at = mx * n + i - c
        return jnp.where((at >= 0) & (at < gx * n), 1.0, 0.0)

    def neighbours(src, i, planes, red, chess, lo, hi, tiles):
        prev, cur, nxt = planes
        low = [turn(t, 1) for t in cur]
        high = [turn(t, -1) for t in cur]
        if len(cur) == 2:
            lane = iota(cur[0].shape, 1)
            low = [jnp.where(lane == 0, low[1 - g], low[g]) for g in range(tiles)]
            high = [jnp.where(lane == LANES - 1, high[1 - g], high[g]) for g in range(tiles)]
        out = []
        for g in range(tiles):
            beside = jnp.where(chess, prev[g], nxt[g]) if red else jnp.where(chess, nxt[g], prev[g])
            total = (cur[g] + beside) + (src[i, g, lo - 1:hi - 1] + src[i, g, lo + 1:hi + 1])
            out.append(total + (low[g] + high[g]))
        return out

    def relax(dst, src, rhs_of, scale, n, k, red, factor, tiles=None, emit=None):
        first, length = span(n, k)
        held = src.shape[1]
        rows = src.shape[2]
        lo, hi = (TOP, rows - TOP) if emit else (PAD, rows - PAD)
        tiles = tiles or held
        chess = evens(hi - lo, LANES)
        planes = [[src[first + j - 1, g, lo:hi] for g in range(held)] for j in range(length + 2)]
        for j in range(length):
            i = first + j
            totals = neighbours(src, i, planes[j:j + 3], red, chess, lo, hi, tiles)
            factor_x = inside(n, i)
            for g in range(tiles):
                b = rhs_of(i, g, lo, hi)
                if factor != 1.0:
                    b = b * factor
                value = (b + totals[g]) * scale[g, lo - PAD:hi - PAD]
                if factor_x is not None:
                    value = value * factor_x
                if emit:
                    emit(j, planes[j + 1][g], value)
                else:
                    dst[i, g, lo:hi] = value

    def residual(red_ref, black_ref, red_rhs, black_rhs, n, j, factor):
        rows = red_ref.shape[2]
        lo, hi = TOP, rows - TOP
        chess = evens(hi - lo, LANES)
        i = c + j
        held = red_ref.shape[1]

        def load(ref):
            return [[ref[i + d, g, lo:hi] for g in range(held if d == 0 else 1)] for d in (-1, 0, 1)]

        red, black = load(red_ref), load(black_ref)
        from_black = neighbours(black_ref, i, black, True, chess, lo, hi, 1)[0]
        from_red = neighbours(red_ref, i, red, False, chess, lo, hi, 1)[0]
        out = red_rhs(i, 0, lo, hi) - (6.0 * red[1][0] - from_black) * (1.0 / factor)
        return out + (black_rhs(i, 0, lo, hi) - (6.0 * black[1][0] - from_red) * (1.0 / factor))

    black0 = a0.at[0]
    rhs0 = [lambda i, g, lo, hi, q=q: a0[q, i, g, lo:hi] for q in (1, 2)]
    for step in range(4):
        k = (4 - step + 1) // 2
        if step % 2 == 0:
            relax(r0, black0, rhs0[0], s0, n0, k, True, 1.0)
        else:
            relax(black0, r0, rhs0[1], s0, n0, k, False, 1.0)
    for j in range(n0):
        w0[j * ly:(j + 1) * ly, :] = residual(r0, black0, rhs0[0], rhs0[1], n0, j, 1.0)
    r = w0[pl.ds(0, n0 * hy, stride=2), :] + w0[pl.ds(1, n0 * hy, stride=2), :]
    source, target = iota((LANES, LANES), 0), iota((LANES, LANES), 1)
    fold = jnp.where(lax.rem(target - left + LANES, hz) == source // 2, 0.125, 0.0)
    r = dot(r, fold)

    own1 = slice(TOP, TOP + hy)
    lane32 = iota((hy, LANES), 1)
    mid = (lane32 >= left) & (lane32 < left + hz)
    chess1 = evens(hy, LANES)
    for j in range(n1):
        one, two = r[2 * j * hy:(2 * j + 1) * hy], r[(2 * j + 1) * hy:(2 * j + 2) * hy]
        red = jnp.where(chess1, one, two)
        black = jnp.where(chess1, two, one)
        tiles_out[j] = jnp.where(mid, red, black)
        a1[0, c + j, 0, own1] = jnp.where(mid, red, 0.0)
        a1[1, c + j, 0, own1] = jnp.where(mid, black, 0.0)

    def pack_edges(read, items, w):
        for d in zdirs:
            first = left + hz - w if d > 0 else left
            packed = jnp.zeros((8, LANES), jnp.float32)
            for t in range(items * groups1):
                here = (lane8 >= w * t) & (lane8 < w * (t + 1))
                packed = jnp.where(here, turn(read(t), w * t - first), packed)
            yield packed

    def post1(mail, out, into, y_in, xy_in, z_out, z_in):
        for s, side in enumerate(sides1):
            mail.add(out, into.at[s], *to(side, 0, 0))
        for yi, d in enumerate(ydirs):
            src = hy - 8 if d > 0 else 0
            mail.add(out.at[:, pl.ds(src, 8)], y_in.at[yi], *to(None, d, 0))
        for s, side in enumerate(sides1):
            for yi, d in enumerate(ydirs):
                src = hy - 8 if d > 0 else 0
                mail.add(out.at[:, pl.ds(src, 8)], xy_in.at[s, yi], *to(side, d, 0))
        for zi, dz in enumerate(zdirs):
            for s, side in enumerate([None] + sides1):
                for yi, d in enumerate((1, 0, -1)):
                    mail.add(z_out.at[zi], z_in.at[zi, s, yi], *to(side, d, dz))

    def regions1():
        yield from ((None, None, j, c + j) for j in range(n1))
        for s, side in enumerate(sides1):
            for j in range(n1):
                at = side.base(c, n1) + j
                if side.dynamic or 0 <= at < 2 * c + n1:
                    yield (s, side, j, at)

    def row_groups():
        yield 0, groups1 - 1, None, 0
        for g in range(groups1):
            yield 1, g, g, None
        yield 2, 0, None, 1

    lane_l = lane8
    mid8 = (lane_l >= left) & (lane_l < left + hz)

    def edges(z_in, s, which, lo, w):
        at = 0 if s is None else s + 1
        low = turn(z_in[0, at, which], left - w - lo)
        high = turn(z_in[1, at, which], left + hz - lo)
        return jnp.where(lane_l < left, low, high)

    items = 2 * n1
    order1 = [(g, q, j) for g in range(groups1) for j in range(n1) for q in range(2)]
    tile_of = lambda t: a1[order1[t][1], c + order1[t][2], 0, TOP + 8 * order1[t][0]:TOP + 8 * order1[t][0] + 8]
    for zi, packed in enumerate(pack_edges(tile_of, items, RHS1)):
        zout[zi] = packed
    mail = Mail(sems.at[1])
    post1(mail, tiles_out, tiles_in, ysides, xysides, zout, zin)
    for ref in (a1, r1, b1, f1):
        for i in range(ref.shape[-4]):
            halo_pair = i < c or i >= c + n1
            lead = (slice(None),) if len(ref.shape) == 5 else ()
            if halo_pair or ref is not a1:
                at = lead + (i,)
                ref[at] = jnp.zeros(ref[at].shape, jnp.float32)
            else:
                for rows in (slice(0, TOP), slice(TOP + hy, None)):
                    at = lead + (i, slice(None), rows)
                    ref[at] = jnp.zeros(ref[at].shape, jnp.float32)
    for ref in (b2r, b2b, r2, v2, b3r, b3b, r3, v3):
        ref[...] = jnp.zeros_like(ref)
    mail.wait()

    near_lanes = (lane_l >= left - RHS1) & (lane_l < left + hz + RHS1)
    for s, side, j, at in regions1():
        for n, (which, group, rows, yi) in enumerate(row_groups()):
            if rows is None:
                base = ysides[yi, j] if s is None else xysides[s, yi, j]
            elif s is None:
                base = None
            else:
                base = tiles_in[s, j, 8 * rows:8 * rows + 8]
            for q in range(2):
                to_rows = slice(PAD + 8 * n, PAD + 8 * n + 8)
                lo = RHS1 * ((group * n1 + j) * 2 + q)
                if base is None:
                    middle = a1[q, at, 0, to_rows]
                else:
                    middle = base if q == 0 else turn(base, LANES - hz)
                outer = edges(zin, s, which, lo, RHS1)
                a1[q, at, 0, to_rows] = jnp.where(mid8, middle, jnp.where(near_lanes, outer, 0.0))

    rhs1 = [lambda i, g, lo, hi, q=q: a1[q, i, g, lo:hi] for q in (0, 1)]
    first, length = span(n1, 2)
    for j in range(length):
        i = first + j
        value = (a1[0, i, 0, PAD:-PAD] * 4.0) * s1[0]
        factor_x = inside(n1, i)
        r1[i, 0, PAD:-PAD] = value if factor_x is None else value * factor_x
    relax(b1, r1, rhs1[1], s1, n1, 2, False, 4.0)
    relax(r1, b1, rhs1[0], s1, n1, 1, True, 4.0)
    relax(b1, r1, rhs1[1], s1, n1, 1, False, 4.0)

    for j in range(n1):
        w1[j, 0:hy, :] = residual(r1, b1, rhs1[0], rhs1[1], n1, j, 4.0)
    r = jnp.concatenate(
        [w1[j, pl.ds(0, qy, stride=2), :] + w1[j, pl.ds(1, qy, stride=2), :] for j in range(n1)], axis=0
    )
    fold = jnp.where(
        (lax.rem(target, qz) == (source - left) // 2) & (source >= left) & (source < left + hz), 0.125, 0.0
    )
    r = dot(r, fold)
    block = lane8 // qz
    per_colour = qy // 8
    one = two = None
    for h in range(per_colour):
        p, q = r[8 * h:8 * h + 8], r[qy + 8 * h:qy + 8 * h + 8]
        here = lax.rem(block, per_colour) == h
        one = p if one is None else jnp.where(here, p, one)
        two = q if two is None else jnp.where(here, q, two)
    tile = jnp.where(evens(8, LANES) ^ (block >= per_colour), one, two)
    pack[...] = tile

    mine = (mx * gy + my) * gz + mz
    slots[mine] = tile

    dist = (-(-REACH2 // (lx // 4)), -(-REACH2 // qy), -(-REACH2 // qz))

    def coords(k):
        steps = (k // (gy * gz), k // gz % gy, k % gz)
        moved = [at + step for at, step in zip((mx, my, mz), steps)]
        at = tuple(jnp.where(v >= size, v - size, v) for v, size in zip(moved, sizes))
        close = True
        for a, b, size, reach in zip(at, (mx, my, mz), sizes, dist):
            if reach < size - 1:
                close = both(close, (a - b <= reach) & (b - a <= reach))
        return at, close

    def number(at):
        return (at[0] * gy + at[1]) * gz + at[2]

    def flipped(at, k):
        bit = 1
        while bit <= k:
            if k & bit:
                at = at + bit - 2 * bit * lax.rem(lax.div(at, bit), 2)
            bit *= 2
        return at

    def partners():
        own_at = (mx, my, mz)
        flips = [[flipped(at, k) for k in range(size)] for at, size in zip(own_at, sizes)]
        order = [(i, j, k) for i in range(gx) for j in range(gy) for k in range(gz)][1:]
        order.sort(key=lambda f: (-(f[0] + min(f[2], 2) + f[1] // 2), -f[1], f[2]))
        for f in order:
            at = tuple(flips[axis][k] for axis, k in enumerate(f))
            close = True
            for a, b, k, reach in zip(at, own_at, f, dist):
                if k > reach:
                    close = both(close, (a - b <= reach) & (b - a <= reach))
            yield at, close

    straight = count <= 64 and all(size & (size - 1) == 0 for size in sizes)

    def others(body):
        if straight:
            for place in partners():
                body(place)
        else:
            def step(k, carry):
                body(coords(k))
                return carry

            lax.fori_loop(1, count, step, 0)

    def gather(place, arriving):
        at, close = place
        d = number(at)
        return pltpu.make_async_remote_copy(
            src_ref=pack,
            dst_ref=slots.at[d if arriving else mine],
            send_sem=gather_sems.at[0, d],
            recv_sem=gather_sems.at[1, d if arriving else mine],
            device_id=at,
            device_id_type=MESH,
        ), close

    def gather_start(place):
        copy, close = gather(place, False)
        when(close, copy.start)

    def gather_wait(place):
        copy, close = gather(place, True)

        def done():
            copy.wait_send()
            copy.wait_recv()

        when(close, done)

    others(gather_start)

    red_out = jnp.where(mid, b1[c, 0, own1], turn(b1[c + n1 - 1, 0, own1], LANES - hz))
    n_out[0] = red_out
    order_n = [(g, j) for g in range(groups1) for j in range(n1)]
    tile_n = lambda t: b1[c + order_n[t][1], 0, TOP + 8 * order_n[t][0]:TOP + 8 * order_n[t][0] + 8]
    for zi, packed in enumerate(pack_edges(tile_n, n1, COR1)):
        nz_out[zi] = packed
    mail1 = Mail(sems.at[2])
    post1(mail1, n_out, n_in, ny_in, nxy_in, nz_out, nz_in)

    for zi, d in enumerate(zdirs):
        packed = jnp.zeros((8, LANES), jnp.float32)
        for i in range(n0):
            v = a0[0, c + i, 0, own]
            for g in range(groups0):
                lo = COR0 * (g * n0 + i)
                first = lz - COR0 if d > 0 else 0
                here = (lane8 >= lo) & (lane8 < lo + COR0)
                packed = jnp.where(here, turn(v[8 * g:8 * g + 8], lo - first), packed)
        g_out[zi] = packed
    mail0 = Mail(sems.at[3])
    for side in near:
        src, dst = side.source(c, n0, 2), side.target(c, n0, 2)
        mail0.add(black0.at[pl.ds(src, 2), 0, own], f0.at[pl.ds(dst, 2), 0, own], *to(side, 0, 0))
        for d in ydirs:
            ysrc, ydst = strip(d, ly)
            mail0.add(
                black0.at[pl.ds(src, 2), 0, pl.ds(ysrc, 8)], f0.at[pl.ds(dst, 2), 0, pl.ds(ydst, 8)], *to(side, d, 0)
            )
    for d in ydirs:
        ysrc, ydst = strip(d, ly)
        mail0.add(
            black0.at[pl.ds(c, n0), 0, pl.ds(ysrc, 8)], f0.at[pl.ds(c, n0), 0, pl.ds(ydst, 8)], *to(None, d, 0)
        )
    for zi, dz in enumerate(zdirs):
        for s, side in enumerate([None] + near):
            for yi, d in enumerate((1, 0, -1)):
                mail0.add(g_out.at[zi], g_in.at[zi, s, yi], *to(side, d, dz))

    others(gather_wait)

    per = LANES // qz
    for k in range(gx * gy):
        cx, cy = k // gy, k % gy
        for g in range(gz // per):
            parts = [slots[k * gz + g * per + q] for q in range(per)]
            for h in range(per_colour):
                for colour, ref in ((0, b2r), (1, b2b)):
                    at = colour * per_colour + h
                    v = None
                    for q in range(per):
                        moved = turn(parts[q], (q - at) * qz)
                        here = (lane8 >= q * qz) & (lane8 < (q + 1) * qz)
                        v = moved if v is None else jnp.where(here, moved, v)
                    ref[1 + cx, PAD + cy * qy + 8 * h:PAD + cy * qy + 8 * h + 8, LANES * g:LANES * (g + 1)] = v

    def coarse_total(src, i, red, rows, full):
        width_z = src.shape[2]
        lo, hi = PAD, PAD + rows
        v = src[i, lo:hi]
        low, high = turn(v, 1), turn(v, -1)
        lane = iota(v.shape, 1)
        if full:
            low = jnp.where(lane == 0, 0.0, low)
            high = jnp.where(lane == width_z - 1, 0.0, high)
        chess = evens(rows, width_z)
        prev, nxt = src[i - 1, lo:hi], src[i + 1, lo:hi]
        beside = jnp.where(chess, prev, nxt) if red else jnp.where(chess, nxt, prev)
        total = (v + beside) + (src[i, lo - 1:hi - 1] + src[i, lo + 1:hi + 1])
        return v, total + (low + high)

    def coarse(dst, src, b, pairs, red, factor, rows, scale, full):
        for i in range(1, pairs + 1):
            _, total = coarse_total(src, i, red, rows, full)
            dst[i, PAD:PAD + rows] = (b[i, PAD:PAD + rows] * factor + total) * scale

    in2 = slice(PAD, PAD + y2)
    for i in range(1, p2 + 1):
        r2[i, in2] = (b2r[i, in2] * 16.0) * SIXTH
    coarse(v2, r2, b2b, p2, False, 16.0, y2, SIXTH, True)
    coarse(r2, v2, b2r, p2, True, 16.0, y2, SIXTH, True)
    coarse(v2, r2, b2b, p2, False, 16.0, y2, SIXTH, True)

    fold = jnp.where(iota((z2, z3p), 1) == iota((z2, z3p), 0) // 2, 0.125, 0.0)
    parts = []
    for i in range(1, p2 + 1):
        red, from_black = r2[i, in2], coarse_total(v2, i, True, y2, True)[1]
        black, from_red = v2[i, in2], coarse_total(r2, i, False, y2, True)[1]
        r = b2r[i, in2] - (6.0 * red - from_black) * 0.0625
        r = r + (b2b[i, in2] - (6.0 * black - from_red) * 0.0625)
        for g in range(z2 // LANES):
            w2[i - 1, g, 0:y2] = r[:, LANES * g:LANES * (g + 1)]
        parts.append(
            jnp.concatenate(
                [
                    w2[i - 1, g, pl.ds(0, y3, stride=2), :] + w2[i - 1, g, pl.ds(1, y3, stride=2), :]
                    for g in range(z2 // LANES)
                ],
                axis=1,
            )
        )
    r = dot(jnp.concatenate(parts, axis=0), fold)
    chess3 = evens(y3, z3p)
    in3 = slice(PAD, PAD + y3)
    for j in range(p3):
        one, two = r[2 * j * y3:(2 * j + 1) * y3], r[(2 * j + 1) * y3:(2 * j + 2) * y3]
        b3r[1 + j, in3] = jnp.where(chess3, one, two)
        b3b[1 + j, in3] = jnp.where(chess3, two, one)

    full3 = z3 == z3p
    scale3 = SIXTH if full3 else jnp.where(iota((y3, z3p), 1) < z3, SIXTH, 0.0)

    def sweep3(_, carry):
        coarse(r3, v3, b3r, p3, True, 64.0, y3, scale3, full3)
        coarse(v3, r3, b3b, p3, False, 64.0, y3, scale3, full3)
        return carry

    if p3 == 1:
        for _ in range(CSWEEPS):
            sweep3(0, 0)
    else:
        lax.fori_loop(0, CSWEEPS, sweep3, 0)

    def plane(red, black, chess, odd):
        return jnp.where(chess, black, red) if odd else jnp.where(chess, red, black)

    grow = jnp.where(iota((z3p, z2), 0) == iota((z3p, z2), 1) // 2, 1.0, 0.0)
    v = jnp.concatenate(
        [plane(r3[1 + i // 2, in3], v3[1 + i // 2, in3], chess3, i % 2) for i in range(p2)], axis=0
    )
    v = dot(v, grow)
    for i in range(p2):
        part = v[i * y3:(i + 1) * y3]
        for g in range(z2 // LANES):
            w2[i, g, pl.ds(0, y3, stride=2), :] = part[:, LANES * g:LANES * (g + 1)]
            w2[i, g, pl.ds(1, y3, stride=2), :] = part[:, LANES * g:LANES * (g + 1)]
    for i in range(p2):
        for g in range(z2 // LANES):
            lanes = slice(LANES * g, LANES * (g + 1))
            v2[1 + i, in2, lanes] = v2[1 + i, in2, lanes] + w2[i, g, 0:y2]
    for _ in range(2):
        coarse(r2, v2, b2r, p2, True, 16.0, y2, SIXTH, True)
        coarse(v2, r2, b2b, p2, False, 16.0, y2, SIXTH, True)

    mail1.wait()
    grow1 = jnp.where(
        iota((z2, LANES), 0) == mz * qz + (iota((z2, LANES), 1) - left + 2 * LANES) // 2 - LANES, 1.0, 0.0
    )
    rows1 = f1.shape[2]
    half1 = rows1 // 2
    rows2 = pl.ds(pl.multiple_of(my * qy, 8), half1)
    chess2 = evens(half1, z2)
    first, length = span(n1, HALO)
    begin = first - c + mx * n1
    shift = 0 if gx <= 2 else 1
    first_even = begin - shift
    tops = []
    for j in range(length):
        at = j + shift
        index = (first_even + (at - at % 2)) // 2 + 1
        if gx > 2:
            index = jnp.clip(index, 0, p2 + 1)
        tops.append(plane(r2[index, rows2], v2[index, rows2], chess2, at % 2))
    v = dot(jnp.concatenate(tops, axis=0), grow1)
    for j in range(length):
        part = v[j * half1:(j + 1) * half1]
        w1[j, pl.ds(0, half1, stride=2), :] = part
        w1[j, pl.ds(1, half1, stride=2), :] = part

    near_lanes = (lane_l >= left - COR1) & (lane_l < left + hz + COR1)
    for s, side, j, at in regions1():
        for n, (which, group, rows, yi) in enumerate(row_groups()):
            to_rows = slice(PAD + 8 * n, PAD + 8 * n + 8)
            if rows is None:
                base = ny_in[yi, 0] if s is None else nxy_in[s, yi, 0]
            elif s is None:
                base = None
            else:
                base = n_in[s, 0, 8 * rows:8 * rows + 8]
            if base is None:
                middle = b1[at, 0, to_rows]
            else:
                middle = base if j == 0 else turn(base, LANES - hz)
            outer = edges(nz_in, s, which, COR1 * (group * n1 + j), COR1)
            value = jnp.where(mid8, middle, jnp.where(near_lanes, outer, 0.0))
            f1[at, 0, to_rows] = value + w1[at - first, to_rows, :]

    for step in range(4):
        k = (5 - step + 1) // 2
        if step % 2 == 0:
            relax(r1, f1, rhs1[0], s1, n1, k, True, 4.0)
        else:
            relax(f1, r1, rhs1[1], s1, n1, k, False, 4.0)

    mail0.wait()
    grow0 = jnp.where(
        iota((LANES, 2 * LANES), 0) == (left + iota((LANES, 2 * LANES), 1) // 2) % LANES, 1.0, 0.0
    )
    half0 = rows0 // 2
    first, length = span(n0, 2)
    chess_h = evens(half0, LANES)
    tops = []
    for j in range(length):
        index = (first - c + j - j % 2) // 2 + c if gx <= 2 else (first - c + j) // 2 + c
        red, black = r1[index, 0, PAD:PAD + half0], f1[index, 0, PAD:PAD + half0]
        tops.append(plane(red, black, chess_h, j % 2))
    v = dot(jnp.concatenate(tops, axis=0), grow0)
    for j in range(length):
        for g in range(2):
            base = (2 * j + g) * rows0
            part = v[j * half0:(j + 1) * half0, LANES * g:LANES * (g + 1)]
            w0[pl.ds(base, half0, stride=2), :] = part
            w0[pl.ds(base + 1, half0, stride=2), :] = part

    for i in range(n0):
        at = c + i
        j = at - first
        lift = w0[pl.ds(pl.multiple_of(2 * j * rows0, 8) + TOP, ly), :]
        f0[at, 0, own] = black0[at, 0, own] + lift
        for rows in (slice(PAD, TOP), slice(TOP + ly, TOP + ly + 8)):
            lift = w0[pl.ds(pl.multiple_of(2 * j * rows0, 8) + rows.start, 8), :]
            f0[at, 0, rows] = f0[at, 0, rows] + lift
    for side in near:
        for k in (1, 2):
            at = side.landing(c, n0, k)
            j = at - first
            lift = w0[pl.ds(pl.multiple_of(2 * j * rows0, 8) + PAD, rows_h), :]
            f0[at, 0, PAD:PAD + rows_h] = f0[at, 0, PAD:PAD + rows_h] + lift
    for s, side in enumerate([None] + near):
        pairs = range(n0) if side is None else (1, 2)
        for k in pairs:
            if side is None:
                at, far = c + k, k
            else:
                at = side.landing(c, n0, k)
                far = None
            for n in range(groups0 + 2):
                which, group = (0, groups0 - 1) if n == 0 else ((2, 0) if n > groups0 else (1, n - 1))
                tiles = []
                for zi in range(2):
                    t = g_in[zi, s, which]
                    if far is not None:
                        lo = COR0 * (group * n0 + far)
                        tiles.append(turn(t, (LANES - COR0 if zi == 0 else 0) - lo))
                    elif side.dynamic:
                        spot = (LANES - COR0 if zi == 0 else 0)
                        a = turn(t, spot - COR0 * (group * n0 + k - 1))
                        b = turn(t, spot - COR0 * (group * n0 + n0 - k))
                        tiles.append(jnp.where(side.up, a, b))
                    else:
                        far_at = n0 - k if side.up else k - 1
                        tiles.append(turn(t, (LANES - COR0 if zi == 0 else 0) - COR0 * (group * n0 + far_at)))
                low, high = tiles
                value = jnp.where(lane8 >= LANES - COR0, low, jnp.where(lane8 < COR0, high, 0.0))
                j = at - first
                to_rows = slice(PAD + 8 * n, PAD + 8 * n + 8)
                lift = w0[pl.ds(pl.multiple_of((2 * j + 1) * rows0, 8) + PAD + 8 * n, 8), :]
                f0[at, 1, to_rows] = value + lift

    relax(r0, f0, rhs0[0], s0, n0, 2, True, 1.0)
    relax(f0, r0, rhs0[1], s0, n0, 1, False, 1.0)
    relax(r0, f0, rhs0[0], s0, n0, 1, True, 1.0)

    def emit(j, red, black):
        out_ref[2 * j] = jnp.where(even, red, black)
        out_ref[2 * j + 1] = jnp.where(even, black, red)

    relax(None, r0, rhs0[1], s0, n0, 0, False, 1.0, tiles=1, emit=emit)


def local(sizes, right_side, start):
    gx, gy, gz = sizes
    lx, ly, lz = start.shape
    f32 = jnp.float32
    count = gx * gy * gz
    near = {1: 0, 2: 1}.get(gx, 2)
    far = {1: 0, 2: 1}.get(gx, 4)
    n0, n1 = lx // 2, lx // 4
    m0, m1 = n0 + 2 * HALO, n1 + 2 * HALO
    r0, r1 = ly + 2 * TOP, ly // 2 + 2 * TOP
    hy = ly // 2
    y2, z2 = gy * ly // 4, gz * lz // 4
    p2, p3 = gx * lx // 8, gx * lx // 16
    y3, z3 = y2 // 2, z2 // 2
    z3p = -(-z3 // LANES) * LANES
    dx = min(gx - 1, -(-REACH2 // (lx // 4)))
    dy = min(gy - 1, -(-REACH2 // (ly // 4)))
    dz = min(gz - 1, -(-REACH2 // (lz // 4)))
    rounds = max(2, sum(max(0, d - 2) for d in (dx, dy, dz)) - 1)
    near_a, far_a = max(near, 1), max(far, 1)

    def vmem(*shape):
        return pltpu.VMEM(shape, f32)

    messages = 24 if gx <= 2 else 48
    return pl.pallas_call(
        functools.partial(kernel, sizes),
        out_shape=jax.ShapeDtypeStruct(start.shape, f32),
        in_specs=[pl.BlockSpec(memory_space=pl.ANY)] * 2,
        out_specs=pl.BlockSpec(memory_space=pltpu.VMEM),
        scratch_shapes=[
            vmem(lx, ly, lz),
            vmem(lx, ly, lz),
            vmem(3, m0, 2, r0, LANES),
            vmem(m0, 2, r0, LANES),
            vmem(m0, 2, r0, LANES),
            vmem(2, r0 - 2 * PAD, LANES),
            vmem(near_a, ly, LANES),
            vmem(near_a, ly, LANES),
            vmem(2, ly, LANES),
            vmem(2, ly + 16, LANES),
            vmem(near_a, 2, 8, LANES),
            vmem(near_a, 2, 3, 8, LANES),
            vmem(near_a, 2, 16, LANES),
            vmem(near_a, 2, 16, LANES),
            vmem(2, m1, 1, r1, LANES),
            vmem(m1, 1, r1, LANES),
            vmem(m1, 1, r1, LANES),
            vmem(m1, 1, r1, LANES),
            vmem(1, r1 - 2 * PAD, LANES),
            vmem(2 * m0 * r0, LANES),
            vmem(m1, r1, LANES),
            vmem(n1, hy, LANES),
            vmem(far_a, n1, hy, LANES),
            vmem(2, n1, 8, LANES),
            vmem(far_a, 2, n1, 8, LANES),
            vmem(2, 8, LANES),
            vmem(2, far + 1, 3, 8, LANES),
            vmem(1, hy, LANES),
            vmem(far_a, 1, hy, LANES),
            vmem(2, 1, 8, LANES),
            vmem(far_a, 2, 1, 8, LANES),
            vmem(2, 8, LANES),
            vmem(2, far + 1, 3, 8, LANES),
            vmem(2, 8, LANES),
            vmem(2, near + 1, 3, 8, LANES),
            vmem(p2 + 2, y2 + 2 * PAD, z2),
            vmem(p2 + 2, y2 + 2 * PAD, z2),
            vmem(p2 + 2, y2 + 2 * PAD, z2),
            vmem(p2 + 2, y2 + 2 * PAD, z2),
            vmem(8, LANES),
            vmem(count, 8, LANES),
            vmem(p2, z2 // LANES, y2, LANES),
            vmem(p3 + 2, y3 + 2 * PAD, z3p),
            vmem(p3 + 2, y3 + 2 * PAD, z3p),
            vmem(p3 + 2, y3 + 2 * PAD, z3p),
            vmem(p3 + 2, y3 + 2 * PAD, z3p),
            pltpu.SemaphoreType.DMA((2,)),
            pltpu.SemaphoreType.REGULAR((rounds,)),
            pltpu.SemaphoreType.DMA((4, 2, messages)),
            pltpu.SemaphoreType.DMA((2, count)),
        ],
        compiler_params=pltpu.CompilerParams(
            collective_id=0, has_side_effects=True, vmem_limit_bytes=GRANT
        ),
    )(right_side, start)


def solution(mesh):
    sizes = (mesh.shape["gx"], mesh.shape["gy"], mesh.shape["gz"])
    spec = P("gx", "gy", "gz")
    return jax.shard_map(
        functools.partial(local, sizes), mesh=mesh, in_specs=(spec, spec), out_specs=spec, check_vma=False
    )
```

```python
import functools

import jax
import jax.numpy as jnp
from jax import lax
from jax.experimental import pallas as pl
from jax.experimental.pallas import tpu as pltpu
from jax.sharding import PartitionSpec as P

MESH = pl.DeviceIdType.MESH
SIXTH = 1.0 / 6.0
PAD = 8
TOP = 16
LANES = 128
HALO = 3
CSWEEPS = 8
REACH2 = 42
EDGE = ((0, 1, 4), (0, 2, 2), (1, 1, 3), (1, 2, 1), (2, 1, 2))
FACE = 5
RHS1 = 5
COR1 = 6
COR0 = 4
GRANT = 56150000


def dot(a, b):
    high = a.astype(jnp.bfloat16)
    rest = a - high.astype(jnp.float32)
    middle = rest.astype(jnp.bfloat16)
    low = (rest - middle.astype(jnp.float32)).astype(jnp.bfloat16)
    b = b.astype(jnp.bfloat16)
    return jnp.dot(
        jnp.concatenate([high, middle, low], axis=1),
        jnp.concatenate([b, b, b], axis=0),
        preferred_element_type=jnp.float32,
    )


def iota(shape, axis):
    return lax.broadcasted_iota(jnp.int32, shape, axis)


def turn(v, shift):
    shift %= v.shape[1]
    return pltpu.roll(v, shift, axis=1) if shift else v


def evens(rows, lanes, add=0):
    shape = (rows // 8, 8, lanes)
    return ((iota(shape, 1) + iota(shape, 2) + add) & 1).reshape(rows, lanes) == 0


def both(*terms):
    out = True
    for term in terms:
        if term is True:
            continue
        out = term if out is True else out & term
    return out


def when(condition, action):
    if condition is True:
        action()
    else:
        pl.when(condition)(action)


class Side:
    def __init__(self, hop, up, send, recv, peer):
        self.hop, self.up, self.send, self.recv, self.peer = hop, up, send, recv, peer
        self.dynamic = not isinstance(up, bool)

    def pick(self, a, b):
        if self.dynamic:
            return jnp.where(self.up, a, b)
        return a if self.up else b

    def source(self, c, n, count):
        return self.pick(c + n - count, c)

    def target(self, c, n, count):
        return self.pick(c - count, c + n)

    def landing(self, c, n, k):
        if self.dynamic:
            return jnp.where(self.up, c + n + k - 1, c - k)
        return c - k if self.up else c + n + k - 1

    def outward(self, c, n, k):
        return self.pick(c + n - k, c + k - 1)

    def base(self, c, n):
        if self.dynamic:
            return jnp.where(self.up, c + n, c - n)
        return c - self.hop * n if self.up else c + self.hop * n

    def send_shift(self):
        return self.pick(0, 1)

    def recv_shift(self):
        return jnp.where(self.up, 1, 0) if self.dynamic else (0 if self.up else 1)


class Mail:
    def __init__(self, sems):
        self.sems, self.count, self.items = sems, 0, []

    def add(self, src, dst, send, recv, peer, tag=None):
        at = self.count
        self.count += 1
        copy = pltpu.make_async_remote_copy(
            src_ref=src,
            dst_ref=dst,
            send_sem=self.sems.at[0, at],
            recv_sem=self.sems.at[1, at],
            device_id=peer,
            device_id_type=MESH,
        )
        self.items.append((tag, copy, send, recv))
        when(send, copy.start)

    def wait(self, tag=None):
        for item in list(self.items):
            name, copy, send, recv = item
            if tag is None or name == tag:
                when(send, copy.wait_send)
                when(recv, copy.wait_recv)
                self.items.remove(item)


def kernel(
    sizes, rhs_hbm, start_hbm, out_ref,
    rhs, start, a0, r0, f0, s0, merged_out, merged_in, zsend, zrecv, esend, erecv, yedge_out, yedge_in,
    a1, r1, b1, f1, s1, w0, w1, tiles_out, tiles_in, ysides, xysides, zout, zin,
    n_out, n_in, ny_in, nxy_in, nz_out, nz_in, g_out, g_in,
    b2r, b2b, r2, v2, pack, slots, w2, b3r, b3b, r3, v3,
    in_sems, relay, sems, gather_sems,
):
    gx, gy, gz = sizes
    count = gx * gy * gz
    mx, my, mz = lax.axis_index("gx"), lax.axis_index("gy"), lax.axis_index("gz")
    lx, ly, lz = start.shape
    n0, n1 = lx // 2, lx // 4
    hy, hz = ly // 2, lz // 2
    qy, qz = hy // 2, hz // 2
    left = (LANES - hz) // 2
    c = HALO
    y2, z2 = gy * qy, gz * qz
    p2, p3 = gx * lx // 8, gx * lx // 16
    y3, z3 = y2 // 2, z2 // 2
    z3p = r3.shape[2]
    groups0, groups1 = ly // 8, hy // 8

    copies = [
        pltpu.make_async_copy(start_hbm, start, in_sems.at[0]),
        pltpu.make_async_copy(rhs_hbm, rhs, in_sems.at[1]),
    ]
    for copy in copies:
        copy.start()

    if gx == 1:
        near, sides1 = [], []
    elif gx == 2:
        near = sides1 = [Side(1, mx == 0, True, True, 1 - mx)]
    else:
        def side(hop, up):
            if up:
                return Side(hop, True, mx + hop < gx, mx >= hop, mx + hop)
            return Side(hop, False, mx >= hop, mx + hop < gx, mx - hop)

        near = [side(1, True), side(1, False)]
        sides1 = near + [side(2, True), side(2, False)]

    def along(at, size, step):
        if step == 0:
            return True, True, at
        if step > 0:
            return at + 1 < size, at >= 1, at + 1
        return at >= 1, at + 1 < size, at - 1

    def to(side, dy, dz):
        sx, rx, px = (True, True, mx) if side is None else (side.send, side.recv, side.peer)
        sy, ry, py = along(my, gy, dy)
        sz, rz, pz = along(mz, gz, dz)
        return both(sx, sy, sz), both(rx, ry, rz), (px, py, pz)

    faces = [to(s, 0, 0) for s in near]
    faces += [to(None, d, 0) for d in (1, -1)] + [to(None, 0, d) for d in (1, -1)]

    def signal_faces(sem):
        for send, _, peer in faces:
            when(send, lambda peer=peer: pl.semaphore_signal(sem, inc=1, device_id=peer, device_id_type=MESH))

    heard = sum([(1 if recv is True else jnp.where(recv, 1, 0)) for _, recv, _ in faces])

    def clear(*refs):
        for ref in refs:
            ref[...] = jnp.zeros_like(ref)

    rows0 = a0.shape[3]
    own = slice(TOP, TOP + ly)
    outside = [i for i in range(a0.shape[1]) if i < c or i >= c + n0]
    clear(zrecv, erecv, yedge_in)
    for q in range(3):
        for i in range(c, c + n0):
            a0[q, i, 0, PAD:TOP] = jnp.zeros((PAD, LANES), jnp.float32)
            a0[q, i, 0, TOP + ly:TOP + ly + PAD] = jnp.zeros((PAD, LANES), jnp.float32)
        if gx != 2:
            for i in outside:
                a0[q, i, 0, own] = jnp.zeros((ly, LANES), jnp.float32)
    if gx != 2:
        clear(merged_in)
    barrier = pltpu.get_barrier_semaphore()
    signal_faces(barrier)
    clear(slots)

    def mask(shape, row0, lane_of, bounds):
        y = iota(shape, 0) + row0
        z = lane_of(iota(shape, 1))
        inside = (y >= 0) & (y < bounds[0]) & (z >= 0) & (z < bounds[1])
        return jnp.where(inside, SIXTH, 0.0)

    even = evens(ly, LANES)
    for copy in copies:
        copy.wait()
    for i in range(n0):
        a0[0, c + i, 0, own] = jnp.where(even, start[2 * i + 1], start[2 * i])
        a0[1, c + i, 0, own] = jnp.where(even, rhs[2 * i], rhs[2 * i + 1])
        a0[2, c + i, 0, own] = jnp.where(even, rhs[2 * i + 1], rhs[2 * i])
    for s, side in enumerate(near):
        third = a0[0, side.outward(c, n0, 3), 0, own]
        second = a0[2, side.outward(c, n0, 2), 0, own]
        merged_out[s] = jnp.where(evens(ly, LANES, side.send_shift()), third, pltpu.roll(second, 1, axis=0))

    pl.semaphore_wait(barrier, heard)

    lane64 = iota((ly, LANES), 1)
    lane8 = iota((8, LANES), 1)
    ydirs = zdirs = (1, -1)
    mail = Mail(sems.at[0])
    for s, side in enumerate(near):
        where = to(side, 0, 0)
        src, dst = side.source(c, n0, 2), side.target(c, n0, 2)
        mail.add(a0.at[0:2, pl.ds(src, 2), 0, own], a0.at[0:2, pl.ds(dst, 2), 0, own], *where)

    def strip(d, rows):
        return (TOP + rows - 8, TOP - 8) if d > 0 else (TOP, TOP + rows)

    for d in ydirs:
        src, dst = strip(d, ly)
        mail.add(
            a0.at[0:3, pl.ds(c, n0), 0, pl.ds(src, 8)],
            a0.at[0:3, pl.ds(c, n0), 0, pl.ds(dst, 8)],
            *to(None, d, 0), "z",
        )
    signal_faces(relay.at[0])
    clear(ysides, xysides, tiles_in, zin, n_in, ny_in, nxy_in, nz_in, g_in)

    slots0 = [(q, i) for i in range(n0) for q in range(3)]
    for zi, d in enumerate(zdirs):
        packed = jnp.zeros((ly, LANES), jnp.float32)
        for t, (q, i) in enumerate(slots0):
            v = a0[q, c + i, 0, own]
            first = lz - FACE if d > 0 else 0
            here = (lane64 >= FACE * t) & (lane64 < FACE * (t + 1))
            packed = jnp.where(here, turn(v, FACE * t - first), packed)
        zsend[zi] = packed
    for zi, d in enumerate(zdirs):
        mail.add(zsend.at[zi], zrecv.at[zi, pl.ds(8, ly)], *to(None, 0, d), "z")

    width = sum(w for _, _, w in EDGE)
    starts = [sum(w for _, _, w in EDGE[:t]) for t in range(len(EDGE))]
    for s, side in enumerate(near):
        for zi, d in enumerate(zdirs):
            packed = jnp.zeros((8, LANES), jnp.float32)
            for (q, k, w), at in zip(EDGE, starts):
                v = a0[q, side.outward(c, n0, k), 0, own]
                for g in range(groups0):
                    lo = width * g + at
                    first = lz - w if d > 0 else 0
                    here = (lane8 >= lo) & (lane8 < lo + w)
                    packed = jnp.where(here, turn(v[8 * g:8 * g + 8], lo - first), packed)
            esend[s, zi] = packed
        for yi, d in enumerate(ydirs):
            for (q, k, w), at in zip(EDGE, starts):
                first = TOP + ly - w if d > 0 else TOP
                yedge_out[s, yi, at:at + w] = a0[q, side.outward(c, n0, k), 0, first:first + w]
    pl.semaphore_wait(relay.at[0], heard)
    signal_faces(relay.at[1])
    for s, side in enumerate(near):
        for yi, d in enumerate(ydirs):
            mail.add(yedge_out.at[s, yi], yedge_in.at[s, yi], *to(side, d, 0), "y")
    for zi, dz in enumerate(zdirs):
        for d in ydirs:
            src, dst = strip(d, ly)
            mail.add(
                zsend.at[zi, pl.ds(src - TOP, 8)], zrecv.at[zi, pl.ds(dst - 8, 8)], *to(None, d, dz), "z"
            )
        for s, side in enumerate(near):
            mail.add(esend.at[s, zi], erecv.at[s, zi, 1], *to(side, 0, dz), "e")
    rounds = relay.shape[0]
    pl.semaphore_wait(relay.at[1], heard)
    for zi, dz in enumerate(zdirs):
        for s, side in enumerate(near):
            for d in ydirs:
                half = pl.ds(4 if d > 0 else 0, 4)
                mail.add(esend.at[s, zi, half], erecv.at[s, zi, 0 if d > 0 else 2, half], *to(side, d, dz), "e")
    for s, side in enumerate(near):
        where = to(side, 0, 0)
        src, dst = side.source(c, n0, 1), side.target(c, n0, 1)
        mail.add(a0.at[2, pl.ds(src, 1), 0, own], a0.at[2, pl.ds(dst, 1), 0, own], *where)
        mail.add(merged_out.at[s], merged_in.at[s], *where)
    for r in range(2, rounds):
        signal_faces(relay.at[r])
        pl.semaphore_wait(relay.at[r], heard)
    clear(r0, f0)
    for q in range(3):
        for i in range(a0.shape[1]):
            a0[q, i, 1] = jnp.zeros((rows0, LANES), jnp.float32)
            edge = PAD if c <= i < c + n0 else TOP
            a0[q, i, 0, 0:edge] = jnp.zeros((edge, LANES), jnp.float32)
            a0[q, i, 0, rows0 - edge:] = jnp.zeros((edge, LANES), jnp.float32)
    if gx == 2:
        for k in range(1, HALO + 1):
            a0[0, jnp.where(mx == 0, c - k, c + n0 + k - 1), 0, own] = jnp.zeros((ly, LANES), jnp.float32)
    fine = (gy * ly, gz * lz)
    s0[0] = mask(s0.shape[1:], my * ly - PAD, lambda k: mz * lz + k, fine)
    s0[1] = mask(s0.shape[1:], my * ly - PAD, lambda k: mz * lz + jnp.where(k < 64, k + lz, k - LANES), fine)
    s1[0] = mask(s1.shape[1:], my * hy - PAD, lambda k: mz * hz + k - left, (gy * hy, gz * hz))

    mail.wait("z")
    rows_h = ly + 16
    lane_h = iota((rows_h, LANES), 1)
    for t, (q, i) in enumerate(slots0):
        low = turn(zrecv[0], LANES - FACE - FACE * t)
        high = turn(zrecv[1], -FACE * t)
        a0[q, c + i, 1, PAD:PAD + rows_h] = jnp.where(
            lane_h >= LANES - FACE, low, jnp.where(lane_h < FACE, high, 0.0)
        )
    def span(n, k):
        if gx == 1:
            return c, n
        k = min(k, n * (gx - 1), HALO)
        if gx == 2:
            return jnp.where(mx == 0, c, c - k), n + k
        return c - k, n + 2 * k

    def inside(n, i):
        if gx <= 2:
            return None
        at = mx * n + i - c
        return jnp.where((at >= 0) & (at < gx * n), 1.0, 0.0)

    def neighbours(src, i, planes, red, chess, lo, hi, tiles):
        prev, cur, nxt = planes
        low = [turn(t, 1) for t in cur]
        high = [turn(t, -1) for t in cur]
        if len(cur) == 2:
            lane = iota(cur[0].shape, 1)
            low = [jnp.where(lane == 0, low[1 - g], low[g]) for g in range(tiles)]
            high = [jnp.where(lane == LANES - 1, high[1 - g], high[g]) for g in range(tiles)]
        out = []
        for g in range(tiles):
            beside = jnp.where(chess, prev[g], nxt[g]) if red else jnp.where(chess, nxt[g], prev[g])
            total = (cur[g] + beside) + (src[i, g, lo - 1:hi - 1] + src[i, g, lo + 1:hi + 1])
            out.append(total + (low[g] + high[g]))
        return out

    def relax(dst, src, rhs_of, scale, n, k, red, factor, tiles=None, emit=None, part=None):
        first, length = part or span(n, k)
        held = src.shape[1]
        rows = src.shape[2]
        lo, hi = (TOP, rows - TOP) if emit else (PAD, rows - PAD)
        tiles = tiles or held
        chess = evens(hi - lo, LANES)
        planes = [[src[first + j - 1, g, lo:hi] for g in range(held)] for j in range(length + 2)]
        for j in range(length):
            i = first + j
            totals = neighbours(src, i, planes[j:j + 3], red, chess, lo, hi, tiles)
            factor_x = inside(n, i)
            for g in range(tiles):
                b = rhs_of(i, g, lo, hi)
                if factor != 1.0:
                    b = b * factor
                value = (b + totals[g]) * scale[g, lo - PAD:hi - PAD]
                if factor_x is not None:
                    value = value * factor_x
                if emit:
                    emit(j, planes[j + 1][g], value)
                else:
                    dst[i, g, lo:hi] = value

    def residual(red_ref, black_ref, red_rhs, black_rhs, n, j, factor):
        rows = red_ref.shape[2]
        lo, hi = TOP, rows - TOP
        chess = evens(hi - lo, LANES)
        i = c + j
        held = red_ref.shape[1]

        def load(ref):
            return [[ref[i + d, g, lo:hi] for g in range(held if d == 0 else 1)] for d in (-1, 0, 1)]

        red, black = load(red_ref), load(black_ref)
        from_black = neighbours(black_ref, i, black, True, chess, lo, hi, 1)[0]
        from_red = neighbours(red_ref, i, red, False, chess, lo, hi, 1)[0]
        out = red_rhs(i, 0, lo, hi) - (6.0 * red[1][0] - from_black) * (1.0 / factor)
        return out + (black_rhs(i, 0, lo, hi) - (6.0 * black[1][0] - from_red) * (1.0 / factor))

    black0 = a0.at[0]
    rhs0 = [lambda i, g, lo, hi, q=q: a0[q, i, g, lo:hi] for q in (1, 2)]
    def sweep0(step, part):
        if step % 2 == 0:
            relax(r0, black0, rhs0[0], s0, n0, 0, True, 1.0, part=part)
        else:
            relax(black0, r0, rhs0[1], s0, n0, 0, False, 1.0, part=part)

    def early(step):
        return n0 - 1 - step if gx == 2 else 0

    for step in range(4):
        if early(step) > 0:
            sweep0(step, (jnp.where(mx == 0, c, c + n0 - early(step)), early(step)))
    mail.wait("e")
    for s, side in enumerate(near):
        for (q, k, w), at in zip(EDGE, starts):
            pair = side.landing(c, n0, k)
            for g in range(groups0 + 2):
                which, group = (0, groups0 - 1) if g == 0 else ((2, 0) if g > groups0 else (1, g - 1))
                lo = width * group + at
                low = turn(erecv[s, 0, which], LANES - w - lo)
                high = turn(erecv[s, 1, which], -lo)
                a0[q, pair, 1, PAD + 8 * g:PAD + 8 * g + 8] = jnp.where(
                    lane8 >= LANES - w, low, jnp.where(lane8 < w, high, 0.0)
                )

    mail.wait("y")
    for s, side in enumerate(near):
        for yi, d in enumerate(ydirs):
            for (q, k, w), at in zip(EDGE, starts):
                first = TOP - w if d > 0 else TOP + ly
                a0[q, side.landing(c, n0, k), 0, first:first + w] = yedge_in[s, yi, at:at + w]
    mail.wait()
    for s, side in enumerate(near):
        v = merged_in[s]
        a0[0, side.landing(c, n0, 3), 0, own] = v
        a0[2, side.landing(c, n0, 2), 0, own] = pltpu.roll(v, ly - 1, axis=0)
    for step in range(4):
        first, length = span(n0, (4 - step + 1) // 2)
        done = max(early(step), 0)
        if done:
            first = first + jnp.where(mx == 0, done, 0)
        sweep0(step, (first, length - done))
    for j in range(n0):
        w0[j * ly:(j + 1) * ly, :] = residual(r0, black0, rhs0[0], rhs0[1], n0, j, 1.0)
    r = w0[pl.ds(0, n0 * hy, stride=2), :] + w0[pl.ds(1, n0 * hy, stride=2), :]
    source, target = iota((LANES, LANES), 0), iota((LANES, LANES), 1)
    fold = jnp.where(lax.rem(target - left + LANES, hz) == source // 2, 0.125, 0.0)
    r = dot(r, fold)

    own1 = slice(TOP, TOP + hy)
    lane32 = iota((hy, LANES), 1)
    mid = (lane32 >= left) & (lane32 < left + hz)
    chess1 = evens(hy, LANES)
    for j in range(n1):
        one, two = r[2 * j * hy:(2 * j + 1) * hy], r[(2 * j + 1) * hy:(2 * j + 2) * hy]
        red = jnp.where(chess1, one, two)
        black = jnp.where(chess1, two, one)
        tiles_out[j] = jnp.where(mid, red, black)
        a1[0, c + j, 0, own1] = jnp.where(mid, red, 0.0)
        a1[1, c + j, 0, own1] = jnp.where(mid, black, 0.0)

    def pack_edges(read, items, w):
        for d in zdirs:
            first = left + hz - w if d > 0 else left
            packed = jnp.zeros((8, LANES), jnp.float32)
            for t in range(items * groups1):
                here = (lane8 >= w * t) & (lane8 < w * (t + 1))
                packed = jnp.where(here, turn(read(t), w * t - first), packed)
            yield packed

    def post1(mail, out, into, y_in, xy_in, z_out, z_in):
        for s, side in enumerate(sides1):
            mail.add(out, into.at[s], *to(side, 0, 0))
        for yi, d in enumerate(ydirs):
            src = hy - 8 if d > 0 else 0
            mail.add(out.at[:, pl.ds(src, 8)], y_in.at[yi], *to(None, d, 0))
        for s, side in enumerate(sides1):
            for yi, d in enumerate(ydirs):
                src = hy - 8 if d > 0 else 0
                mail.add(out.at[:, pl.ds(src, 8)], xy_in.at[s, yi], *to(side, d, 0))
        for zi, dz in enumerate(zdirs):
            for s, side in enumerate([None] + sides1):
                for yi, d in enumerate((1, 0, -1)):
                    mail.add(z_out.at[zi], z_in.at[zi, s, yi], *to(side, d, dz))

    def regions1():
        yield from ((None, None, j, c + j) for j in range(n1))
        for s, side in enumerate(sides1):
            for j in range(n1):
                at = side.base(c, n1) + j
                if side.dynamic or 0 <= at < 2 * c + n1:
                    yield (s, side, j, at)

    def row_groups():
        yield 0, groups1 - 1, None, 0
        for g in range(groups1):
            yield 1, g, g, None
        yield 2, 0, None, 1

    lane_l = lane8
    mid8 = (lane_l >= left) & (lane_l < left + hz)

    def edges(z_in, s, which, lo, w):
        at = 0 if s is None else s + 1
        low = turn(z_in[0, at, which], left - w - lo)
        high = turn(z_in[1, at, which], left + hz - lo)
        return jnp.where(lane_l < left, low, high)

    items = 2 * n1
    order1 = [(g, q, j) for g in range(groups1) for j in range(n1) for q in range(2)]
    tile_of = lambda t: a1[order1[t][1], c + order1[t][2], 0, TOP + 8 * order1[t][0]:TOP + 8 * order1[t][0] + 8]
    for zi, packed in enumerate(pack_edges(tile_of, items, RHS1)):
        zout[zi] = packed
    mail = Mail(sems.at[1])
    post1(mail, tiles_out, tiles_in, ysides, xysides, zout, zin)
    for ref in (a1, r1, b1, f1):
        for i in range(ref.shape[-4]):
            halo_pair = i < c or i >= c + n1
            lead = (slice(None),) if len(ref.shape) == 5 else ()
            if halo_pair or ref is not a1:
                at = lead + (i,)
                ref[at] = jnp.zeros(ref[at].shape, jnp.float32)
            else:
                for rows in (slice(0, TOP), slice(TOP + hy, None)):
                    at = lead + (i, slice(None), rows)
                    ref[at] = jnp.zeros(ref[at].shape, jnp.float32)
    for ref in (b2r, b2b, r2, v2, b3r, b3b, r3, v3):
        ref[...] = jnp.zeros_like(ref)
    mail.wait()

    near_lanes = (lane_l >= left - RHS1) & (lane_l < left + hz + RHS1)
    for s, side, j, at in regions1():
        for n, (which, group, rows, yi) in enumerate(row_groups()):
            if rows is None:
                base = ysides[yi, j] if s is None else xysides[s, yi, j]
            elif s is None:
                base = None
            else:
                base = tiles_in[s, j, 8 * rows:8 * rows + 8]
            for q in range(2):
                to_rows = slice(PAD + 8 * n, PAD + 8 * n + 8)
                lo = RHS1 * ((group * n1 + j) * 2 + q)
                if base is None:
                    middle = a1[q, at, 0, to_rows]
                else:
                    middle = base if q == 0 else turn(base, LANES - hz)
                outer = edges(zin, s, which, lo, RHS1)
                a1[q, at, 0, to_rows] = jnp.where(mid8, middle, jnp.where(near_lanes, outer, 0.0))

    rhs1 = [lambda i, g, lo, hi, q=q: a1[q, i, g, lo:hi] for q in (0, 1)]
    first, length = span(n1, 2)
    for j in range(length):
        i = first + j
        value = (a1[0, i, 0, PAD:-PAD] * 4.0) * s1[0]
        factor_x = inside(n1, i)
        r1[i, 0, PAD:-PAD] = value if factor_x is None else value * factor_x
    relax(b1, r1, rhs1[1], s1, n1, 2, False, 4.0)
    relax(r1, b1, rhs1[0], s1, n1, 1, True, 4.0)
    relax(b1, r1, rhs1[1], s1, n1, 1, False, 4.0)

    for j in range(n1):
        w1[j, 0:hy, :] = residual(r1, b1, rhs1[0], rhs1[1], n1, j, 4.0)
    r = jnp.concatenate(
        [w1[j, pl.ds(0, qy, stride=2), :] + w1[j, pl.ds(1, qy, stride=2), :] for j in range(n1)], axis=0
    )
    fold = jnp.where(
        (lax.rem(target, qz) == (source - left) // 2) & (source >= left) & (source < left + hz), 0.125, 0.0
    )
    r = dot(r, fold)
    block = lane8 // qz
    per_colour = qy // 8
    one = two = None
    for h in range(per_colour):
        p, q = r[8 * h:8 * h + 8], r[qy + 8 * h:qy + 8 * h + 8]
        here = lax.rem(block, per_colour) == h
        one = p if one is None else jnp.where(here, p, one)
        two = q if two is None else jnp.where(here, q, two)
    tile = jnp.where(evens(8, LANES) ^ (block >= per_colour), one, two)
    pack[...] = tile

    mine = (mx * gy + my) * gz + mz
    slots[mine] = tile

    dist = (-(-REACH2 // (lx // 4)), -(-REACH2 // qy), -(-REACH2 // qz))

    def coords(k):
        steps = (k // (gy * gz), k // gz % gy, k % gz)
        moved = [at + step for at, step in zip((mx, my, mz), steps)]
        at = tuple(jnp.where(v >= size, v - size, v) for v, size in zip(moved, sizes))
        close = True
        for a, b, size, reach in zip(at, (mx, my, mz), sizes, dist):
            if reach < size - 1:
                close = both(close, (a - b <= reach) & (b - a <= reach))
        return at, close

    def number(at):
        return (at[0] * gy + at[1]) * gz + at[2]

    def flipped(at, k):
        bit = 1
        while bit <= k:
            if k & bit:
                at = at + bit - 2 * bit * lax.rem(lax.div(at, bit), 2)
            bit *= 2
        return at

    def partners():
        own_at = (mx, my, mz)
        flips = [[flipped(at, k) for k in range(size)] for at, size in zip(own_at, sizes)]
        order = [(i, j, k) for i in range(gx) for j in range(gy) for k in range(gz)][1:]
        order.sort(key=lambda f: (-(f[0] + min(f[2], 2) + f[1] // 2), -f[1], f[2]))
        for f in order:
            at = tuple(flips[axis][k] for axis, k in enumerate(f))
            close = True
            for a, b, k, reach in zip(at, own_at, f, dist):
                if k > reach:
                    close = both(close, (a - b <= reach) & (b - a <= reach))
            yield at, close

    straight = count <= 64 and all(size & (size - 1) == 0 for size in sizes)

    def others(body):
        if straight:
            for place in partners():
                body(place)
        else:
            def step(k, carry):
                body(coords(k))
                return carry

            lax.fori_loop(1, count, step, 0)

    def gather(place, arriving):
        at, close = place
        d = number(at)
        return pltpu.make_async_remote_copy(
            src_ref=pack,
            dst_ref=slots.at[d if arriving else mine],
            send_sem=gather_sems.at[0, d],
            recv_sem=gather_sems.at[1, d if arriving else mine],
            device_id=at,
            device_id_type=MESH,
        ), close

    def gather_start(place):
        copy, close = gather(place, False)
        when(close, copy.start)

    def gather_wait(place):
        copy, close = gather(place, True)

        def done():
            copy.wait_send()
            copy.wait_recv()

        when(close, done)

    others(gather_start)

    red_out = jnp.where(mid, b1[c, 0, own1], turn(b1[c + n1 - 1, 0, own1], LANES - hz))
    n_out[0] = red_out
    order_n = [(g, j) for g in range(groups1) for j in range(n1)]
    tile_n = lambda t: b1[c + order_n[t][1], 0, TOP + 8 * order_n[t][0]:TOP + 8 * order_n[t][0] + 8]
    for zi, packed in enumerate(pack_edges(tile_n, n1, COR1)):
        nz_out[zi] = packed
    mail1 = Mail(sems.at[2])
    post1(mail1, n_out, n_in, ny_in, nxy_in, nz_out, nz_in)

    for zi, d in enumerate(zdirs):
        packed = jnp.zeros((8, LANES), jnp.float32)
        for i in range(n0):
            v = a0[0, c + i, 0, own]
            for g in range(groups0):
                lo = COR0 * (g * n0 + i)
                first = lz - COR0 if d > 0 else 0
                here = (lane8 >= lo) & (lane8 < lo + COR0)
                packed = jnp.where(here, turn(v[8 * g:8 * g + 8], lo - first), packed)
        g_out[zi] = packed
    mail0 = Mail(sems.at[3])
    for side in near:
        src, dst = side.source(c, n0, 2), side.target(c, n0, 2)
        mail0.add(black0.at[pl.ds(src, 2), 0, own], f0.at[pl.ds(dst, 2), 0, own], *to(side, 0, 0))
        for d in ydirs:
            ysrc, ydst = strip(d, ly)
            mail0.add(
                black0.at[pl.ds(src, 2), 0, pl.ds(ysrc, 8)], f0.at[pl.ds(dst, 2), 0, pl.ds(ydst, 8)], *to(side, d, 0)
            )
    for d in ydirs:
        ysrc, ydst = strip(d, ly)
        mail0.add(
            black0.at[pl.ds(c, n0), 0, pl.ds(ysrc, 8)], f0.at[pl.ds(c, n0), 0, pl.ds(ydst, 8)], *to(None, d, 0)
        )
    for zi, dz in enumerate(zdirs):
        for s, side in enumerate([None] + near):
            for yi, d in enumerate((1, 0, -1)):
                mail0.add(g_out.at[zi], g_in.at[zi, s, yi], *to(side, d, dz))

    others(gather_wait)

    per = LANES // qz
    for k in range(gx * gy):
        cx, cy = k // gy, k % gy
        for g in range(gz // per):
            parts = [slots[k * gz + g * per + q] for q in range(per)]
            for h in range(per_colour):
                for colour, ref in ((0, b2r), (1, b2b)):
                    at = colour * per_colour + h
                    v = None
                    for q in range(per):
                        moved = turn(parts[q], (q - at) * qz)
                        here = (lane8 >= q * qz) & (lane8 < (q + 1) * qz)
                        v = moved if v is None else jnp.where(here, moved, v)
                    ref[1 + cx, PAD + cy * qy + 8 * h:PAD + cy * qy + 8 * h + 8, LANES * g:LANES * (g + 1)] = v

    def coarse_total(src, i, red, rows, full):
        width_z = src.shape[2]
        lo, hi = PAD, PAD + rows
        v = src[i, lo:hi]
        low, high = turn(v, 1), turn(v, -1)
        lane = iota(v.shape, 1)
        if full:
            low = jnp.where(lane == 0, 0.0, low)
            high = jnp.where(lane == width_z - 1, 0.0, high)
        chess = evens(rows, width_z)
        prev, nxt = src[i - 1, lo:hi], src[i + 1, lo:hi]
        beside = jnp.where(chess, prev, nxt) if red else jnp.where(chess, nxt, prev)
        total = (v + beside) + (src[i, lo - 1:hi - 1] + src[i, lo + 1:hi + 1])
        return v, total + (low + high)

    def coarse(dst, src, b, pairs, red, factor, rows, scale, full):
        for i in range(1, pairs + 1):
            _, total = coarse_total(src, i, red, rows, full)
            dst[i, PAD:PAD + rows] = (b[i, PAD:PAD + rows] * factor + total) * scale

    in2 = slice(PAD, PAD + y2)
    for i in range(1, p2 + 1):
        r2[i, in2] = (b2r[i, in2] * 16.0) * SIXTH
    coarse(v2, r2, b2b, p2, False, 16.0, y2, SIXTH, True)
    coarse(r2, v2, b2r, p2, True, 16.0, y2, SIXTH, True)
    coarse(v2, r2, b2b, p2, False, 16.0, y2, SIXTH, True)

    fold = jnp.where(iota((z2, z3p), 1) == iota((z2, z3p), 0) // 2, 0.125, 0.0)
    parts = []
    for i in range(1, p2 + 1):
        red, from_black = r2[i, in2], coarse_total(v2, i, True, y2, True)[1]
        black, from_red = v2[i, in2], coarse_total(r2, i, False, y2, True)[1]
        r = b2r[i, in2] - (6.0 * red - from_black) * 0.0625
        r = r + (b2b[i, in2] - (6.0 * black - from_red) * 0.0625)
        for g in range(z2 // LANES):
            w2[i - 1, g, 0:y2] = r[:, LANES * g:LANES * (g + 1)]
        parts.append(
            jnp.concatenate(
                [
                    w2[i - 1, g, pl.ds(0, y3, stride=2), :] + w2[i - 1, g, pl.ds(1, y3, stride=2), :]
                    for g in range(z2 // LANES)
                ],
                axis=1,
            )
        )
    r = dot(jnp.concatenate(parts, axis=0), fold)
    chess3 = evens(y3, z3p)
    in3 = slice(PAD, PAD + y3)
    for j in range(p3):
        one, two = r[2 * j * y3:(2 * j + 1) * y3], r[(2 * j + 1) * y3:(2 * j + 2) * y3]
        b3r[1 + j, in3] = jnp.where(chess3, one, two)
        b3b[1 + j, in3] = jnp.where(chess3, two, one)

    full3 = z3 == z3p
    scale3 = SIXTH if full3 else jnp.where(iota((y3, z3p), 1) < z3, SIXTH, 0.0)

    def sweep3(_, carry):
        coarse(r3, v3, b3r, p3, True, 64.0, y3, scale3, full3)
        coarse(v3, r3, b3b, p3, False, 64.0, y3, scale3, full3)
        return carry

    if p3 == 1:
        for _ in range(CSWEEPS):
            sweep3(0, 0)
    else:
        lax.fori_loop(0, CSWEEPS, sweep3, 0)

    def plane(red, black, chess, odd):
        return jnp.where(chess, black, red) if odd else jnp.where(chess, red, black)

    grow = jnp.where(iota((z3p, z2), 0) == iota((z3p, z2), 1) // 2, 1.0, 0.0)
    v = jnp.concatenate(
        [plane(r3[1 + i // 2, in3], v3[1 + i // 2, in3], chess3, i % 2) for i in range(p2)], axis=0
    )
    v = dot(v, grow)
    for i in range(p2):
        part = v[i * y3:(i + 1) * y3]
        for g in range(z2 // LANES):
            w2[i, g, pl.ds(0, y3, stride=2), :] = part[:, LANES * g:LANES * (g + 1)]
            w2[i, g, pl.ds(1, y3, stride=2), :] = part[:, LANES * g:LANES * (g + 1)]
    for i in range(p2):
        for g in range(z2 // LANES):
            lanes = slice(LANES * g, LANES * (g + 1))
            v2[1 + i, in2, lanes] = v2[1 + i, in2, lanes] + w2[i, g, 0:y2]
    for _ in range(2):
        coarse(r2, v2, b2r, p2, True, 16.0, y2, SIXTH, True)
        coarse(v2, r2, b2b, p2, False, 16.0, y2, SIXTH, True)

    mail1.wait()
    grow1 = jnp.where(
        iota((z2, LANES), 0) == mz * qz + (iota((z2, LANES), 1) - left + 2 * LANES) // 2 - LANES, 1.0, 0.0
    )
    rows1 = f1.shape[2]
    half1 = rows1 // 2
    rows2 = pl.ds(pl.multiple_of(my * qy, 8), half1)
    chess2 = evens(half1, z2)
    first, length = span(n1, HALO)
    begin = first - c + mx * n1
    shift = 0 if gx <= 2 else 1
    first_even = begin - shift
    tops = []
    for j in range(length):
        at = j + shift
        index = (first_even + (at - at % 2)) // 2 + 1
        if gx > 2:
            index = jnp.clip(index, 0, p2 + 1)
        tops.append(plane(r2[index, rows2], v2[index, rows2], chess2, at % 2))
    v = dot(jnp.concatenate(tops, axis=0), grow1)
    for j in range(length):
        part = v[j * half1:(j + 1) * half1]
        w1[j, pl.ds(0, half1, stride=2), :] = part
        w1[j, pl.ds(1, half1, stride=2), :] = part

    near_lanes = (lane_l >= left - COR1) & (lane_l < left + hz + COR1)
    for s, side, j, at in regions1():
        for n, (which, group, rows, yi) in enumerate(row_groups()):
            to_rows = slice(PAD + 8 * n, PAD + 8 * n + 8)
            if rows is None:
                base = ny_in[yi, 0] if s is None else nxy_in[s, yi, 0]
            elif s is None:
                base = None
            else:
                base = n_in[s, 0, 8 * rows:8 * rows + 8]
            if base is None:
                middle = b1[at, 0, to_rows]
            else:
                middle = base if j == 0 else turn(base, LANES - hz)
            outer = edges(nz_in, s, which, COR1 * (group * n1 + j), COR1)
            value = jnp.where(mid8, middle, jnp.where(near_lanes, outer, 0.0))
            f1[at, 0, to_rows] = value + w1[at - first, to_rows, :]

    for step in range(4):
        k = (5 - step + 1) // 2
        if step % 2 == 0:
            relax(r1, f1, rhs1[0], s1, n1, k, True, 4.0)
        else:
            relax(f1, r1, rhs1[1], s1, n1, k, False, 4.0)

    mail0.wait()
    grow0 = jnp.where(
        iota((LANES, 2 * LANES), 0) == (left + iota((LANES, 2 * LANES), 1) // 2) % LANES, 1.0, 0.0
    )
    half0 = rows0 // 2
    first, length = span(n0, 2)
    chess_h = evens(half0, LANES)
    tops = []
    for j in range(length):
        index = (first - c + j - j % 2) // 2 + c if gx <= 2 else (first - c + j) // 2 + c
        red, black = r1[index, 0, PAD:PAD + half0], f1[index, 0, PAD:PAD + half0]
        tops.append(plane(red, black, chess_h, j % 2))
    v = dot(jnp.concatenate(tops, axis=0), grow0)
    for j in range(length):
        for g in range(2):
            base = (2 * j + g) * rows0
            part = v[j * half0:(j + 1) * half0, LANES * g:LANES * (g + 1)]
            w0[pl.ds(base, half0, stride=2), :] = part
            w0[pl.ds(base + 1, half0, stride=2), :] = part

    for i in range(n0):
        at = c + i
        j = at - first
        lift = w0[pl.ds(pl.multiple_of(2 * j * rows0, 8) + TOP, ly), :]
        f0[at, 0, own] = black0[at, 0, own] + lift
        for rows in (slice(PAD, TOP), slice(TOP + ly, TOP + ly + 8)):
            lift = w0[pl.ds(pl.multiple_of(2 * j * rows0, 8) + rows.start, 8), :]
            f0[at, 0, rows] = f0[at, 0, rows] + lift
    for side in near:
        for k in (1, 2):
            at = side.landing(c, n0, k)
            j = at - first
            lift = w0[pl.ds(pl.multiple_of(2 * j * rows0, 8) + PAD, rows_h), :]
            f0[at, 0, PAD:PAD + rows_h] = f0[at, 0, PAD:PAD + rows_h] + lift
    for s, side in enumerate([None] + near):
        pairs = range(n0) if side is None else (1, 2)
        for k in pairs:
            if side is None:
                at, far = c + k, k
            else:
                at = side.landing(c, n0, k)
                far = None
            for n in range(groups0 + 2):
                which, group = (0, groups0 - 1) if n == 0 else ((2, 0) if n > groups0 else (1, n - 1))
                tiles = []
                for zi in range(2):
                    t = g_in[zi, s, which]
                    if far is not None:
                        lo = COR0 * (group * n0 + far)
                        tiles.append(turn(t, (LANES - COR0 if zi == 0 else 0) - lo))
                    elif side.dynamic:
                        spot = (LANES - COR0 if zi == 0 else 0)
                        a = turn(t, spot - COR0 * (group * n0 + k - 1))
                        b = turn(t, spot - COR0 * (group * n0 + n0 - k))
                        tiles.append(jnp.where(side.up, a, b))
                    else:
                        far_at = n0 - k if side.up else k - 1
                        tiles.append(turn(t, (LANES - COR0 if zi == 0 else 0) - COR0 * (group * n0 + far_at)))
                low, high = tiles
                value = jnp.where(lane8 >= LANES - COR0, low, jnp.where(lane8 < COR0, high, 0.0))
                j = at - first
                to_rows = slice(PAD + 8 * n, PAD + 8 * n + 8)
                lift = w0[pl.ds(pl.multiple_of((2 * j + 1) * rows0, 8) + PAD + 8 * n, 8), :]
                f0[at, 1, to_rows] = value + lift

    relax(r0, f0, rhs0[0], s0, n0, 2, True, 1.0)
    relax(f0, r0, rhs0[1], s0, n0, 1, False, 1.0)
    relax(r0, f0, rhs0[0], s0, n0, 1, True, 1.0)

    def emit(j, red, black):
        out_ref[2 * j] = jnp.where(even, red, black)
        out_ref[2 * j + 1] = jnp.where(even, black, red)

    relax(None, r0, rhs0[1], s0, n0, 0, False, 1.0, tiles=1, emit=emit)


def local(sizes, right_side, start):
    gx, gy, gz = sizes
    lx, ly, lz = start.shape
    f32 = jnp.float32
    count = gx * gy * gz
    near = {1: 0, 2: 1}.get(gx, 2)
    far = {1: 0, 2: 1}.get(gx, 4)
    n0, n1 = lx // 2, lx // 4
    m0, m1 = n0 + 2 * HALO, n1 + 2 * HALO
    r0, r1 = ly + 2 * TOP, ly // 2 + 2 * TOP
    hy = ly // 2
    y2, z2 = gy * ly // 4, gz * lz // 4
    p2, p3 = gx * lx // 8, gx * lx // 16
    y3, z3 = y2 // 2, z2 // 2
    z3p = -(-z3 // LANES) * LANES
    dx = min(gx - 1, -(-REACH2 // (lx // 4)))
    dy = min(gy - 1, -(-REACH2 // (ly // 4)))
    dz = min(gz - 1, -(-REACH2 // (lz // 4)))
    rounds = max(2, sum(max(0, d - 2) for d in (dx, dy, dz)) - 1)
    near_a, far_a = max(near, 1), max(far, 1)

    def vmem(*shape):
        return pltpu.VMEM(shape, f32)

    messages = 24 if gx <= 2 else 48
    return pl.pallas_call(
        functools.partial(kernel, sizes),
        out_shape=jax.ShapeDtypeStruct(start.shape, f32),
        in_specs=[pl.BlockSpec(memory_space=pl.ANY)] * 2,
        out_specs=pl.BlockSpec(memory_space=pltpu.VMEM),
        scratch_shapes=[
            vmem(lx, ly, lz),
            vmem(lx, ly, lz),
            vmem(3, m0, 2, r0, LANES),
            vmem(m0, 2, r0, LANES),
            vmem(m0, 2, r0, LANES),
            vmem(2, r0 - 2 * PAD, LANES),
            vmem(near_a, ly, LANES),
            vmem(near_a, ly, LANES),
            vmem(2, ly, LANES),
            vmem(2, ly + 16, LANES),
            vmem(near_a, 2, 8, LANES),
            vmem(near_a, 2, 3, 8, LANES),
            vmem(near_a, 2, 16, LANES),
            vmem(near_a, 2, 16, LANES),
            vmem(2, m1, 1, r1, LANES),
            vmem(m1, 1, r1, LANES),
            vmem(m1, 1, r1, LANES),
            vmem(m1, 1, r1, LANES),
            vmem(1, r1 - 2 * PAD, LANES),
            vmem(2 * m0 * r0, LANES),
            vmem(m1, r1, LANES),
            vmem(n1, hy, LANES),
            vmem(far_a, n1, hy, LANES),
            vmem(2, n1, 8, LANES),
            vmem(far_a, 2, n1, 8, LANES),
            vmem(2, 8, LANES),
            vmem(2, far + 1, 3, 8, LANES),
            vmem(1, hy, LANES),
            vmem(far_a, 1, hy, LANES),
            vmem(2, 1, 8, LANES),
            vmem(far_a, 2, 1, 8, LANES),
            vmem(2, 8, LANES),
            vmem(2, far + 1, 3, 8, LANES),
            vmem(2, 8, LANES),
            vmem(2, near + 1, 3, 8, LANES),
            vmem(p2 + 2, y2 + 2 * PAD, z2),
            vmem(p2 + 2, y2 + 2 * PAD, z2),
            vmem(p2 + 2, y2 + 2 * PAD, z2),
            vmem(p2 + 2, y2 + 2 * PAD, z2),
            vmem(8, LANES),
            vmem(count, 8, LANES),
            vmem(p2, z2 // LANES, y2, LANES),
            vmem(p3 + 2, y3 + 2 * PAD, z3p),
            vmem(p3 + 2, y3 + 2 * PAD, z3p),
            vmem(p3 + 2, y3 + 2 * PAD, z3p),
            vmem(p3 + 2, y3 + 2 * PAD, z3p),
            pltpu.SemaphoreType.DMA((2,)),
            pltpu.SemaphoreType.REGULAR((rounds,)),
            pltpu.SemaphoreType.DMA((4, 2, messages)),
            pltpu.SemaphoreType.DMA((2, count)),
        ],
        compiler_params=pltpu.CompilerParams(
            collective_id=0, has_side_effects=True, vmem_limit_bytes=GRANT
        ),
    )(right_side, start)


def solution(mesh):
    sizes = (mesh.shape["gx"], mesh.shape["gy"], mesh.shape["gz"])
    spec = P("gx", "gy", "gz")
    return jax.shard_map(
        functools.partial(local, sizes), mesh=mesh, in_specs=(spec, spec), out_specs=spec, check_vma=False
    )
```

```python
import functools

import jax
import jax.numpy as jnp
from jax import lax
from jax.experimental import pallas as pl
from jax.experimental.pallas import tpu as pltpu
from jax.sharding import PartitionSpec as P

MESH = pl.DeviceIdType.MESH
SIXTH = 1.0 / 6.0
PAD = 8
TOP = 16
LANES = 128
HALO = 3
CSWEEPS = 8
REACH2 = 42
EDGE = ((0, 1, 4), (0, 2, 2), (1, 1, 3), (1, 2, 1), (2, 1, 2))
FACE = 5
RHS1 = 5
COR1 = 6
COR0 = 4
GRANT = 56150000


def dot(a, b):
    high = a.astype(jnp.bfloat16)
    rest = a - high.astype(jnp.float32)
    middle = rest.astype(jnp.bfloat16)
    low = (rest - middle.astype(jnp.float32)).astype(jnp.bfloat16)
    b = b.astype(jnp.bfloat16)
    return jnp.dot(
        jnp.concatenate([high, middle, low], axis=1),
        jnp.concatenate([b, b, b], axis=0),
        preferred_element_type=jnp.float32,
    )


def iota(shape, axis):
    return lax.broadcasted_iota(jnp.int32, shape, axis)


def turn(v, shift):
    shift %= v.shape[1]
    return pltpu.roll(v, shift, axis=1) if shift else v


def evens(rows, lanes, add=0):
    shape = (rows // 8, 8, lanes)
    return ((iota(shape, 1) + iota(shape, 2) + add) & 1).reshape(rows, lanes) == 0


def both(*terms):
    out = True
    for term in terms:
        if term is True:
            continue
        out = term if out is True else out & term
    return out


def when(condition, action):
    if condition is True:
        action()
    else:
        pl.when(condition)(action)


class Side:
    def __init__(self, hop, up, send, recv, peer):
        self.hop, self.up, self.send, self.recv, self.peer = hop, up, send, recv, peer
        self.dynamic = not isinstance(up, bool)

    def pick(self, a, b):
        if self.dynamic:
            return jnp.where(self.up, a, b)
        return a if self.up else b

    def source(self, c, n, count):
        return self.pick(c + n - count, c)

    def target(self, c, n, count):
        return self.pick(c - count, c + n)

    def landing(self, c, n, k):
        if self.dynamic:
            return jnp.where(self.up, c + n + k - 1, c - k)
        return c - k if self.up else c + n + k - 1

    def outward(self, c, n, k):
        return self.pick(c + n - k, c + k - 1)

    def base(self, c, n):
        if self.dynamic:
            return jnp.where(self.up, c + n, c - n)
        return c - self.hop * n if self.up else c + self.hop * n

    def send_shift(self):
        return self.pick(0, 1)

    def recv_shift(self):
        return jnp.where(self.up, 1, 0) if self.dynamic else (0 if self.up else 1)


class Mail:
    def __init__(self, sems):
        self.sems, self.count, self.items = sems, 0, []

    def add(self, src, dst, send, recv, peer, tag=None):
        at = self.count
        self.count += 1
        copy = pltpu.make_async_remote_copy(
            src_ref=src,
            dst_ref=dst,
            send_sem=self.sems.at[0, at],
            recv_sem=self.sems.at[1, at],
            device_id=peer,
            device_id_type=MESH,
        )
        self.items.append((tag, copy, send, recv))
        when(send, copy.start)

    def wait(self, tag=None):
        for item in list(self.items):
            name, copy, send, recv = item
            if tag is None or name == tag:
                when(send, copy.wait_send)
                when(recv, copy.wait_recv)
                self.items.remove(item)


def kernel(
    sizes, rhs_hbm, start_hbm, out_ref,
    rhs, start, a0, r0, f0, s0, merged_out, merged_in, zsend, zrecv, esend, erecv, yedge_out, yedge_in,
    a1, r1, b1, f1, s1, w0, w1, tiles_out, tiles_in, ysides, xysides, zout, zin,
    n_out, n_in, ny_in, nxy_in, nz_out, nz_in, g_out, g_in,
    b2r, b2b, r2, v2, pack, slots, w2, b3r, b3b, r3, v3,
    in_sems, relay, sems, gather_sems,
):
    gx, gy, gz = sizes
    count = gx * gy * gz
    mx, my, mz = lax.axis_index("gx"), lax.axis_index("gy"), lax.axis_index("gz")
    lx, ly, lz = start.shape
    n0, n1 = lx // 2, lx // 4
    hy, hz = ly // 2, lz // 2
    qy, qz = hy // 2, hz // 2
    left = (LANES - hz) // 2
    c = HALO
    y2, z2 = gy * qy, gz * qz
    p2, p3 = gx * lx // 8, gx * lx // 16
    y3, z3 = y2 // 2, z2 // 2
    z3p = r3.shape[2]
    groups0, groups1 = ly // 8, hy // 8

    copies = [
        pltpu.make_async_copy(start_hbm, start, in_sems.at[0]),
        pltpu.make_async_copy(rhs_hbm, rhs, in_sems.at[1]),
    ]
    for copy in copies:
        copy.start()

    if gx == 1:
        near, sides1 = [], []
    elif gx == 2:
        near = sides1 = [Side(1, mx == 0, True, True, 1 - mx)]
    else:
        def side(hop, up):
            if up:
                return Side(hop, True, mx + hop < gx, mx >= hop, mx + hop)
            return Side(hop, False, mx >= hop, mx + hop < gx, mx - hop)

        near = [side(1, True), side(1, False)]
        sides1 = near + [side(2, True), side(2, False)]

    def along(at, size, step):
        if step == 0:
            return True, True, at
        if step > 0:
            return at + 1 < size, at >= 1, at + 1
        return at >= 1, at + 1 < size, at - 1

    def to(side, dy, dz):
        sx, rx, px = (True, True, mx) if side is None else (side.send, side.recv, side.peer)
        sy, ry, py = along(my, gy, dy)
        sz, rz, pz = along(mz, gz, dz)
        return both(sx, sy, sz), both(rx, ry, rz), (px, py, pz)

    faces = [to(s, 0, 0) for s in near]
    faces += [to(None, d, 0) for d in (1, -1)] + [to(None, 0, d) for d in (1, -1)]

    def signal_faces(sem):
        for send, _, peer in faces:
            when(send, lambda peer=peer: pl.semaphore_signal(sem, inc=1, device_id=peer, device_id_type=MESH))

    heard = sum([(1 if recv is True else jnp.where(recv, 1, 0)) for _, recv, _ in faces])

    def clear(*refs):
        for ref in refs:
            ref[...] = jnp.zeros_like(ref)

    rows0 = a0.shape[3]
    own = slice(TOP, TOP + ly)
    outside = [i for i in range(a0.shape[1]) if i < c or i >= c + n0]
    clear(zrecv, erecv, yedge_in)
    for q in range(3):
        for i in range(c, c + n0):
            a0[q, i, 0, PAD:TOP] = jnp.zeros((PAD, LANES), jnp.float32)
            a0[q, i, 0, TOP + ly:TOP + ly + PAD] = jnp.zeros((PAD, LANES), jnp.float32)
        if gx != 2:
            for i in outside:
                a0[q, i, 0, own] = jnp.zeros((ly, LANES), jnp.float32)
    if gx != 2:
        clear(merged_in)
    barrier = pltpu.get_barrier_semaphore()
    signal_faces(barrier)
    clear(slots)

    def mask(shape, row0, lane_of, bounds):
        y = iota(shape, 0) + row0
        z = lane_of(iota(shape, 1))
        inside = (y >= 0) & (y < bounds[0]) & (z >= 0) & (z < bounds[1])
        return jnp.where(inside, SIXTH, 0.0)

    even = evens(ly, LANES)
    for copy in copies:
        copy.wait()
    for i in range(n0):
        a0[0, c + i, 0, own] = jnp.where(even, start[2 * i + 1], start[2 * i])
        a0[1, c + i, 0, own] = jnp.where(even, rhs[2 * i], rhs[2 * i + 1])
        a0[2, c + i, 0, own] = jnp.where(even, rhs[2 * i + 1], rhs[2 * i])
    for s, side in enumerate(near):
        third = a0[0, side.outward(c, n0, 3), 0, own]
        second = a0[2, side.outward(c, n0, 2), 0, own]
        merged_out[s] = jnp.where(evens(ly, LANES, side.send_shift()), third, pltpu.roll(second, 1, axis=0))

    pl.semaphore_wait(barrier, heard)

    lane64 = iota((ly, LANES), 1)
    lane8 = iota((8, LANES), 1)
    ydirs = zdirs = (1, -1)
    mail = Mail(sems.at[0])
    for s, side in enumerate(near):
        where = to(side, 0, 0)
        src, dst = side.source(c, n0, 2), side.target(c, n0, 2)
        mail.add(a0.at[0:2, pl.ds(src, 2), 0, own], a0.at[0:2, pl.ds(dst, 2), 0, own], *where)

    def strip(d, rows):
        return (TOP + rows - 8, TOP - 8) if d > 0 else (TOP, TOP + rows)

    for d in ydirs:
        src, dst = strip(d, ly)
        mail.add(
            a0.at[0:3, pl.ds(c, n0), 0, pl.ds(src, 8)],
            a0.at[0:3, pl.ds(c, n0), 0, pl.ds(dst, 8)],
            *to(None, d, 0), "z",
        )
    signal_faces(relay.at[0])
    clear(ysides, xysides, tiles_in, zin, n_in, ny_in, nxy_in, nz_in, g_in)

    slots0 = [(q, i) for i in range(n0) for q in range(3)]
    for zi, d in enumerate(zdirs):
        packed = jnp.zeros((ly, LANES), jnp.float32)
        for t, (q, i) in enumerate(slots0):
            v = a0[q, c + i, 0, own]
            first = lz - FACE if d > 0 else 0
            here = (lane64 >= FACE * t) & (lane64 < FACE * (t + 1))
            packed = jnp.where(here, turn(v, FACE * t - first), packed)
        zsend[zi] = packed
    for zi, d in enumerate(zdirs):
        mail.add(zsend.at[zi], zrecv.at[zi, pl.ds(8, ly)], *to(None, 0, d), "z")

    width = sum(w for _, _, w in EDGE)
    starts = [sum(w for _, _, w in EDGE[:t]) for t in range(len(EDGE))]
    for s, side in enumerate(near):
        for zi, d in enumerate(zdirs):
            packed = jnp.zeros((8, LANES), jnp.float32)
            for (q, k, w), at in zip(EDGE, starts):
                v = a0[q, side.outward(c, n0, k), 0, own]
                for g in range(groups0):
                    lo = width * g + at
                    first = lz - w if d > 0 else 0
                    here = (lane8 >= lo) & (lane8 < lo + w)
                    packed = jnp.where(here, turn(v[8 * g:8 * g + 8], lo - first), packed)
            esend[s, zi] = packed
        for yi, d in enumerate(ydirs):
            for (q, k, w), at in zip(EDGE, starts):
                first = TOP + ly - w if d > 0 else TOP
                yedge_out[s, yi, at:at + w] = a0[q, side.outward(c, n0, k), 0, first:first + w]
    pl.semaphore_wait(relay.at[0], heard)
    signal_faces(relay.at[1])
    for s, side in enumerate(near):
        for yi, d in enumerate(ydirs):
            mail.add(yedge_out.at[s, yi], yedge_in.at[s, yi], *to(side, d, 0), "y")
    for zi, dz in enumerate(zdirs):
        for d in ydirs:
            src, dst = strip(d, ly)
            mail.add(
                zsend.at[zi, pl.ds(src - TOP, 8)], zrecv.at[zi, pl.ds(dst - 8, 8)], *to(None, d, dz), "z"
            )
        for s, side in enumerate(near):
            mail.add(esend.at[s, zi], erecv.at[s, zi, 1], *to(side, 0, dz), "e")
    rounds = relay.shape[0]
    pl.semaphore_wait(relay.at[1], heard)
    for zi, dz in enumerate(zdirs):
        for s, side in enumerate(near):
            for d in ydirs:
                half = pl.ds(4 if d > 0 else 0, 4)
                mail.add(esend.at[s, zi, half], erecv.at[s, zi, 0 if d > 0 else 2, half], *to(side, d, dz), "e")
    for s, side in enumerate(near):
        where = to(side, 0, 0)
        src, dst = side.source(c, n0, 1), side.target(c, n0, 1)
        mail.add(a0.at[2, pl.ds(src, 1), 0, own], a0.at[2, pl.ds(dst, 1), 0, own], *where)
        mail.add(merged_out.at[s], merged_in.at[s], *where)
    for r in range(2, rounds):
        signal_faces(relay.at[r])
        pl.semaphore_wait(relay.at[r], heard)
    clear(r0, f0)
    for q in range(3):
        for i in range(a0.shape[1]):
            a0[q, i, 1] = jnp.zeros((rows0, LANES), jnp.float32)
            edge = PAD if c <= i < c + n0 else TOP
            a0[q, i, 0, 0:edge] = jnp.zeros((edge, LANES), jnp.float32)
            a0[q, i, 0, rows0 - edge:] = jnp.zeros((edge, LANES), jnp.float32)
    if gx == 2:
        for k in range(1, HALO + 1):
            a0[0, jnp.where(mx == 0, c - k, c + n0 + k - 1), 0, own] = jnp.zeros((ly, LANES), jnp.float32)
    fine = (gy * ly, gz * lz)
    s0[0] = mask(s0.shape[1:], my * ly - PAD, lambda k: mz * lz + k, fine)
    s0[1] = mask(s0.shape[1:], my * ly - PAD, lambda k: mz * lz + jnp.where(k < 64, k + lz, k - LANES), fine)
    s1[0] = mask(s1.shape[1:], my * hy - PAD, lambda k: mz * hz + k - left, (gy * hy, gz * hz))

    mail.wait("z")
    rows_h = ly + 16
    lane_h = iota((rows_h, LANES), 1)
    for t, (q, i) in enumerate(slots0):
        low = turn(zrecv[0], LANES - FACE - FACE * t)
        high = turn(zrecv[1], -FACE * t)
        a0[q, c + i, 1, PAD:PAD + rows_h] = jnp.where(
            lane_h >= LANES - FACE, low, jnp.where(lane_h < FACE, high, 0.0)
        )
    def span(n, k):
        if gx == 1:
            return c, n
        k = min(k, n * (gx - 1), HALO)
        if gx == 2:
            return jnp.where(mx == 0, c, c - k), n + k
        return c - k, n + 2 * k

    def inside(n, i):
        if gx <= 2:
            return None
        at = mx * n + i - c
        return jnp.where((at >= 0) & (at < gx * n), 1.0, 0.0)

    def neighbours(src, i, planes, red, chess, lo, hi, tiles):
        prev, cur, nxt = planes
        low = [turn(t, 1) for t in cur]
        high = [turn(t, -1) for t in cur]
        if len(cur) == 2:
            lane = iota(cur[0].shape, 1)
            low = [jnp.where(lane == 0, low[1 - g], low[g]) for g in range(tiles)]
            high = [jnp.where(lane == LANES - 1, high[1 - g], high[g]) for g in range(tiles)]
        out = []
        for g in range(tiles):
            beside = jnp.where(chess, prev[g], nxt[g]) if red else jnp.where(chess, nxt[g], prev[g])
            total = (cur[g] + beside) + (src[i, g, lo - 1:hi - 1] + src[i, g, lo + 1:hi + 1])
            out.append(total + (low[g] + high[g]))
        return out

    def relax(dst, src, rhs_of, scale, n, k, red, factor, tiles=None, emit=None, part=None):
        first, length = part or span(n, k)
        held = src.shape[1]
        rows = src.shape[2]
        lo, hi = (TOP, rows - TOP) if emit else (PAD, rows - PAD)
        tiles = tiles or held
        chess = evens(hi - lo, LANES)
        planes = [[src[first + j - 1, g, lo:hi] for g in range(held)] for j in range(length + 2)]
        for j in range(length):
            i = first + j
            totals = neighbours(src, i, planes[j:j + 3], red, chess, lo, hi, tiles)
            factor_x = inside(n, i)
            for g in range(tiles):
                b = rhs_of(i, g, lo, hi)
                if factor != 1.0:
                    b = b * factor
                value = (b + totals[g]) * scale[g, lo - PAD:hi - PAD]
                if factor_x is not None:
                    value = value * factor_x
                if emit:
                    emit(j, planes[j + 1][g], value)
                else:
                    dst[i, g, lo:hi] = value

    def residual(red_ref, black_ref, red_rhs, black_rhs, n, j, factor):
        rows = red_ref.shape[2]
        lo, hi = TOP, rows - TOP
        chess = evens(hi - lo, LANES)
        i = c + j
        held = red_ref.shape[1]

        def load(ref):
            return [[ref[i + d, g, lo:hi] for g in range(held if d == 0 else 1)] for d in (-1, 0, 1)]

        red, black = load(red_ref), load(black_ref)
        from_black = neighbours(black_ref, i, black, True, chess, lo, hi, 1)[0]
        from_red = neighbours(red_ref, i, red, False, chess, lo, hi, 1)[0]
        out = red_rhs(i, 0, lo, hi) - (6.0 * red[1][0] - from_black) * (1.0 / factor)
        return out + (black_rhs(i, 0, lo, hi) - (6.0 * black[1][0] - from_red) * (1.0 / factor))

    black0 = a0.at[0]
    rhs0 = [lambda i, g, lo, hi, q=q: a0[q, i, g, lo:hi] for q in (1, 2)]
    def sweep0(step, part):
        if step % 2 == 0:
            relax(r0, black0, rhs0[0], s0, n0, 0, True, 1.0, part=part)
        else:
            relax(black0, r0, rhs0[1], s0, n0, 0, False, 1.0, part=part)

    def early(step):
        return n0 - 1 - step if gx == 2 else 0

    for step in range(4):
        if early(step) > 0:
            sweep0(step, (jnp.where(mx == 0, c, c + n0 - early(step)), early(step)))
    mail.wait("e")
    for s, side in enumerate(near):
        for (q, k, w), at in zip(EDGE, starts):
            pair = side.landing(c, n0, k)
            for g in range(groups0 + 2):
                which, group = (0, groups0 - 1) if g == 0 else ((2, 0) if g > groups0 else (1, g - 1))
                lo = width * group + at
                low = turn(erecv[s, 0, which], LANES - w - lo)
                high = turn(erecv[s, 1, which], -lo)
                a0[q, pair, 1, PAD + 8 * g:PAD + 8 * g + 8] = jnp.where(
                    lane8 >= LANES - w, low, jnp.where(lane8 < w, high, 0.0)
                )

    mail.wait("y")
    for s, side in enumerate(near):
        for yi, d in enumerate(ydirs):
            for (q, k, w), at in zip(EDGE, starts):
                first = TOP - w if d > 0 else TOP + ly
                a0[q, side.landing(c, n0, k), 0, first:first + w] = yedge_in[s, yi, at:at + w]
    mail.wait()
    for s, side in enumerate(near):
        v = merged_in[s]
        a0[0, side.landing(c, n0, 3), 0, own] = v
        a0[2, side.landing(c, n0, 2), 0, own] = pltpu.roll(v, ly - 1, axis=0)
    for step in range(4):
        first, length = span(n0, (4 - step + 1) // 2)
        done = max(early(step), 0)
        if done:
            first = first + jnp.where(mx == 0, done, 0)
        sweep0(step, (first, length - done))
    for j in range(n0):
        w0[j * ly:(j + 1) * ly, :] = residual(r0, black0, rhs0[0], rhs0[1], n0, j, 1.0)
    r = w0[pl.ds(0, n0 * hy, stride=2), :] + w0[pl.ds(1, n0 * hy, stride=2), :]
    source, target = iota((LANES, LANES), 0), iota((LANES, LANES), 1)
    fold = jnp.where(lax.rem(target - left + LANES, hz) == source // 2, 0.125, 0.0)
    r = dot(r, fold)

    own1 = slice(TOP, TOP + hy)
    lane32 = iota((hy, LANES), 1)
    mid = (lane32 >= left) & (lane32 < left + hz)
    chess1 = evens(hy, LANES)
    for j in range(n1):
        one, two = r[2 * j * hy:(2 * j + 1) * hy], r[(2 * j + 1) * hy:(2 * j + 2) * hy]
        red = jnp.where(chess1, one, two)
        black = jnp.where(chess1, two, one)
        tiles_out[j] = jnp.where(mid, red, black)
        a1[0, c + j, 0, own1] = jnp.where(mid, red, 0.0)
        a1[1, c + j, 0, own1] = jnp.where(mid, black, 0.0)

    def pack_edges(read, items, w):
        for d in zdirs:
            first = left + hz - w if d > 0 else left
            packed = jnp.zeros((8, LANES), jnp.float32)
            for t in range(items * groups1):
                here = (lane8 >= w * t) & (lane8 < w * (t + 1))
                packed = jnp.where(here, turn(read(t), w * t - first), packed)
            yield packed

    def post1(mail, out, into, y_in, xy_in, z_out, z_in):
        for s, side in enumerate(sides1):
            mail.add(out, into.at[s], *to(side, 0, 0))
        for yi, d in enumerate(ydirs):
            src = hy - 8 if d > 0 else 0
            mail.add(out.at[:, pl.ds(src, 8)], y_in.at[yi], *to(None, d, 0))
        for s, side in enumerate(sides1):
            for yi, d in enumerate(ydirs):
                src = hy - 8 if d > 0 else 0
                mail.add(out.at[:, pl.ds(src, 8)], xy_in.at[s, yi], *to(side, d, 0))
        for zi, dz in enumerate(zdirs):
            for s, side in enumerate([None] + sides1):
                for yi, d in enumerate((1, 0, -1)):
                    mail.add(z_out.at[zi], z_in.at[zi, s, yi], *to(side, d, dz))

    def regions1():
        yield from ((None, None, j, c + j) for j in range(n1))
        for s, side in enumerate(sides1):
            for j in range(n1):
                at = side.base(c, n1) + j
                if side.dynamic or 0 <= at < 2 * c + n1:
                    yield (s, side, j, at)

    def row_groups():
        yield 0, groups1 - 1, None, 0
        for g in range(groups1):
            yield 1, g, g, None
        yield 2, 0, None, 1

    lane_l = lane8
    mid8 = (lane_l >= left) & (lane_l < left + hz)

    def edges(z_in, s, which, lo, w):
        at = 0 if s is None else s + 1
        low = turn(z_in[0, at, which], left - w - lo)
        high = turn(z_in[1, at, which], left + hz - lo)
        return jnp.where(lane_l < left, low, high)

    items = 2 * n1
    order1 = [(g, q, j) for g in range(groups1) for j in range(n1) for q in range(2)]
    tile_of = lambda t: a1[order1[t][1], c + order1[t][2], 0, TOP + 8 * order1[t][0]:TOP + 8 * order1[t][0] + 8]
    for zi, packed in enumerate(pack_edges(tile_of, items, RHS1)):
        zout[zi] = packed
    mail = Mail(sems.at[1])
    post1(mail, tiles_out, tiles_in, ysides, xysides, zout, zin)
    for ref in (a1, r1, b1, f1):
        for i in range(ref.shape[-4]):
            halo_pair = i < c or i >= c + n1
            lead = (slice(None),) if len(ref.shape) == 5 else ()
            if halo_pair or ref is not a1:
                at = lead + (i,)
                ref[at] = jnp.zeros(ref[at].shape, jnp.float32)
            else:
                for rows in (slice(0, TOP), slice(TOP + hy, None)):
                    at = lead + (i, slice(None), rows)
                    ref[at] = jnp.zeros(ref[at].shape, jnp.float32)
    for ref in (b2r, b2b, r2, v2, b3r, b3b, r3, v3):
        ref[...] = jnp.zeros_like(ref)
    mail.wait()

    near_lanes = (lane_l >= left - RHS1) & (lane_l < left + hz + RHS1)
    for s, side, j, at in regions1():
        for n, (which, group, rows, yi) in enumerate(row_groups()):
            if rows is None:
                base = ysides[yi, j] if s is None else xysides[s, yi, j]
            elif s is None:
                base = None
            else:
                base = tiles_in[s, j, 8 * rows:8 * rows + 8]
            for q in range(2):
                to_rows = slice(PAD + 8 * n, PAD + 8 * n + 8)
                lo = RHS1 * ((group * n1 + j) * 2 + q)
                if base is None:
                    middle = a1[q, at, 0, to_rows]
                else:
                    middle = base if q == 0 else turn(base, LANES - hz)
                outer = edges(zin, s, which, lo, RHS1)
                a1[q, at, 0, to_rows] = jnp.where(mid8, middle, jnp.where(near_lanes, outer, 0.0))

    rhs1 = [lambda i, g, lo, hi, q=q: a1[q, i, g, lo:hi] for q in (0, 1)]
    first, length = span(n1, 2)
    for j in range(length):
        i = first + j
        value = (a1[0, i, 0, PAD:-PAD] * 4.0) * s1[0]
        factor_x = inside(n1, i)
        r1[i, 0, PAD:-PAD] = value if factor_x is None else value * factor_x
    relax(b1, r1, rhs1[1], s1, n1, 2, False, 4.0)
    relax(r1, b1, rhs1[0], s1, n1, 1, True, 4.0)
    relax(b1, r1, rhs1[1], s1, n1, 1, False, 4.0)

    for j in range(n1):
        w1[j, 0:hy, :] = residual(r1, b1, rhs1[0], rhs1[1], n1, j, 4.0)
    r = jnp.concatenate(
        [w1[j, pl.ds(0, qy, stride=2), :] + w1[j, pl.ds(1, qy, stride=2), :] for j in range(n1)], axis=0
    )
    fold = jnp.where(
        (lax.rem(target, qz) == (source - left) // 2) & (source >= left) & (source < left + hz), 0.125, 0.0
    )
    r = dot(r, fold)
    block = lane8 // qz
    per_colour = qy // 8
    one = two = None
    for h in range(per_colour):
        p, q = r[8 * h:8 * h + 8], r[qy + 8 * h:qy + 8 * h + 8]
        here = lax.rem(block, per_colour) == h
        one = p if one is None else jnp.where(here, p, one)
        two = q if two is None else jnp.where(here, q, two)
    tile = jnp.where(evens(8, LANES) ^ (block >= per_colour), one, two)
    pack[...] = tile

    mine = (mx * gy + my) * gz + mz
    slots[mine] = tile

    dist = (-(-REACH2 // (lx // 4)), -(-REACH2 // qy), -(-REACH2 // qz))

    def coords(k):
        steps = (k // (gy * gz), k // gz % gy, k % gz)
        moved = [at + step for at, step in zip((mx, my, mz), steps)]
        at = tuple(jnp.where(v >= size, v - size, v) for v, size in zip(moved, sizes))
        close = True
        for a, b, size, reach in zip(at, (mx, my, mz), sizes, dist):
            if reach < size - 1:
                close = both(close, (a - b <= reach) & (b - a <= reach))
        return at, close

    def number(at):
        return (at[0] * gy + at[1]) * gz + at[2]

    def flipped(at, k):
        bit = 1
        while bit <= k:
            if k & bit:
                at = at + bit - 2 * bit * lax.rem(lax.div(at, bit), 2)
            bit *= 2
        return at

    def partners():
        own_at = (mx, my, mz)
        flips = [[flipped(at, k) for k in range(size)] for at, size in zip(own_at, sizes)]
        order = [(i, j, k) for i in range(gx) for j in range(gy) for k in range(gz)][1:]
        order.sort(key=lambda f: (-(f[0] + min(f[2], 2) + f[1] // 2), -f[1], f[2]))
        for f in order:
            at = tuple(flips[axis][k] for axis, k in enumerate(f))
            close = True
            for a, b, k, reach in zip(at, own_at, f, dist):
                if k > reach:
                    close = both(close, (a - b <= reach) & (b - a <= reach))
            yield at, close

    straight = count <= 64 and all(size & (size - 1) == 0 for size in sizes)

    def others(body):
        if straight:
            for place in partners():
                body(place)
        else:
            def step(k, carry):
                body(coords(k))
                return carry

            lax.fori_loop(1, count, step, 0)

    def gather(place, arriving):
        at, close = place
        d = number(at)
        return pltpu.make_async_remote_copy(
            src_ref=pack,
            dst_ref=slots.at[d if arriving else mine],
            send_sem=gather_sems.at[0, d],
            recv_sem=gather_sems.at[1, d if arriving else mine],
            device_id=at,
            device_id_type=MESH,
        ), close

    def gather_start(place):
        copy, close = gather(place, False)
        when(close, copy.start)

    def gather_wait(place):
        copy, close = gather(place, True)

        def done():
            copy.wait_send()
            copy.wait_recv()

        when(close, done)

    others(gather_start)

    red_out = jnp.where(mid, b1[c, 0, own1], turn(b1[c + n1 - 1, 0, own1], LANES - hz))
    n_out[0] = red_out
    order_n = [(g, j) for g in range(groups1) for j in range(n1)]
    tile_n = lambda t: b1[c + order_n[t][1], 0, TOP + 8 * order_n[t][0]:TOP + 8 * order_n[t][0] + 8]
    for zi, packed in enumerate(pack_edges(tile_n, n1, COR1)):
        nz_out[zi] = packed
    mail1 = Mail(sems.at[2])
    post1(mail1, n_out, n_in, ny_in, nxy_in, nz_out, nz_in)

    for zi, d in enumerate(zdirs):
        packed = jnp.zeros((8, LANES), jnp.float32)
        for i in range(n0):
            v = a0[0, c + i, 0, own]
            for g in range(groups0):
                lo = COR0 * (g * n0 + i)
                first = lz - COR0 if d > 0 else 0
                here = (lane8 >= lo) & (lane8 < lo + COR0)
                packed = jnp.where(here, turn(v[8 * g:8 * g + 8], lo - first), packed)
        g_out[zi] = packed
    mail0 = Mail(sems.at[3])
    for side in near:
        src, dst = side.source(c, n0, 2), side.target(c, n0, 2)
        mail0.add(black0.at[pl.ds(src, 2), 0, own], f0.at[pl.ds(dst, 2), 0, own], *to(side, 0, 0))
        for d in ydirs:
            ysrc, ydst = strip(d, ly)
            mail0.add(
                black0.at[pl.ds(src, 2), 0, pl.ds(ysrc, 8)], f0.at[pl.ds(dst, 2), 0, pl.ds(ydst, 8)], *to(side, d, 0)
            )
    for d in ydirs:
        ysrc, ydst = strip(d, ly)
        mail0.add(
            black0.at[pl.ds(c, n0), 0, pl.ds(ysrc, 8)], f0.at[pl.ds(c, n0), 0, pl.ds(ydst, 8)], *to(None, d, 0)
        )
    for zi, dz in enumerate(zdirs):
        for s, side in enumerate([None] + near):
            for yi, d in enumerate((1, 0, -1)):
                mail0.add(g_out.at[zi], g_in.at[zi, s, yi], *to(side, d, dz))

    others(gather_wait)

    per = LANES // qz
    for k in range(gx * gy):
        cx, cy = k // gy, k % gy
        for g in range(gz // per):
            parts = [slots[k * gz + g * per + q] for q in range(per)]
            for h in range(per_colour):
                for colour, ref in ((0, b2r), (1, b2b)):
                    at = colour * per_colour + h
                    v = None
                    for q in range(per):
                        moved = turn(parts[q], (q - at) * qz)
                        here = (lane8 >= q * qz) & (lane8 < (q + 1) * qz)
                        v = moved if v is None else jnp.where(here, moved, v)
                    ref[1 + cx, PAD + cy * qy + 8 * h:PAD + cy * qy + 8 * h + 8, LANES * g:LANES * (g + 1)] = v

    def coarse_total(src, i, red, rows, full):
        width_z = src.shape[2]
        lo, hi = PAD, PAD + rows
        v = src[i, lo:hi]
        low, high = turn(v, 1), turn(v, -1)
        lane = iota(v.shape, 1)
        if full:
            low = jnp.where(lane == 0, 0.0, low)
            high = jnp.where(lane == width_z - 1, 0.0, high)
        chess = evens(rows, width_z)
        prev, nxt = src[i - 1, lo:hi], src[i + 1, lo:hi]
        beside = jnp.where(chess, prev, nxt) if red else jnp.where(chess, nxt, prev)
        total = (v + beside) + (src[i, lo - 1:hi - 1] + src[i, lo + 1:hi + 1])
        return v, total + (low + high)

    def coarse(dst, src, b, pairs, red, factor, rows, scale, full):
        for i in range(1, pairs + 1):
            _, total = coarse_total(src, i, red, rows, full)
            dst[i, PAD:PAD + rows] = (b[i, PAD:PAD + rows] * factor + total) * scale

    def sweep(red, black, red_rhs, black_rhs, pairs, factor, rows, scale, full):
        width_z = black.shape[2]
        lo, hi = PAD, PAD + rows
        lane = iota((rows, width_z), 1)
        chess = evens(rows, width_z)

        def moved(v, k):
            out = turn(v, k)
            if full:
                out = jnp.where(lane < k, 0.0, out) if k > 0 else jnp.where(lane >= width_z + k, 0.0, out)
            return out

        here, before, after = scale
        beside_z = []
        for i in range(1, pairs + 1):
            v = black[i, lo:hi]
            beside = jnp.where(chess, black[i - 1, lo:hi], black[i + 1, lo:hi])
            rest = (red_rhs[i, lo:hi] * factor + (v + beside)) + (black[i, lo - 1:hi - 1] + black[i, lo + 1:hi + 1])
            red[i, lo:hi] = (rest + (moved(v, 1) + moved(v, -1))) * here
            low = (turn(rest, 1) + (moved(v, 2) + v)) * before
            high = (turn(rest, -1) + (v + moved(v, -2))) * after
            beside_z.append(low + high)
        for i in range(1, pairs + 1):
            v = red[i, lo:hi]
            beside = jnp.where(chess, red[i + 1, lo:hi], red[i - 1, lo:hi])
            total = (v + beside) + (red[i, lo - 1:hi - 1] + red[i, lo + 1:hi + 1])
            black[i, lo:hi] = (black_rhs[i, lo:hi] * factor + (total + beside_z[i - 1])) * here

    def scales(rows, width_z, cells):
        lane = iota((rows, width_z), 1)
        return tuple(
            jnp.where((lane - k >= 0) & (lane - k < cells), SIXTH, 0.0) if k or cells < width_z else SIXTH
            for k in (0, 1, -1)
        )

    in2 = slice(PAD, PAD + y2)
    scale2 = scales(y2, z2, z2)
    for i in range(1, p2 + 1):
        r2[i, in2] = (b2r[i, in2] * 16.0) * SIXTH
    coarse(v2, r2, b2b, p2, False, 16.0, y2, SIXTH, True)
    sweep(r2, v2, b2r, b2b, p2, 16.0, y2, scale2, True)

    fold = jnp.where(iota((z2, z3p), 1) == iota((z2, z3p), 0) // 2, 0.125, 0.0)
    parts = []
    for i in range(1, p2 + 1):
        red, from_black = r2[i, in2], coarse_total(v2, i, True, y2, True)[1]
        black, from_red = v2[i, in2], coarse_total(r2, i, False, y2, True)[1]
        r = b2r[i, in2] - (6.0 * red - from_black) * 0.0625
        r = r + (b2b[i, in2] - (6.0 * black - from_red) * 0.0625)
        for g in range(z2 // LANES):
            w2[i - 1, g, 0:y2] = r[:, LANES * g:LANES * (g + 1)]
        parts.append(
            jnp.concatenate(
                [
                    w2[i - 1, g, pl.ds(0, y3, stride=2), :] + w2[i - 1, g, pl.ds(1, y3, stride=2), :]
                    for g in range(z2 // LANES)
                ],
                axis=1,
            )
        )
    r = dot(jnp.concatenate(parts, axis=0), fold)
    chess3 = evens(y3, z3p)
    in3 = slice(PAD, PAD + y3)
    for j in range(p3):
        one, two = r[2 * j * y3:(2 * j + 1) * y3], r[(2 * j + 1) * y3:(2 * j + 2) * y3]
        b3r[1 + j, in3] = jnp.where(chess3, one, two)
        b3b[1 + j, in3] = jnp.where(chess3, two, one)

    full3 = z3 == z3p
    scale3 = scales(y3, z3p, z3)

    def sweep3(_, carry):
        sweep(r3, v3, b3r, b3b, p3, 64.0, y3, scale3, full3)
        return carry

    if p3 == 1:
        for _ in range(CSWEEPS):
            sweep3(0, 0)
    else:
        lax.fori_loop(0, CSWEEPS, sweep3, 0)

    def plane(red, black, chess, odd):
        return jnp.where(chess, black, red) if odd else jnp.where(chess, red, black)

    grow = jnp.where(iota((z3p, z2), 0) == iota((z3p, z2), 1) // 2, 1.0, 0.0)
    v = jnp.concatenate(
        [plane(r3[1 + i // 2, in3], v3[1 + i // 2, in3], chess3, i % 2) for i in range(p2)], axis=0
    )
    v = dot(v, grow)
    for i in range(p2):
        part = v[i * y3:(i + 1) * y3]
        for g in range(z2 // LANES):
            w2[i, g, pl.ds(0, y3, stride=2), :] = part[:, LANES * g:LANES * (g + 1)]
            w2[i, g, pl.ds(1, y3, stride=2), :] = part[:, LANES * g:LANES * (g + 1)]
    for i in range(p2):
        for g in range(z2 // LANES):
            lanes = slice(LANES * g, LANES * (g + 1))
            v2[1 + i, in2, lanes] = v2[1 + i, in2, lanes] + w2[i, g, 0:y2]
    for _ in range(2):
        sweep(r2, v2, b2r, b2b, p2, 16.0, y2, scale2, True)

    mail1.wait()
    grow1 = jnp.where(
        iota((z2, LANES), 0) == mz * qz + (iota((z2, LANES), 1) - left + 2 * LANES) // 2 - LANES, 1.0, 0.0
    )
    rows1 = f1.shape[2]
    half1 = rows1 // 2
    rows2 = pl.ds(pl.multiple_of(my * qy, 8), half1)
    chess2 = evens(half1, z2)
    first, length = span(n1, HALO)
    begin = first - c + mx * n1
    shift = 0 if gx <= 2 else 1
    first_even = begin - shift
    tops = []
    for j in range(length):
        at = j + shift
        index = (first_even + (at - at % 2)) // 2 + 1
        if gx > 2:
            index = jnp.clip(index, 0, p2 + 1)
        tops.append(plane(r2[index, rows2], v2[index, rows2], chess2, at % 2))
    v = dot(jnp.concatenate(tops, axis=0), grow1)
    for j in range(length):
        part = v[j * half1:(j + 1) * half1]
        w1[j, pl.ds(0, half1, stride=2), :] = part
        w1[j, pl.ds(1, half1, stride=2), :] = part

    near_lanes = (lane_l >= left - COR1) & (lane_l < left + hz + COR1)
    for s, side, j, at in regions1():
        for n, (which, group, rows, yi) in enumerate(row_groups()):
            to_rows = slice(PAD + 8 * n, PAD + 8 * n + 8)
            if rows is None:
                base = ny_in[yi, 0] if s is None else nxy_in[s, yi, 0]
            elif s is None:
                base = None
            else:
                base = n_in[s, 0, 8 * rows:8 * rows + 8]
            if base is None:
                middle = b1[at, 0, to_rows]
            else:
                middle = base if j == 0 else turn(base, LANES - hz)
            outer = edges(nz_in, s, which, COR1 * (group * n1 + j), COR1)
            value = jnp.where(mid8, middle, jnp.where(near_lanes, outer, 0.0))
            f1[at, 0, to_rows] = value + w1[at - first, to_rows, :]

    for step in range(4):
        k = (5 - step + 1) // 2
        if step % 2 == 0:
            relax(r1, f1, rhs1[0], s1, n1, k, True, 4.0)
        else:
            relax(f1, r1, rhs1[1], s1, n1, k, False, 4.0)

    mail0.wait()
    grow0 = jnp.where(
        iota((LANES, 2 * LANES), 0) == (left + iota((LANES, 2 * LANES), 1) // 2) % LANES, 1.0, 0.0
    )
    half0 = rows0 // 2
    first, length = span(n0, 2)
    chess_h = evens(half0, LANES)
    tops = []
    for j in range(length):
        index = (first - c + j - j % 2) // 2 + c if gx <= 2 else (first - c + j) // 2 + c
        red, black = r1[index, 0, PAD:PAD + half0], f1[index, 0, PAD:PAD + half0]
        tops.append(plane(red, black, chess_h, j % 2))
    v = dot(jnp.concatenate(tops, axis=0), grow0)
    for j in range(length):
        for g in range(2):
            base = (2 * j + g) * rows0
            part = v[j * half0:(j + 1) * half0, LANES * g:LANES * (g + 1)]
            w0[pl.ds(base, half0, stride=2), :] = part
            w0[pl.ds(base + 1, half0, stride=2), :] = part

    for i in range(n0):
        at = c + i
        j = at - first
        lift = w0[pl.ds(pl.multiple_of(2 * j * rows0, 8) + TOP, ly), :]
        f0[at, 0, own] = black0[at, 0, own] + lift
        for rows in (slice(PAD, TOP), slice(TOP + ly, TOP + ly + 8)):
            lift = w0[pl.ds(pl.multiple_of(2 * j * rows0, 8) + rows.start, 8), :]
            f0[at, 0, rows] = f0[at, 0, rows] + lift
    for side in near:
        for k in (1, 2):
            at = side.landing(c, n0, k)
            j = at - first
            lift = w0[pl.ds(pl.multiple_of(2 * j * rows0, 8) + PAD, rows_h), :]
            f0[at, 0, PAD:PAD + rows_h] = f0[at, 0, PAD:PAD + rows_h] + lift
    for s, side in enumerate([None] + near):
        pairs = range(n0) if side is None else (1, 2)
        for k in pairs:
            if side is None:
                at, far = c + k, k
            else:
                at = side.landing(c, n0, k)
                far = None
            for n in range(groups0 + 2):
                which, group = (0, groups0 - 1) if n == 0 else ((2, 0) if n > groups0 else (1, n - 1))
                tiles = []
                for zi in range(2):
                    t = g_in[zi, s, which]
                    if far is not None:
                        lo = COR0 * (group * n0 + far)
                        tiles.append(turn(t, (LANES - COR0 if zi == 0 else 0) - lo))
                    elif side.dynamic:
                        spot = (LANES - COR0 if zi == 0 else 0)
                        a = turn(t, spot - COR0 * (group * n0 + k - 1))
                        b = turn(t, spot - COR0 * (group * n0 + n0 - k))
                        tiles.append(jnp.where(side.up, a, b))
                    else:
                        far_at = n0 - k if side.up else k - 1
                        tiles.append(turn(t, (LANES - COR0 if zi == 0 else 0) - COR0 * (group * n0 + far_at)))
                low, high = tiles
                value = jnp.where(lane8 >= LANES - COR0, low, jnp.where(lane8 < COR0, high, 0.0))
                j = at - first
                to_rows = slice(PAD + 8 * n, PAD + 8 * n + 8)
                lift = w0[pl.ds(pl.multiple_of((2 * j + 1) * rows0, 8) + PAD + 8 * n, 8), :]
                f0[at, 1, to_rows] = value + lift

    relax(r0, f0, rhs0[0], s0, n0, 2, True, 1.0)
    relax(f0, r0, rhs0[1], s0, n0, 1, False, 1.0)
    relax(r0, f0, rhs0[0], s0, n0, 1, True, 1.0)

    def emit(j, red, black):
        out_ref[2 * j] = jnp.where(even, red, black)
        out_ref[2 * j + 1] = jnp.where(even, black, red)

    relax(None, r0, rhs0[1], s0, n0, 0, False, 1.0, tiles=1, emit=emit)


def local(sizes, right_side, start):
    gx, gy, gz = sizes
    lx, ly, lz = start.shape
    f32 = jnp.float32
    count = gx * gy * gz
    near = {1: 0, 2: 1}.get(gx, 2)
    far = {1: 0, 2: 1}.get(gx, 4)
    n0, n1 = lx // 2, lx // 4
    m0, m1 = n0 + 2 * HALO, n1 + 2 * HALO
    r0, r1 = ly + 2 * TOP, ly // 2 + 2 * TOP
    hy = ly // 2
    y2, z2 = gy * ly // 4, gz * lz // 4
    p2, p3 = gx * lx // 8, gx * lx // 16
    y3, z3 = y2 // 2, z2 // 2
    z3p = -(-z3 // LANES) * LANES
    dx = min(gx - 1, -(-REACH2 // (lx // 4)))
    dy = min(gy - 1, -(-REACH2 // (ly // 4)))
    dz = min(gz - 1, -(-REACH2 // (lz // 4)))
    rounds = max(2, sum(max(0, d - 2) for d in (dx, dy, dz)) - 1)
    near_a, far_a = max(near, 1), max(far, 1)

    def vmem(*shape):
        return pltpu.VMEM(shape, f32)

    messages = 24 if gx <= 2 else 48
    return pl.pallas_call(
        functools.partial(kernel, sizes),
        out_shape=jax.ShapeDtypeStruct(start.shape, f32),
        in_specs=[pl.BlockSpec(memory_space=pl.ANY)] * 2,
        out_specs=pl.BlockSpec(memory_space=pltpu.VMEM),
        scratch_shapes=[
            vmem(lx, ly, lz),
            vmem(lx, ly, lz),
            vmem(3, m0, 2, r0, LANES),
            vmem(m0, 2, r0, LANES),
            vmem(m0, 2, r0, LANES),
            vmem(2, r0 - 2 * PAD, LANES),
            vmem(near_a, ly, LANES),
            vmem(near_a, ly, LANES),
            vmem(2, ly, LANES),
            vmem(2, ly + 16, LANES),
            vmem(near_a, 2, 8, LANES),
            vmem(near_a, 2, 3, 8, LANES),
            vmem(near_a, 2, 16, LANES),
            vmem(near_a, 2, 16, LANES),
            vmem(2, m1, 1, r1, LANES),
            vmem(m1, 1, r1, LANES),
            vmem(m1, 1, r1, LANES),
            vmem(m1, 1, r1, LANES),
            vmem(1, r1 - 2 * PAD, LANES),
            vmem(2 * m0 * r0, LANES),
            vmem(m1, r1, LANES),
            vmem(n1, hy, LANES),
            vmem(far_a, n1, hy, LANES),
            vmem(2, n1, 8, LANES),
            vmem(far_a, 2, n1, 8, LANES),
            vmem(2, 8, LANES),
            vmem(2, far + 1, 3, 8, LANES),
            vmem(1, hy, LANES),
            vmem(far_a, 1, hy, LANES),
            vmem(2, 1, 8, LANES),
            vmem(far_a, 2, 1, 8, LANES),
            vmem(2, 8, LANES),
            vmem(2, far + 1, 3, 8, LANES),
            vmem(2, 8, LANES),
            vmem(2, near + 1, 3, 8, LANES),
            vmem(p2 + 2, y2 + 2 * PAD, z2),
            vmem(p2 + 2, y2 + 2 * PAD, z2),
            vmem(p2 + 2, y2 + 2 * PAD, z2),
            vmem(p2 + 2, y2 + 2 * PAD, z2),
            vmem(8, LANES),
            vmem(count, 8, LANES),
            vmem(p2, z2 // LANES, y2, LANES),
            vmem(p3 + 2, y3 + 2 * PAD, z3p),
            vmem(p3 + 2, y3 + 2 * PAD, z3p),
            vmem(p3 + 2, y3 + 2 * PAD, z3p),
            vmem(p3 + 2, y3 + 2 * PAD, z3p),
            pltpu.SemaphoreType.DMA((2,)),
            pltpu.SemaphoreType.REGULAR((rounds,)),
            pltpu.SemaphoreType.DMA((4, 2, messages)),
            pltpu.SemaphoreType.DMA((2, count)),
        ],
        compiler_params=pltpu.CompilerParams(
            collective_id=0, has_side_effects=True, vmem_limit_bytes=GRANT
        ),
    )(right_side, start)


def solution(mesh):
    sizes = (mesh.shape["gx"], mesh.shape["gy"], mesh.shape["gz"])
    spec = P("gx", "gy", "gz")
    return jax.shard_map(
        functools.partial(local, sizes), mesh=mesh, in_specs=(spec, spec), out_specs=spec, check_vma=False
    )
```

```python
import functools

import jax
import jax.numpy as jnp
from jax import lax
from jax.experimental import pallas as pl
from jax.experimental.pallas import tpu as pltpu
from jax.sharding import PartitionSpec as P

MESH = pl.DeviceIdType.MESH
SIXTH = 1.0 / 6.0
PAD = 8
TOP = 16
LANES = 128
HALO = 3
CSWEEPS = 8
REACH2 = 42
EDGE = ((0, 1, 4), (0, 2, 2), (1, 1, 3), (1, 2, 1), (2, 1, 2))
FACE = 5
RHS1 = 5
COR1 = 6
COR0 = 4
GRANT = 56150000


def dot(a, b):
    high = a.astype(jnp.bfloat16)
    rest = a - high.astype(jnp.float32)
    middle = rest.astype(jnp.bfloat16)
    low = (rest - middle.astype(jnp.float32)).astype(jnp.bfloat16)
    b = b.astype(jnp.bfloat16)
    return jnp.dot(
        jnp.concatenate([high, middle, low], axis=1),
        jnp.concatenate([b, b, b], axis=0),
        preferred_element_type=jnp.float32,
    )


def iota(shape, axis):
    return lax.broadcasted_iota(jnp.int32, shape, axis)


def turn(v, shift):
    shift %= v.shape[1]
    return pltpu.roll(v, shift, axis=1) if shift else v


def evens(rows, lanes, add=0):
    shape = (rows // 8, 8, lanes)
    return ((iota(shape, 1) + iota(shape, 2) + add) & 1).reshape(rows, lanes) == 0


def both(*terms):
    out = True
    for term in terms:
        if term is True:
            continue
        out = term if out is True else out & term
    return out


def when(condition, action):
    if condition is True:
        action()
    else:
        pl.when(condition)(action)


class Side:
    def __init__(self, hop, up, send, recv, peer):
        self.hop, self.up, self.send, self.recv, self.peer = hop, up, send, recv, peer
        self.dynamic = not isinstance(up, bool)

    def pick(self, a, b):
        if self.dynamic:
            return jnp.where(self.up, a, b)
        return a if self.up else b

    def source(self, c, n, count):
        return self.pick(c + n - count, c)

    def target(self, c, n, count):
        return self.pick(c - count, c + n)

    def landing(self, c, n, k):
        if self.dynamic:
            return jnp.where(self.up, c + n + k - 1, c - k)
        return c - k if self.up else c + n + k - 1

    def outward(self, c, n, k):
        return self.pick(c + n - k, c + k - 1)

    def base(self, c, n):
        if self.dynamic:
            return jnp.where(self.up, c + n, c - n)
        return c - self.hop * n if self.up else c + self.hop * n

    def send_shift(self):
        return self.pick(0, 1)

    def recv_shift(self):
        return jnp.where(self.up, 1, 0) if self.dynamic else (0 if self.up else 1)


class Mail:
    def __init__(self, sems):
        self.sems, self.count, self.items = sems, 0, []

    def add(self, src, dst, send, recv, peer, tag=None):
        at = self.count
        self.count += 1
        copy = pltpu.make_async_remote_copy(
            src_ref=src,
            dst_ref=dst,
            send_sem=self.sems.at[0, at],
            recv_sem=self.sems.at[1, at],
            device_id=peer,
            device_id_type=MESH,
        )
        self.items.append((tag, copy, send, recv))
        when(send, copy.start)

    def wait(self, tag=None):
        for item in list(self.items):
            name, copy, send, recv = item
            if tag is None or name == tag:
                when(send, copy.wait_send)
                when(recv, copy.wait_recv)
                self.items.remove(item)


def kernel(
    sizes, rhs_hbm, start_hbm, out_ref,
    rhs, start, a0, r0, f0, s0, merged_out, merged_in, zsend, zrecv, esend, erecv, yedge_out, yedge_in,
    a1, r1, b1, f1, s1, w0, w1, tiles_out, tiles_in, ysides, xysides, zout, zin,
    n_out, n_in, ny_in, nxy_in, nz_out, nz_in, g_out, g_in,
    b2r, b2b, r2, v2, pack, slots, w2, b3r, b3b, r3, v3,
    in_sems, relay, sems, gather_sems,
):
    gx, gy, gz = sizes
    count = gx * gy * gz
    mx, my, mz = lax.axis_index("gx"), lax.axis_index("gy"), lax.axis_index("gz")
    lx, ly, lz = start.shape
    n0, n1 = lx // 2, lx // 4
    hy, hz = ly // 2, lz // 2
    qy, qz = hy // 2, hz // 2
    left = (LANES - hz) // 2
    c = HALO
    y2, z2 = gy * qy, gz * qz
    p2, p3 = gx * lx // 8, gx * lx // 16
    y3, z3 = y2 // 2, z2 // 2
    z3p = r3.shape[2]
    groups0, groups1 = ly // 8, hy // 8

    copies = [
        pltpu.make_async_copy(start_hbm, start, in_sems.at[0]),
        pltpu.make_async_copy(rhs_hbm, rhs, in_sems.at[1]),
    ]
    for copy in copies:
        copy.start()

    if gx == 1:
        near, sides1 = [], []
    elif gx == 2:
        near = sides1 = [Side(1, mx == 0, True, True, 1 - mx)]
    else:
        def side(hop, up):
            if up:
                return Side(hop, True, mx + hop < gx, mx >= hop, mx + hop)
            return Side(hop, False, mx >= hop, mx + hop < gx, mx - hop)

        near = [side(1, True), side(1, False)]
        sides1 = near + [side(2, True), side(2, False)]

    def along(at, size, step):
        if step == 0:
            return True, True, at
        if step > 0:
            return at + 1 < size, at >= 1, at + 1
        return at >= 1, at + 1 < size, at - 1

    def to(side, dy, dz):
        sx, rx, px = (True, True, mx) if side is None else (side.send, side.recv, side.peer)
        sy, ry, py = along(my, gy, dy)
        sz, rz, pz = along(mz, gz, dz)
        return both(sx, sy, sz), both(rx, ry, rz), (px, py, pz)

    faces = [to(s, 0, 0) for s in near]
    faces += [to(None, d, 0) for d in (1, -1)] + [to(None, 0, d) for d in (1, -1)]

    def signal_faces(sem):
        for send, _, peer in faces:
            when(send, lambda peer=peer: pl.semaphore_signal(sem, inc=1, device_id=peer, device_id_type=MESH))

    heard = sum([(1 if recv is True else jnp.where(recv, 1, 0)) for _, recv, _ in faces])

    def clear(*refs):
        for ref in refs:
            ref[...] = jnp.zeros_like(ref)

    rows0 = a0.shape[3]
    own = slice(TOP, TOP + ly)
    outside = [i for i in range(a0.shape[1]) if i < c or i >= c + n0]
    clear(zrecv, erecv, yedge_in)
    for q in range(3):
        for i in range(c, c + n0):
            a0[q, i, 0, PAD:TOP] = jnp.zeros((PAD, LANES), jnp.float32)
            a0[q, i, 0, TOP + ly:TOP + ly + PAD] = jnp.zeros((PAD, LANES), jnp.float32)
        if gx != 2:
            for i in outside:
                a0[q, i, 0, own] = jnp.zeros((ly, LANES), jnp.float32)
    if gx != 2:
        clear(merged_in)
    barrier = pltpu.get_barrier_semaphore()
    signal_faces(barrier)
    clear(slots)

    def mask(shape, row0, lane_of, bounds):
        y = iota(shape, 0) + row0
        z = lane_of(iota(shape, 1))
        inside = (y >= 0) & (y < bounds[0]) & (z >= 0) & (z < bounds[1])
        return jnp.where(inside, SIXTH, 0.0)

    even = evens(ly, LANES)
    for copy in copies:
        copy.wait()
    for i in range(n0):
        a0[0, c + i, 0, own] = jnp.where(even, start[2 * i + 1], start[2 * i])
        a0[1, c + i, 0, own] = jnp.where(even, rhs[2 * i], rhs[2 * i + 1])
        a0[2, c + i, 0, own] = jnp.where(even, rhs[2 * i + 1], rhs[2 * i])
    for s, side in enumerate(near):
        third = a0[0, side.outward(c, n0, 3), 0, own]
        second = a0[2, side.outward(c, n0, 2), 0, own]
        merged_out[s] = jnp.where(evens(ly, LANES, side.send_shift()), third, pltpu.roll(second, 1, axis=0))

    pl.semaphore_wait(barrier, heard)

    lane64 = iota((ly, LANES), 1)
    lane8 = iota((8, LANES), 1)
    ydirs = zdirs = (1, -1)
    mail = Mail(sems.at[0])
    for s, side in enumerate(near):
        where = to(side, 0, 0)
        src, dst = side.source(c, n0, 2), side.target(c, n0, 2)
        mail.add(a0.at[0:2, pl.ds(src, 2), 0, own], a0.at[0:2, pl.ds(dst, 2), 0, own], *where)

    def strip(d, rows):
        return (TOP + rows - 8, TOP - 8) if d > 0 else (TOP, TOP + rows)

    for d in ydirs:
        src, dst = strip(d, ly)
        mail.add(
            a0.at[0:3, pl.ds(c, n0), 0, pl.ds(src, 8)],
            a0.at[0:3, pl.ds(c, n0), 0, pl.ds(dst, 8)],
            *to(None, d, 0), "z",
        )
    signal_faces(relay.at[0])
    clear(ysides, xysides, tiles_in, zin, n_in, ny_in, nxy_in, nz_in, g_in)

    slots0 = [(q, i) for i in range(n0) for q in range(3)]
    for zi, d in enumerate(zdirs):
        packed = jnp.zeros((ly, LANES), jnp.float32)
        for t, (q, i) in enumerate(slots0):
            v = a0[q, c + i, 0, own]
            first = lz - FACE if d > 0 else 0
            here = (lane64 >= FACE * t) & (lane64 < FACE * (t + 1))
            packed = jnp.where(here, turn(v, FACE * t - first), packed)
        zsend[zi] = packed
    for zi, d in enumerate(zdirs):
        mail.add(zsend.at[zi], zrecv.at[zi, pl.ds(8, ly)], *to(None, 0, d), "z")

    width = sum(w for _, _, w in EDGE)
    starts = [sum(w for _, _, w in EDGE[:t]) for t in range(len(EDGE))]
    for s, side in enumerate(near):
        for zi, d in enumerate(zdirs):
            packed = jnp.zeros((8, LANES), jnp.float32)
            for (q, k, w), at in zip(EDGE, starts):
                v = a0[q, side.outward(c, n0, k), 0, own]
                for g in range(groups0):
                    lo = width * g + at
                    first = lz - w if d > 0 else 0
                    here = (lane8 >= lo) & (lane8 < lo + w)
                    packed = jnp.where(here, turn(v[8 * g:8 * g + 8], lo - first), packed)
            esend[s, zi] = packed
        for yi, d in enumerate(ydirs):
            for (q, k, w), at in zip(EDGE, starts):
                first = TOP + ly - w if d > 0 else TOP
                yedge_out[s, yi, at:at + w] = a0[q, side.outward(c, n0, k), 0, first:first + w]
    pl.semaphore_wait(relay.at[0], heard)
    signal_faces(relay.at[1])
    for s, side in enumerate(near):
        for yi, d in enumerate(ydirs):
            mail.add(yedge_out.at[s, yi], yedge_in.at[s, yi], *to(side, d, 0), "y")
    for zi, dz in enumerate(zdirs):
        for d in ydirs:
            src, dst = strip(d, ly)
            mail.add(
                zsend.at[zi, pl.ds(src - TOP, 8)], zrecv.at[zi, pl.ds(dst - 8, 8)], *to(None, d, dz), "z"
            )
        for s, side in enumerate(near):
            mail.add(esend.at[s, zi], erecv.at[s, zi, 1], *to(side, 0, dz), "e")
    rounds = relay.shape[0]
    pl.semaphore_wait(relay.at[1], heard)
    for zi, dz in enumerate(zdirs):
        for s, side in enumerate(near):
            for d in ydirs:
                half = pl.ds(4 if d > 0 else 0, 4)
                mail.add(esend.at[s, zi, half], erecv.at[s, zi, 0 if d > 0 else 2, half], *to(side, d, dz), "e")
    for s, side in enumerate(near):
        where = to(side, 0, 0)
        src, dst = side.source(c, n0, 1), side.target(c, n0, 1)
        mail.add(a0.at[2, pl.ds(src, 1), 0, own], a0.at[2, pl.ds(dst, 1), 0, own], *where)
        mail.add(merged_out.at[s], merged_in.at[s], *where)
    for r in range(2, rounds):
        signal_faces(relay.at[r])
        pl.semaphore_wait(relay.at[r], heard)
    clear(r0, f0)
    for q in range(3):
        for i in range(a0.shape[1]):
            a0[q, i, 1] = jnp.zeros((rows0, LANES), jnp.float32)
            edge = PAD if c <= i < c + n0 else TOP
            a0[q, i, 0, 0:edge] = jnp.zeros((edge, LANES), jnp.float32)
            a0[q, i, 0, rows0 - edge:] = jnp.zeros((edge, LANES), jnp.float32)
    if gx == 2:
        for k in range(1, HALO + 1):
            a0[0, jnp.where(mx == 0, c - k, c + n0 + k - 1), 0, own] = jnp.zeros((ly, LANES), jnp.float32)
    fine = (gy * ly, gz * lz)
    s0[0] = mask(s0.shape[1:], my * ly - PAD, lambda k: mz * lz + k, fine)
    s0[1] = mask(s0.shape[1:], my * ly - PAD, lambda k: mz * lz + jnp.where(k < 64, k + lz, k - LANES), fine)
    s1[0] = mask(s1.shape[1:], my * hy - PAD, lambda k: mz * hz + k - left, (gy * hy, gz * hz))

    mail.wait("z")
    rows_h = ly + 16
    lane_h = iota((rows_h, LANES), 1)
    for t, (q, i) in enumerate(slots0):
        low = turn(zrecv[0], LANES - FACE - FACE * t)
        high = turn(zrecv[1], -FACE * t)
        a0[q, c + i, 1, PAD:PAD + rows_h] = jnp.where(
            lane_h >= LANES - FACE, low, jnp.where(lane_h < FACE, high, 0.0)
        )
    def span(n, k):
        if gx == 1:
            return c, n
        k = min(k, n * (gx - 1), HALO)
        if gx == 2:
            return jnp.where(mx == 0, c, c - k), n + k
        return c - k, n + 2 * k

    def inside(n, i):
        if gx <= 2:
            return None
        at = mx * n + i - c
        return jnp.where((at >= 0) & (at < gx * n), 1.0, 0.0)

    def neighbours(src, i, planes, red, chess, lo, hi, tiles):
        prev, cur, nxt = planes
        low = [turn(t, 1) for t in cur]
        high = [turn(t, -1) for t in cur]
        if len(cur) == 2:
            lane = iota(cur[0].shape, 1)
            low = [jnp.where(lane == 0, low[1 - g], low[g]) for g in range(tiles)]
            high = [jnp.where(lane == LANES - 1, high[1 - g], high[g]) for g in range(tiles)]
        out = []
        for g in range(tiles):
            beside = jnp.where(chess, prev[g], nxt[g]) if red else jnp.where(chess, nxt[g], prev[g])
            total = (cur[g] + beside) + (src[i, g, lo - 1:hi - 1] + src[i, g, lo + 1:hi + 1])
            out.append(total + (low[g] + high[g]))
        return out

    def relax(dst, src, rhs_of, scale, n, k, red, factor, tiles=None, emit=None, part=None):
        first, length = part or span(n, k)
        held = src.shape[1]
        rows = src.shape[2]
        lo, hi = (TOP, rows - TOP) if emit else (PAD, rows - PAD)
        tiles = tiles or held
        chess = evens(hi - lo, LANES)
        planes = [[src[first + j - 1, g, lo:hi] for g in range(held)] for j in range(length + 2)]
        for j in range(length):
            i = first + j
            totals = neighbours(src, i, planes[j:j + 3], red, chess, lo, hi, tiles)
            factor_x = inside(n, i)
            for g in range(tiles):
                b = rhs_of(i, g, lo, hi)
                if factor != 1.0:
                    b = b * factor
                value = (b + totals[g]) * scale[g, lo - PAD:hi - PAD]
                if factor_x is not None:
                    value = value * factor_x
                if emit:
                    emit(j, planes[j + 1][g], value)
                else:
                    dst[i, g, lo:hi] = value

    def residual(red_ref, black_ref, red_rhs, black_rhs, n, j, factor):
        rows = red_ref.shape[2]
        lo, hi = TOP, rows - TOP
        chess = evens(hi - lo, LANES)
        i = c + j
        held = red_ref.shape[1]

        def load(ref):
            return [[ref[i + d, g, lo:hi] for g in range(held if d == 0 else 1)] for d in (-1, 0, 1)]

        red, black = load(red_ref), load(black_ref)
        from_black = neighbours(black_ref, i, black, True, chess, lo, hi, 1)[0]
        from_red = neighbours(red_ref, i, red, False, chess, lo, hi, 1)[0]
        out = red_rhs(i, 0, lo, hi) - (6.0 * red[1][0] - from_black) * (1.0 / factor)
        return out + (black_rhs(i, 0, lo, hi) - (6.0 * black[1][0] - from_red) * (1.0 / factor))

    black0 = a0.at[0]
    rhs0 = [lambda i, g, lo, hi, q=q: a0[q, i, g, lo:hi] for q in (1, 2)]
    def sweep0(step, part):
        if step % 2 == 0:
            relax(r0, black0, rhs0[0], s0, n0, 0, True, 1.0, part=part)
        else:
            relax(black0, r0, rhs0[1], s0, n0, 0, False, 1.0, part=part)

    def early(step):
        return n0 - 1 - step if gx == 2 else 0

    for step in range(4):
        if early(step) > 0:
            sweep0(step, (jnp.where(mx == 0, c, c + n0 - early(step)), early(step)))
    mail.wait("e")
    for s, side in enumerate(near):
        for (q, k, w), at in zip(EDGE, starts):
            pair = side.landing(c, n0, k)
            for g in range(groups0 + 2):
                which, group = (0, groups0 - 1) if g == 0 else ((2, 0) if g > groups0 else (1, g - 1))
                lo = width * group + at
                low = turn(erecv[s, 0, which], LANES - w - lo)
                high = turn(erecv[s, 1, which], -lo)
                a0[q, pair, 1, PAD + 8 * g:PAD + 8 * g + 8] = jnp.where(
                    lane8 >= LANES - w, low, jnp.where(lane8 < w, high, 0.0)
                )

    mail.wait("y")
    for s, side in enumerate(near):
        for yi, d in enumerate(ydirs):
            for (q, k, w), at in zip(EDGE, starts):
                first = TOP - w if d > 0 else TOP + ly
                a0[q, side.landing(c, n0, k), 0, first:first + w] = yedge_in[s, yi, at:at + w]
    mail.wait()
    for s, side in enumerate(near):
        v = merged_in[s]
        a0[0, side.landing(c, n0, 3), 0, own] = v
        a0[2, side.landing(c, n0, 2), 0, own] = pltpu.roll(v, ly - 1, axis=0)
    for step in range(4):
        first, length = span(n0, (4 - step + 1) // 2)
        done = max(early(step), 0)
        if done:
            first = first + jnp.where(mx == 0, done, 0)
        sweep0(step, (first, length - done))
    for j in range(n0):
        w0[j * ly:(j + 1) * ly, :] = residual(r0, black0, rhs0[0], rhs0[1], n0, j, 1.0)
    r = w0[pl.ds(0, n0 * hy, stride=2), :] + w0[pl.ds(1, n0 * hy, stride=2), :]
    source, target = iota((LANES, LANES), 0), iota((LANES, LANES), 1)
    fold = jnp.where(lax.rem(target - left + LANES, hz) == source // 2, 0.125, 0.0)
    r = dot(r, fold)

    own1 = slice(TOP, TOP + hy)
    lane32 = iota((hy, LANES), 1)
    mid = (lane32 >= left) & (lane32 < left + hz)
    chess1 = evens(hy, LANES)
    for j in range(n1):
        one, two = r[2 * j * hy:(2 * j + 1) * hy], r[(2 * j + 1) * hy:(2 * j + 2) * hy]
        red = jnp.where(chess1, one, two)
        black = jnp.where(chess1, two, one)
        tiles_out[j] = jnp.where(mid, red, black)
        a1[0, c + j, 0, own1] = jnp.where(mid, red, 0.0)
        a1[1, c + j, 0, own1] = jnp.where(mid, black, 0.0)

    def pack_edges(read, items, w):
        for d in zdirs:
            first = left + hz - w if d > 0 else left
            packed = jnp.zeros((8, LANES), jnp.float32)
            for t in range(items * groups1):
                here = (lane8 >= w * t) & (lane8 < w * (t + 1))
                packed = jnp.where(here, turn(read(t), w * t - first), packed)
            yield packed

    def post1(mail, out, into, y_in, xy_in, z_out, z_in, corner):
        far_first = list(enumerate([None] + sides1))[::-1]
        for steps in ((1, -1), (0,)):
            for s, side in far_first:
                for zi, dz in enumerate(zdirs):
                    for d in steps:
                        few = corner if d and side is not None else 8
                        rows = pl.ds(8 - few if d > 0 else 0, few)
                        mail.add(z_out.at[zi, rows], z_in.at[zi, s, 1 - d, rows], *to(side, d, dz))
        for s, side in enumerate(sides1):
            for yi, d in enumerate(ydirs):
                src = hy - 8 if d > 0 else 0
                mail.add(out.at[:, pl.ds(src, 8)], xy_in.at[s, yi], *to(side, d, 0))
        for s, side in enumerate(sides1):
            mail.add(out, into.at[s], *to(side, 0, 0))
        for yi, d in enumerate(ydirs):
            src = hy - 8 if d > 0 else 0
            mail.add(out.at[:, pl.ds(src, 8)], y_in.at[yi], *to(None, d, 0))

    def regions1():
        yield from ((None, None, j, c + j) for j in range(n1))
        for s, side in enumerate(sides1):
            for j in range(n1):
                at = side.base(c, n1) + j
                if side.dynamic or 0 <= at < 2 * c + n1:
                    yield (s, side, j, at)

    def row_groups():
        yield 0, groups1 - 1, None, 0
        for g in range(groups1):
            yield 1, g, g, None
        yield 2, 0, None, 1

    lane_l = lane8
    mid8 = (lane_l >= left) & (lane_l < left + hz)

    def edges(z_in, s, which, lo, w):
        at = 0 if s is None else s + 1
        low = turn(z_in[0, at, which], left - w - lo)
        high = turn(z_in[1, at, which], left + hz - lo)
        return jnp.where(lane_l < left, low, high)

    items = 2 * n1
    order1 = [(g, q, j) for g in range(groups1) for j in range(n1) for q in range(2)]
    tile_of = lambda t: a1[order1[t][1], c + order1[t][2], 0, TOP + 8 * order1[t][0]:TOP + 8 * order1[t][0] + 8]
    for zi, packed in enumerate(pack_edges(tile_of, items, RHS1)):
        zout[zi] = packed
    mail = Mail(sems.at[1])
    post1(mail, tiles_out, tiles_in, ysides, xysides, zout, zin, 4)
    for ref in (a1, r1, b1, f1):
        for i in range(ref.shape[-4]):
            halo_pair = i < c or i >= c + n1
            lead = (slice(None),) if len(ref.shape) == 5 else ()
            if halo_pair or ref is not a1:
                at = lead + (i,)
                ref[at] = jnp.zeros(ref[at].shape, jnp.float32)
            else:
                for rows in (slice(0, TOP), slice(TOP + hy, None)):
                    at = lead + (i, slice(None), rows)
                    ref[at] = jnp.zeros(ref[at].shape, jnp.float32)
    for ref in (b2r, b2b, r2, v2, b3r, b3b, r3, v3):
        ref[...] = jnp.zeros_like(ref)
    mail.wait()

    near_lanes = (lane_l >= left - RHS1) & (lane_l < left + hz + RHS1)
    for s, side, j, at in regions1():
        for n, (which, group, rows, yi) in enumerate(row_groups()):
            if rows is None:
                base = ysides[yi, j] if s is None else xysides[s, yi, j]
            elif s is None:
                base = None
            else:
                base = tiles_in[s, j, 8 * rows:8 * rows + 8]
            for q in range(2):
                to_rows = slice(PAD + 8 * n, PAD + 8 * n + 8)
                lo = RHS1 * ((group * n1 + j) * 2 + q)
                if base is None:
                    middle = a1[q, at, 0, to_rows]
                else:
                    middle = base if q == 0 else turn(base, LANES - hz)
                outer = edges(zin, s, which, lo, RHS1)
                a1[q, at, 0, to_rows] = jnp.where(mid8, middle, jnp.where(near_lanes, outer, 0.0))

    rhs1 = [lambda i, g, lo, hi, q=q: a1[q, i, g, lo:hi] for q in (0, 1)]
    first, length = span(n1, 2)
    for j in range(length):
        i = first + j
        value = (a1[0, i, 0, PAD:-PAD] * 4.0) * s1[0]
        factor_x = inside(n1, i)
        r1[i, 0, PAD:-PAD] = value if factor_x is None else value * factor_x
    relax(b1, r1, rhs1[1], s1, n1, 2, False, 4.0)
    relax(r1, b1, rhs1[0], s1, n1, 1, True, 4.0)
    relax(b1, r1, rhs1[1], s1, n1, 1, False, 4.0)

    for j in range(n1):
        w1[j, 0:hy, :] = residual(r1, b1, rhs1[0], rhs1[1], n1, j, 4.0)
    r = jnp.concatenate(
        [w1[j, pl.ds(0, qy, stride=2), :] + w1[j, pl.ds(1, qy, stride=2), :] for j in range(n1)], axis=0
    )
    fold = jnp.where(
        (lax.rem(target, qz) == (source - left) // 2) & (source >= left) & (source < left + hz), 0.125, 0.0
    )
    r = dot(r, fold)
    block = lane8 // qz
    per_colour = qy // 8
    one = two = None
    for h in range(per_colour):
        p, q = r[8 * h:8 * h + 8], r[qy + 8 * h:qy + 8 * h + 8]
        here = lax.rem(block, per_colour) == h
        one = p if one is None else jnp.where(here, p, one)
        two = q if two is None else jnp.where(here, q, two)
    tile = jnp.where(evens(8, LANES) ^ (block >= per_colour), one, two)
    pack[...] = tile

    mine = (mx * gy + my) * gz + mz
    slots[mine] = tile

    dist = (-(-REACH2 // (lx // 4)), -(-REACH2 // qy), -(-REACH2 // qz))

    def coords(k):
        steps = (k // (gy * gz), k // gz % gy, k % gz)
        moved = [at + step for at, step in zip((mx, my, mz), steps)]
        at = tuple(jnp.where(v >= size, v - size, v) for v, size in zip(moved, sizes))
        close = True
        for a, b, size, reach in zip(at, (mx, my, mz), sizes, dist):
            if reach < size - 1:
                close = both(close, (a - b <= reach) & (b - a <= reach))
        return at, close

    def number(at):
        return (at[0] * gy + at[1]) * gz + at[2]

    def flipped(at, k):
        bit = 1
        while bit <= k:
            if k & bit:
                at = at + bit - 2 * bit * lax.rem(lax.div(at, bit), 2)
            bit *= 2
        return at

    def partners():
        own_at = (mx, my, mz)
        flips = [[flipped(at, k) for k in range(size)] for at, size in zip(own_at, sizes)]
        order = [(i, j, k) for i in range(gx) for j in range(gy) for k in range(gz)][1:]
        order.sort(key=lambda f: (-f[0], -min(f[2], 2), -f[1]))
        for f in order:
            at = tuple(flips[axis][k] for axis, k in enumerate(f))
            close = True
            for a, b, k, reach in zip(at, own_at, f, dist):
                if k > reach:
                    close = both(close, (a - b <= reach) & (b - a <= reach))
            yield at, close

    straight = count <= 64 and all(size & (size - 1) == 0 for size in sizes)

    def others(body):
        if straight:
            for place in partners():
                body(place)
        else:
            def step(k, carry):
                body(coords(k))
                return carry

            lax.fori_loop(1, count, step, 0)

    def gather(place, arriving):
        at, close = place
        d = number(at)
        return pltpu.make_async_remote_copy(
            src_ref=pack,
            dst_ref=slots.at[d if arriving else mine],
            send_sem=gather_sems.at[0, d],
            recv_sem=gather_sems.at[1, d if arriving else mine],
            device_id=at,
            device_id_type=MESH,
        ), close

    def gather_start(place):
        copy, close = gather(place, False)
        when(close, copy.start)

    def gather_wait(place):
        copy, close = gather(place, True)

        def done():
            copy.wait_send()
            copy.wait_recv()

        when(close, done)

    others(gather_start)

    red_out = jnp.where(mid, b1[c, 0, own1], turn(b1[c + n1 - 1, 0, own1], LANES - hz))
    n_out[0] = red_out
    order_n = [(g, j) for g in range(groups1) for j in range(n1)]
    tile_n = lambda t: b1[c + order_n[t][1], 0, TOP + 8 * order_n[t][0]:TOP + 8 * order_n[t][0] + 8]
    for zi, packed in enumerate(pack_edges(tile_n, n1, COR1)):
        nz_out[zi] = packed
    mail1 = Mail(sems.at[2])
    post1(mail1, n_out, n_in, ny_in, nxy_in, nz_out, nz_in, 8)

    for zi, d in enumerate(zdirs):
        packed = jnp.zeros((8, LANES), jnp.float32)
        for i in range(n0):
            v = a0[0, c + i, 0, own]
            for g in range(groups0):
                lo = COR0 * (g * n0 + i)
                first = lz - COR0 if d > 0 else 0
                here = (lane8 >= lo) & (lane8 < lo + COR0)
                packed = jnp.where(here, turn(v[8 * g:8 * g + 8], lo - first), packed)
        g_out[zi] = packed
    mail0 = Mail(sems.at[3])
    for side in near:
        src, dst = side.source(c, n0, 2), side.target(c, n0, 2)
        mail0.add(black0.at[pl.ds(src, 2), 0, own], f0.at[pl.ds(dst, 2), 0, own], *to(side, 0, 0))
        for d in ydirs:
            ysrc, ydst = strip(d, ly)
            mail0.add(
                black0.at[pl.ds(src, 2), 0, pl.ds(ysrc, 8)], f0.at[pl.ds(dst, 2), 0, pl.ds(ydst, 8)], *to(side, d, 0)
            )
    for d in ydirs:
        ysrc, ydst = strip(d, ly)
        mail0.add(
            black0.at[pl.ds(c, n0), 0, pl.ds(ysrc, 8)], f0.at[pl.ds(c, n0), 0, pl.ds(ydst, 8)], *to(None, d, 0)
        )
    for zi, dz in enumerate(zdirs):
        for s, side in enumerate([None] + near):
            for yi, d in enumerate((1, 0, -1)):
                mail0.add(g_out.at[zi], g_in.at[zi, s, yi], *to(side, d, dz))

    others(gather_wait)

    per = LANES // qz
    for k in range(gx * gy):
        cx, cy = k // gy, k % gy
        for g in range(gz // per):
            parts = [slots[k * gz + g * per + q] for q in range(per)]
            for h in range(per_colour):
                for colour, ref in ((0, b2r), (1, b2b)):
                    at = colour * per_colour + h
                    v = None
                    for q in range(per):
                        moved = turn(parts[q], (q - at) * qz)
                        here = (lane8 >= q * qz) & (lane8 < (q + 1) * qz)
                        v = moved if v is None else jnp.where(here, moved, v)
                    ref[1 + cx, PAD + cy * qy + 8 * h:PAD + cy * qy + 8 * h + 8, LANES * g:LANES * (g + 1)] = v

    def coarse_total(src, i, red, rows, full):
        width_z = src.shape[2]
        lo, hi = PAD, PAD + rows
        v = src[i, lo:hi]
        low, high = turn(v, 1), turn(v, -1)
        lane = iota(v.shape, 1)
        if full:
            low = jnp.where(lane == 0, 0.0, low)
            high = jnp.where(lane == width_z - 1, 0.0, high)
        chess = evens(rows, width_z)
        prev, nxt = src[i - 1, lo:hi], src[i + 1, lo:hi]
        beside = jnp.where(chess, prev, nxt) if red else jnp.where(chess, nxt, prev)
        total = (v + beside) + (src[i, lo - 1:hi - 1] + src[i, lo + 1:hi + 1])
        return v, total + (low + high)

    def coarse(dst, src, b, pairs, red, factor, rows, scale, full):
        for i in range(1, pairs + 1):
            _, total = coarse_total(src, i, red, rows, full)
            dst[i, PAD:PAD + rows] = (b[i, PAD:PAD + rows] * factor + total) * scale

    def sweep(red, black, red_rhs, black_rhs, pairs, factor, rows, scale, full):
        width_z = black.shape[2]
        lo, hi = PAD, PAD + rows
        lane = iota((rows, width_z), 1)
        chess = evens(rows, width_z)

        def moved(v, k):
            out = turn(v, k)
            if full:
                out = jnp.where(lane < k, 0.0, out) if k > 0 else jnp.where(lane >= width_z + k, 0.0, out)
            return out

        here, before, after = scale
        beside_z = []
        for i in range(1, pairs + 1):
            v = black[i, lo:hi]
            beside = jnp.where(chess, black[i - 1, lo:hi], black[i + 1, lo:hi])
            rest = (red_rhs[i, lo:hi] * factor + (v + beside)) + (black[i, lo - 1:hi - 1] + black[i, lo + 1:hi + 1])
            red[i, lo:hi] = (rest + (moved(v, 1) + moved(v, -1))) * here
            low = (turn(rest, 1) + (moved(v, 2) + v)) * before
            high = (turn(rest, -1) + (v + moved(v, -2))) * after
            beside_z.append(low + high)
        for i in range(1, pairs + 1):
            v = red[i, lo:hi]
            beside = jnp.where(chess, red[i + 1, lo:hi], red[i - 1, lo:hi])
            total = (v + beside) + (red[i, lo - 1:hi - 1] + red[i, lo + 1:hi + 1])
            black[i, lo:hi] = (black_rhs[i, lo:hi] * factor + (total + beside_z[i - 1])) * here

    def scales(rows, width_z, cells):
        lane = iota((rows, width_z), 1)
        return tuple(
            jnp.where((lane - k >= 0) & (lane - k < cells), SIXTH, 0.0) if k or cells < width_z else SIXTH
            for k in (0, 1, -1)
        )

    in2 = slice(PAD, PAD + y2)
    scale2 = scales(y2, z2, z2)
    for i in range(1, p2 + 1):
        r2[i, in2] = (b2r[i, in2] * 16.0) * SIXTH
    coarse(v2, r2, b2b, p2, False, 16.0, y2, SIXTH, True)
    sweep(r2, v2, b2r, b2b, p2, 16.0, y2, scale2, True)

    fold = jnp.where(iota((z2, z3p), 1) == iota((z2, z3p), 0) // 2, 0.125, 0.0)
    parts = []
    for i in range(1, p2 + 1):
        red, from_black = r2[i, in2], coarse_total(v2, i, True, y2, True)[1]
        black, from_red = v2[i, in2], coarse_total(r2, i, False, y2, True)[1]
        r = b2r[i, in2] - (6.0 * red - from_black) * 0.0625
        r = r + (b2b[i, in2] - (6.0 * black - from_red) * 0.0625)
        for g in range(z2 // LANES):
            w2[i - 1, g, 0:y2] = r[:, LANES * g:LANES * (g + 1)]
        parts.append(
            jnp.concatenate(
                [
                    w2[i - 1, g, pl.ds(0, y3, stride=2), :] + w2[i - 1, g, pl.ds(1, y3, stride=2), :]
                    for g in range(z2 // LANES)
                ],
                axis=1,
            )
        )
    r = dot(jnp.concatenate(parts, axis=0), fold)
    chess3 = evens(y3, z3p)
    in3 = slice(PAD, PAD + y3)
    for j in range(p3):
        one, two = r[2 * j * y3:(2 * j + 1) * y3], r[(2 * j + 1) * y3:(2 * j + 2) * y3]
        b3r[1 + j, in3] = jnp.where(chess3, one, two)
        b3b[1 + j, in3] = jnp.where(chess3, two, one)

    full3 = z3 == z3p
    scale3 = scales(y3, z3p, z3)

    def sweep3(_, carry):
        sweep(r3, v3, b3r, b3b, p3, 64.0, y3, scale3, full3)
        return carry

    if p3 == 1:
        for _ in range(CSWEEPS):
            sweep3(0, 0)
    else:
        lax.fori_loop(0, CSWEEPS, sweep3, 0)

    def plane(red, black, chess, odd):
        return jnp.where(chess, black, red) if odd else jnp.where(chess, red, black)

    grow = jnp.where(iota((z3p, z2), 0) == iota((z3p, z2), 1) // 2, 1.0, 0.0)
    v = jnp.concatenate(
        [plane(r3[1 + i // 2, in3], v3[1 + i // 2, in3], chess3, i % 2) for i in range(p2)], axis=0
    )
    v = dot(v, grow)
    for i in range(p2):
        part = v[i * y3:(i + 1) * y3]
        for g in range(z2 // LANES):
            w2[i, g, pl.ds(0, y3, stride=2), :] = part[:, LANES * g:LANES * (g + 1)]
            w2[i, g, pl.ds(1, y3, stride=2), :] = part[:, LANES * g:LANES * (g + 1)]
    for i in range(p2):
        for g in range(z2 // LANES):
            lanes = slice(LANES * g, LANES * (g + 1))
            v2[1 + i, in2, lanes] = v2[1 + i, in2, lanes] + w2[i, g, 0:y2]
    for _ in range(2):
        sweep(r2, v2, b2r, b2b, p2, 16.0, y2, scale2, True)

    mail1.wait()
    grow1 = jnp.where(
        iota((z2, LANES), 0) == mz * qz + (iota((z2, LANES), 1) - left + 2 * LANES) // 2 - LANES, 1.0, 0.0
    )
    rows1 = f1.shape[2]
    half1 = rows1 // 2
    rows2 = pl.ds(pl.multiple_of(my * qy, 8), half1)
    chess2 = evens(half1, z2)
    first, length = span(n1, HALO)
    begin = first - c + mx * n1
    shift = 0 if gx <= 2 else 1
    first_even = begin - shift
    tops = []
    for j in range(length):
        at = j + shift
        index = (first_even + (at - at % 2)) // 2 + 1
        if gx > 2:
            index = jnp.clip(index, 0, p2 + 1)
        tops.append(plane(r2[index, rows2], v2[index, rows2], chess2, at % 2))
    v = dot(jnp.concatenate(tops, axis=0), grow1)
    for j in range(length):
        part = v[j * half1:(j + 1) * half1]
        w1[j, pl.ds(0, half1, stride=2), :] = part
        w1[j, pl.ds(1, half1, stride=2), :] = part

    near_lanes = (lane_l >= left - COR1) & (lane_l < left + hz + COR1)
    for s, side, j, at in regions1():
        for n, (which, group, rows, yi) in enumerate(row_groups()):
            to_rows = slice(PAD + 8 * n, PAD + 8 * n + 8)
            if rows is None:
                base = ny_in[yi, 0] if s is None else nxy_in[s, yi, 0]
            elif s is None:
                base = None
            else:
                base = n_in[s, 0, 8 * rows:8 * rows + 8]
            if base is None:
                middle = b1[at, 0, to_rows]
            else:
                middle = base if j == 0 else turn(base, LANES - hz)
            outer = edges(nz_in, s, which, COR1 * (group * n1 + j), COR1)
            value = jnp.where(mid8, middle, jnp.where(near_lanes, outer, 0.0))
            f1[at, 0, to_rows] = value + w1[at - first, to_rows, :]

    for step in range(4):
        k = (5 - step + 1) // 2
        if step % 2 == 0:
            relax(r1, f1, rhs1[0], s1, n1, k, True, 4.0)
        else:
            relax(f1, r1, rhs1[1], s1, n1, k, False, 4.0)

    mail0.wait()
    grow0 = jnp.where(
        iota((LANES, 2 * LANES), 0) == (left + iota((LANES, 2 * LANES), 1) // 2) % LANES, 1.0, 0.0
    )
    half0 = rows0 // 2
    first, length = span(n0, 2)
    chess_h = evens(half0, LANES)
    tops = []
    for j in range(length):
        index = (first - c + j - j % 2) // 2 + c if gx <= 2 else (first - c + j) // 2 + c
        red, black = r1[index, 0, PAD:PAD + half0], f1[index, 0, PAD:PAD + half0]
        tops.append(plane(red, black, chess_h, j % 2))
    v = dot(jnp.concatenate(tops, axis=0), grow0)
    for j in range(length):
        for g in range(2):
            base = (2 * j + g) * rows0
            part = v[j * half0:(j + 1) * half0, LANES * g:LANES * (g + 1)]
            w0[pl.ds(base, half0, stride=2), :] = part
            w0[pl.ds(base + 1, half0, stride=2), :] = part

    for i in range(n0):
        at = c + i
        j = at - first
        lift = w0[pl.ds(pl.multiple_of(2 * j * rows0, 8) + TOP, ly), :]
        f0[at, 0, own] = black0[at, 0, own] + lift
        for rows in (slice(PAD, TOP), slice(TOP + ly, TOP + ly + 8)):
            lift = w0[pl.ds(pl.multiple_of(2 * j * rows0, 8) + rows.start, 8), :]
            f0[at, 0, rows] = f0[at, 0, rows] + lift
    for side in near:
        for k in (1, 2):
            at = side.landing(c, n0, k)
            j = at - first
            lift = w0[pl.ds(pl.multiple_of(2 * j * rows0, 8) + PAD, rows_h), :]
            f0[at, 0, PAD:PAD + rows_h] = f0[at, 0, PAD:PAD + rows_h] + lift
    for s, side in enumerate([None] + near):
        pairs = range(n0) if side is None else (1, 2)
        for k in pairs:
            if side is None:
                at, far = c + k, k
            else:
                at = side.landing(c, n0, k)
                far = None
            for n in range(groups0 + 2):
                which, group = (0, groups0 - 1) if n == 0 else ((2, 0) if n > groups0 else (1, n - 1))
                tiles = []
                for zi in range(2):
                    t = g_in[zi, s, which]
                    if far is not None:
                        lo = COR0 * (group * n0 + far)
                        tiles.append(turn(t, (LANES - COR0 if zi == 0 else 0) - lo))
                    elif side.dynamic:
                        spot = (LANES - COR0 if zi == 0 else 0)
                        a = turn(t, spot - COR0 * (group * n0 + k - 1))
                        b = turn(t, spot - COR0 * (group * n0 + n0 - k))
                        tiles.append(jnp.where(side.up, a, b))
                    else:
                        far_at = n0 - k if side.up else k - 1
                        tiles.append(turn(t, (LANES - COR0 if zi == 0 else 0) - COR0 * (group * n0 + far_at)))
                low, high = tiles
                value = jnp.where(lane8 >= LANES - COR0, low, jnp.where(lane8 < COR0, high, 0.0))
                j = at - first
                to_rows = slice(PAD + 8 * n, PAD + 8 * n + 8)
                lift = w0[pl.ds(pl.multiple_of((2 * j + 1) * rows0, 8) + PAD + 8 * n, 8), :]
                f0[at, 1, to_rows] = value + lift

    relax(r0, f0, rhs0[0], s0, n0, 2, True, 1.0)
    relax(f0, r0, rhs0[1], s0, n0, 1, False, 1.0)
    relax(r0, f0, rhs0[0], s0, n0, 1, True, 1.0)

    def emit(j, red, black):
        out_ref[2 * j] = jnp.where(even, red, black)
        out_ref[2 * j + 1] = jnp.where(even, black, red)

    relax(None, r0, rhs0[1], s0, n0, 0, False, 1.0, tiles=1, emit=emit)


def local(sizes, right_side, start):
    gx, gy, gz = sizes
    lx, ly, lz = start.shape
    f32 = jnp.float32
    count = gx * gy * gz
    near = {1: 0, 2: 1}.get(gx, 2)
    far = {1: 0, 2: 1}.get(gx, 4)
    n0, n1 = lx // 2, lx // 4
    m0, m1 = n0 + 2 * HALO, n1 + 2 * HALO
    r0, r1 = ly + 2 * TOP, ly // 2 + 2 * TOP
    hy = ly // 2
    y2, z2 = gy * ly // 4, gz * lz // 4
    p2, p3 = gx * lx // 8, gx * lx // 16
    y3, z3 = y2 // 2, z2 // 2
    z3p = -(-z3 // LANES) * LANES
    dx = min(gx - 1, -(-REACH2 // (lx // 4)))
    dy = min(gy - 1, -(-REACH2 // (ly // 4)))
    dz = min(gz - 1, -(-REACH2 // (lz // 4)))
    rounds = max(2, sum(max(0, d - 2) for d in (dx, dy, dz)) - 1)
    near_a, far_a = max(near, 1), max(far, 1)

    def vmem(*shape):
        return pltpu.VMEM(shape, f32)

    messages = 24 if gx <= 2 else 48
    return pl.pallas_call(
        functools.partial(kernel, sizes),
        out_shape=jax.ShapeDtypeStruct(start.shape, f32),
        in_specs=[pl.BlockSpec(memory_space=pl.ANY)] * 2,
        out_specs=pl.BlockSpec(memory_space=pltpu.VMEM),
        scratch_shapes=[
            vmem(lx, ly, lz),
            vmem(lx, ly, lz),
            vmem(3, m0, 2, r0, LANES),
            vmem(m0, 2, r0, LANES),
            vmem(m0, 2, r0, LANES),
            vmem(2, r0 - 2 * PAD, LANES),
            vmem(near_a, ly, LANES),
            vmem(near_a, ly, LANES),
            vmem(2, ly, LANES),
            vmem(2, ly + 16, LANES),
            vmem(near_a, 2, 8, LANES),
            vmem(near_a, 2, 3, 8, LANES),
            vmem(near_a, 2, 16, LANES),
            vmem(near_a, 2, 16, LANES),
            vmem(2, m1, 1, r1, LANES),
            vmem(m1, 1, r1, LANES),
            vmem(m1, 1, r1, LANES),
            vmem(m1, 1, r1, LANES),
            vmem(1, r1 - 2 * PAD, LANES),
            vmem(2 * m0 * r0, LANES),
            vmem(m1, r1, LANES),
            vmem(n1, hy, LANES),
            vmem(far_a, n1, hy, LANES),
            vmem(2, n1, 8, LANES),
            vmem(far_a, 2, n1, 8, LANES),
            vmem(2, 8, LANES),
            vmem(2, far + 1, 3, 8, LANES),
            vmem(1, hy, LANES),
            vmem(far_a, 1, hy, LANES),
            vmem(2, 1, 8, LANES),
            vmem(far_a, 2, 1, 8, LANES),
            vmem(2, 8, LANES),
            vmem(2, far + 1, 3, 8, LANES),
            vmem(2, 8, LANES),
            vmem(2, near + 1, 3, 8, LANES),
            vmem(p2 + 2, y2 + 2 * PAD, z2),
            vmem(p2 + 2, y2 + 2 * PAD, z2),
            vmem(p2 + 2, y2 + 2 * PAD, z2),
            vmem(p2 + 2, y2 + 2 * PAD, z2),
            vmem(8, LANES),
            vmem(count, 8, LANES),
            vmem(p2, z2 // LANES, y2, LANES),
            vmem(p3 + 2, y3 + 2 * PAD, z3p),
            vmem(p3 + 2, y3 + 2 * PAD, z3p),
            vmem(p3 + 2, y3 + 2 * PAD, z3p),
            vmem(p3 + 2, y3 + 2 * PAD, z3p),
            pltpu.SemaphoreType.DMA((2,)),
            pltpu.SemaphoreType.REGULAR((rounds,)),
            pltpu.SemaphoreType.DMA((4, 2, messages)),
            pltpu.SemaphoreType.DMA((2, count)),
        ],
        compiler_params=pltpu.CompilerParams(
            collective_id=0, has_side_effects=True, vmem_limit_bytes=GRANT
        ),
    )(right_side, start)


def solution(mesh):
    sizes = (mesh.shape["gx"], mesh.shape["gy"], mesh.shape["gz"])
    spec = P("gx", "gy", "gz")
    return jax.shard_map(
        functools.partial(local, sizes), mesh=mesh, in_specs=(spec, spec), out_specs=spec, check_vma=False
    )
```

```python
import functools

import jax
import jax.numpy as jnp
from jax import lax
from jax.experimental import pallas as pl
from jax.experimental.pallas import tpu as pltpu
from jax.sharding import PartitionSpec as P

MESH = pl.DeviceIdType.MESH
SIXTH = 1.0 / 6.0
PAD = 8
TOP = 16
LANES = 128
HALO = 3
CSWEEPS = 8
REACH2 = 42
EDGE = ((0, 1, 4), (0, 2, 2), (1, 1, 3), (1, 2, 1), (2, 1, 2))
FACE = 5
RHS1 = 5
COR1 = 6
COR0 = 4
GRANT = 56150000


def dot(a, b):
    high = a.astype(jnp.bfloat16)
    rest = a - high.astype(jnp.float32)
    middle = rest.astype(jnp.bfloat16)
    low = (rest - middle.astype(jnp.float32)).astype(jnp.bfloat16)
    b = b.astype(jnp.bfloat16)
    return jnp.dot(
        jnp.concatenate([high, middle, low], axis=1),
        jnp.concatenate([b, b, b], axis=0),
        preferred_element_type=jnp.float32,
    )


def iota(shape, axis):
    return lax.broadcasted_iota(jnp.int32, shape, axis)


def turn(v, shift):
    shift %= v.shape[1]
    return pltpu.roll(v, shift, axis=1) if shift else v


def evens(rows, lanes, add=0):
    shape = (rows // 8, 8, lanes)
    return ((iota(shape, 1) + iota(shape, 2) + add) & 1).reshape(rows, lanes) == 0


def both(*terms):
    out = True
    for term in terms:
        if term is True:
            continue
        out = term if out is True else out & term
    return out


def when(condition, action):
    if condition is True:
        action()
    else:
        pl.when(condition)(action)


class Side:
    def __init__(self, hop, up, send, recv, peer):
        self.hop, self.up, self.send, self.recv, self.peer = hop, up, send, recv, peer
        self.dynamic = not isinstance(up, bool)

    def pick(self, a, b):
        if self.dynamic:
            return jnp.where(self.up, a, b)
        return a if self.up else b

    def source(self, c, n, count):
        return self.pick(c + n - count, c)

    def target(self, c, n, count):
        return self.pick(c - count, c + n)

    def landing(self, c, n, k):
        if self.dynamic:
            return jnp.where(self.up, c + n + k - 1, c - k)
        return c - k if self.up else c + n + k - 1

    def outward(self, c, n, k):
        return self.pick(c + n - k, c + k - 1)

    def base(self, c, n):
        if self.dynamic:
            return jnp.where(self.up, c + n, c - n)
        return c - self.hop * n if self.up else c + self.hop * n

    def send_shift(self):
        return self.pick(0, 1)

    def recv_shift(self):
        return jnp.where(self.up, 1, 0) if self.dynamic else (0 if self.up else 1)


class Mail:
    def __init__(self, sems):
        self.sems, self.count, self.items = sems, 0, []

    def add(self, src, dst, send, recv, peer, tag=None):
        at = self.count
        self.count += 1
        copy = pltpu.make_async_remote_copy(
            src_ref=src,
            dst_ref=dst,
            send_sem=self.sems.at[0, at],
            recv_sem=self.sems.at[1, at],
            device_id=peer,
            device_id_type=MESH,
        )
        self.items.append((tag, copy, send, recv))
        when(send, copy.start)

    def wait(self, tag=None):
        for item in list(self.items):
            name, copy, send, recv = item
            if tag is None or name == tag:
                when(send, copy.wait_send)
                when(recv, copy.wait_recv)
                self.items.remove(item)


def kernel(
    sizes, rhs_hbm, start_hbm, out_ref,
    rhs, start, a0, r0, f0, s0, merged_out, merged_in, zsend, zrecv, esend, erecv, yedge_out, yedge_in,
    a1, r1, b1, f1, s1, w0, w1, tiles_out, tiles_in, ysides, xysides, zout, zin,
    n_out, n_in, ny_in, nxy_in, nz_out, nz_in, g_out, g_in,
    b2r, b2b, r2, v2, pack, slots, w2, b3r, b3b, r3, v3,
    in_sems, relay, sems, gather_sems,
):
    gx, gy, gz = sizes
    count = gx * gy * gz
    mx, my, mz = lax.axis_index("gx"), lax.axis_index("gy"), lax.axis_index("gz")
    lx, ly, lz = start.shape
    n0, n1 = lx // 2, lx // 4
    hy, hz = ly // 2, lz // 2
    qy, qz = hy // 2, hz // 2
    left = (LANES - hz) // 2
    c = HALO
    y2, z2 = gy * qy, gz * qz
    p2, p3 = gx * lx // 8, gx * lx // 16
    y3, z3 = y2 // 2, z2 // 2
    z3p = r3.shape[2]
    groups0, groups1 = ly // 8, hy // 8

    copies = [
        pltpu.make_async_copy(start_hbm, start, in_sems.at[0]),
        pltpu.make_async_copy(rhs_hbm, rhs, in_sems.at[1]),
    ]
    for copy in copies:
        copy.start()

    if gx == 1:
        near, sides1 = [], []
    elif gx == 2:
        near = sides1 = [Side(1, mx == 0, True, True, 1 - mx)]
    else:
        def side(hop, up):
            if up:
                return Side(hop, True, mx + hop < gx, mx >= hop, mx + hop)
            return Side(hop, False, mx >= hop, mx + hop < gx, mx - hop)

        near = [side(1, True), side(1, False)]
        sides1 = near + [side(2, True), side(2, False)]

    def along(at, size, step):
        if step == 0:
            return True, True, at
        if step > 0:
            return at + 1 < size, at >= 1, at + 1
        return at >= 1, at + 1 < size, at - 1

    def to(side, dy, dz):
        sx, rx, px = (True, True, mx) if side is None else (side.send, side.recv, side.peer)
        sy, ry, py = along(my, gy, dy)
        sz, rz, pz = along(mz, gz, dz)
        return both(sx, sy, sz), both(rx, ry, rz), (px, py, pz)

    faces = [to(s, 0, 0) for s in near]
    faces += [to(None, d, 0) for d in (1, -1)] + [to(None, 0, d) for d in (1, -1)]

    def signal_faces(sem):
        for send, _, peer in faces:
            when(send, lambda peer=peer: pl.semaphore_signal(sem, inc=1, device_id=peer, device_id_type=MESH))

    heard = sum([(1 if recv is True else jnp.where(recv, 1, 0)) for _, recv, _ in faces])

    def clear(*refs):
        for ref in refs:
            ref[...] = jnp.zeros_like(ref)

    rows0 = a0.shape[3]
    own = slice(TOP, TOP + ly)
    outside = [i for i in range(a0.shape[1]) if i < c or i >= c + n0]
    clear(zrecv, erecv, yedge_in)
    for q in range(3):
        for i in range(c, c + n0):
            a0[q, i, 0, PAD:TOP] = jnp.zeros((PAD, LANES), jnp.float32)
            a0[q, i, 0, TOP + ly:TOP + ly + PAD] = jnp.zeros((PAD, LANES), jnp.float32)
        if gx != 2:
            for i in outside:
                a0[q, i, 0, own] = jnp.zeros((ly, LANES), jnp.float32)
    if gx != 2:
        clear(merged_in)
    barrier = pltpu.get_barrier_semaphore()
    signal_faces(barrier)
    clear(slots)

    def mask(shape, row0, lane_of, bounds):
        y = iota(shape, 0) + row0
        z = lane_of(iota(shape, 1))
        inside = (y >= 0) & (y < bounds[0]) & (z >= 0) & (z < bounds[1])
        return jnp.where(inside, SIXTH, 0.0)

    even = evens(ly, LANES)
    for copy in copies:
        copy.wait()
    for i in range(n0):
        a0[0, c + i, 0, own] = jnp.where(even, start[2 * i + 1], start[2 * i])
        a0[1, c + i, 0, own] = jnp.where(even, rhs[2 * i], rhs[2 * i + 1])
        a0[2, c + i, 0, own] = jnp.where(even, rhs[2 * i + 1], rhs[2 * i])
    for s, side in enumerate(near):
        third = a0[0, side.outward(c, n0, 3), 0, own]
        second = a0[2, side.outward(c, n0, 2), 0, own]
        merged_out[s] = jnp.where(evens(ly, LANES, side.send_shift()), third, pltpu.roll(second, 1, axis=0))

    pl.semaphore_wait(barrier, heard)

    lane64 = iota((ly, LANES), 1)
    lane8 = iota((8, LANES), 1)
    ydirs = zdirs = (1, -1)
    mail = Mail(sems.at[0])
    for s, side in enumerate(near):
        where = to(side, 0, 0)
        src, dst = side.source(c, n0, 2), side.target(c, n0, 2)
        mail.add(a0.at[0:2, pl.ds(src, 2), 0, own], a0.at[0:2, pl.ds(dst, 2), 0, own], *where, "x")

    def strip(d, rows):
        return (TOP + rows - 8, TOP - 8) if d > 0 else (TOP, TOP + rows)

    for d in ydirs:
        src, dst = strip(d, ly)
        mail.add(
            a0.at[0:3, pl.ds(c, n0), 0, pl.ds(src, 8)],
            a0.at[0:3, pl.ds(c, n0), 0, pl.ds(dst, 8)],
            *to(None, d, 0), "z",
        )
    signal_faces(relay.at[0])
    clear(ysides, xysides, tiles_in, zin, n_in, ny_in, nxy_in, nz_in, g_in)

    slots0 = [(q, i) for i in range(n0) for q in range(3)]
    for zi, d in enumerate(zdirs):
        packed = jnp.zeros((ly, LANES), jnp.float32)
        for t, (q, i) in enumerate(slots0):
            v = a0[q, c + i, 0, own]
            first = lz - FACE if d > 0 else 0
            here = (lane64 >= FACE * t) & (lane64 < FACE * (t + 1))
            packed = jnp.where(here, turn(v, FACE * t - first), packed)
        zsend[zi] = packed
    for zi, d in enumerate(zdirs):
        mail.add(zsend.at[zi], zrecv.at[zi, pl.ds(8, ly)], *to(None, 0, d), "z")

    width = sum(w for _, _, w in EDGE)
    starts = [sum(w for _, _, w in EDGE[:t]) for t in range(len(EDGE))]
    for s, side in enumerate(near):
        for zi, d in enumerate(zdirs):
            packed = jnp.zeros((8, LANES), jnp.float32)
            for (q, k, w), at in zip(EDGE, starts):
                v = a0[q, side.outward(c, n0, k), 0, own]
                for g in range(groups0):
                    lo = width * g + at
                    first = lz - w if d > 0 else 0
                    here = (lane8 >= lo) & (lane8 < lo + w)
                    packed = jnp.where(here, turn(v[8 * g:8 * g + 8], lo - first), packed)
            esend[s, zi] = packed
        for yi, d in enumerate(ydirs):
            for (q, k, w), at in zip(EDGE, starts):
                first = TOP + ly - w if d > 0 else TOP
                yedge_out[s, yi, at:at + w] = a0[q, side.outward(c, n0, k), 0, first:first + w]
    pl.semaphore_wait(relay.at[0], heard)
    signal_faces(relay.at[1])
    for s, side in enumerate(near):
        for yi, d in enumerate(ydirs):
            filled = pl.ds(0, width)
            mail.add(yedge_out.at[s, yi, filled], yedge_in.at[s, yi, filled], *to(side, d, 0), "y")
    for zi, dz in enumerate(zdirs):
        for d in ydirs:
            src, dst = strip(d, ly)
            mail.add(
                zsend.at[zi, pl.ds(src - TOP, 8)], zrecv.at[zi, pl.ds(dst - 8, 8)], *to(None, d, dz), "z"
            )
        for s, side in enumerate(near):
            mail.add(esend.at[s, zi], erecv.at[s, zi, 1], *to(side, 0, dz), "e")
    rounds = relay.shape[0]
    pl.semaphore_wait(relay.at[1], heard)
    for zi, dz in enumerate(zdirs):
        for s, side in enumerate(near):
            for d in ydirs:
                half = pl.ds(4 if d > 0 else 0, 4)
                mail.add(esend.at[s, zi, half], erecv.at[s, zi, 0 if d > 0 else 2, half], *to(side, d, dz), "e")
    for s, side in enumerate(near):
        where = to(side, 0, 0)
        src, dst = side.source(c, n0, 1), side.target(c, n0, 1)
        mail.add(a0.at[2, pl.ds(src, 1), 0, own], a0.at[2, pl.ds(dst, 1), 0, own], *where)
        mail.add(merged_out.at[s], merged_in.at[s], *where)
    for r in range(2, rounds):
        signal_faces(relay.at[r])
        pl.semaphore_wait(relay.at[r], heard)
    clear(r0, f0)
    for q in range(3):
        for i in range(a0.shape[1]):
            a0[q, i, 1] = jnp.zeros((rows0, LANES), jnp.float32)
            edge = PAD if c <= i < c + n0 else TOP
            a0[q, i, 0, 0:edge] = jnp.zeros((edge, LANES), jnp.float32)
            a0[q, i, 0, rows0 - edge:] = jnp.zeros((edge, LANES), jnp.float32)
    if gx == 2:
        for k in range(1, HALO + 1):
            a0[0, jnp.where(mx == 0, c - k, c + n0 + k - 1), 0, own] = jnp.zeros((ly, LANES), jnp.float32)
    fine = (gy * ly, gz * lz)
    s0[0] = mask(s0.shape[1:], my * ly - PAD, lambda k: mz * lz + k, fine)
    s0[1] = mask(s0.shape[1:], my * ly - PAD, lambda k: mz * lz + jnp.where(k < 64, k + lz, k - LANES), fine)
    s1[0] = mask(s1.shape[1:], my * hy - PAD, lambda k: mz * hz + k - left, (gy * hy, gz * hz))

    mail.wait("z")
    rows_h = ly + 16
    lane_h = iota((rows_h, LANES), 1)
    for t, (q, i) in enumerate(slots0):
        low = turn(zrecv[0], LANES - FACE - FACE * t)
        high = turn(zrecv[1], -FACE * t)
        a0[q, c + i, 1, PAD:PAD + rows_h] = jnp.where(
            lane_h >= LANES - FACE, low, jnp.where(lane_h < FACE, high, 0.0)
        )
    def span(n, k):
        if gx == 1:
            return c, n
        k = min(k, n * (gx - 1), HALO)
        if gx == 2:
            return jnp.where(mx == 0, c, c - k), n + k
        return c - k, n + 2 * k

    def inside(n, i):
        if gx <= 2:
            return None
        at = mx * n + i - c
        return jnp.where((at >= 0) & (at < gx * n), 1.0, 0.0)

    def neighbours(src, i, planes, red, chess, lo, hi, tiles):
        prev, cur, nxt = planes
        low = [turn(t, 1) for t in cur]
        high = [turn(t, -1) for t in cur]
        if len(cur) == 2:
            lane = iota(cur[0].shape, 1)
            low = [jnp.where(lane == 0, low[1 - g], low[g]) for g in range(tiles)]
            high = [jnp.where(lane == LANES - 1, high[1 - g], high[g]) for g in range(tiles)]
        out = []
        for g in range(tiles):
            beside = jnp.where(chess, prev[g], nxt[g]) if red else jnp.where(chess, nxt[g], prev[g])
            total = (cur[g] + beside) + (src[i, g, lo - 1:hi - 1] + src[i, g, lo + 1:hi + 1])
            out.append(total + (low[g] + high[g]))
        return out

    def relax(dst, src, rhs_of, scale, n, k, red, factor, tiles=None, emit=None, part=None):
        first, length = part or span(n, k)
        held = src.shape[1]
        rows = src.shape[2]
        lo, hi = (TOP, rows - TOP) if emit else (PAD, rows - PAD)
        tiles = tiles or held
        chess = evens(hi - lo, LANES)
        planes = [[src[first + j - 1, g, lo:hi] for g in range(held)] for j in range(length + 2)]
        for j in range(length):
            i = first + j
            totals = neighbours(src, i, planes[j:j + 3], red, chess, lo, hi, tiles)
            factor_x = inside(n, i)
            for g in range(tiles):
                b = rhs_of(i, g, lo, hi)
                if factor != 1.0:
                    b = b * factor
                value = (b + totals[g]) * scale[g, lo - PAD:hi - PAD]
                if factor_x is not None:
                    value = value * factor_x
                if emit:
                    emit(j, planes[j + 1][g], value)
                else:
                    dst[i, g, lo:hi] = value

    def residual(red_ref, black_ref, red_rhs, black_rhs, n, j, factor):
        rows = red_ref.shape[2]
        lo, hi = TOP, rows - TOP
        chess = evens(hi - lo, LANES)
        i = c + j
        held = red_ref.shape[1]

        def load(ref):
            return [[ref[i + d, g, lo:hi] for g in range(held if d == 0 else 1)] for d in (-1, 0, 1)]

        red, black = load(red_ref), load(black_ref)
        from_black = neighbours(black_ref, i, black, True, chess, lo, hi, 1)[0]
        from_red = neighbours(red_ref, i, red, False, chess, lo, hi, 1)[0]
        out = red_rhs(i, 0, lo, hi) - (6.0 * red[1][0] - from_black) * (1.0 / factor)
        return out + (black_rhs(i, 0, lo, hi) - (6.0 * black[1][0] - from_red) * (1.0 / factor))

    black0 = a0.at[0]
    rhs0 = [lambda i, g, lo, hi, q=q: a0[q, i, g, lo:hi] for q in (1, 2)]
    def sweep0(step, part):
        if step % 2 == 0:
            relax(r0, black0, rhs0[0], s0, n0, 0, True, 1.0, part=part)
        else:
            relax(black0, r0, rhs0[1], s0, n0, 0, False, 1.0, part=part)

    def early(step):
        return n0 - 1 - step if gx == 2 and n0 >= 4 else 0

    for step in range(4):
        if early(step) > 0:
            sweep0(step, (jnp.where(mx == 0, c, c + n0 - early(step)), early(step)))
    mail.wait("e")
    for s, side in enumerate(near):
        for (q, k, w), at in zip(EDGE, starts):
            pair = side.landing(c, n0, k)
            for g in range(groups0 + 2):
                which, group = (0, groups0 - 1) if g == 0 else ((2, 0) if g > groups0 else (1, g - 1))
                lo = width * group + at
                low = turn(erecv[s, 0, which], LANES - w - lo)
                high = turn(erecv[s, 1, which], -lo)
                a0[q, pair, 1, PAD + 8 * g:PAD + 8 * g + 8] = jnp.where(
                    lane8 >= LANES - w, low, jnp.where(lane8 < w, high, 0.0)
                )

    mail.wait("y")
    for s, side in enumerate(near):
        for yi, d in enumerate(ydirs):
            for (q, k, w), at in zip(EDGE, starts):
                first = TOP - w if d > 0 else TOP + ly
                a0[q, side.landing(c, n0, k), 0, first:first + w] = yedge_in[s, yi, at:at + w]
    late = 2 if gx == 2 and n0 >= 4 else 0
    if late:
        mail.wait("x")
        for step in range(4):
            sweep0(step, (jnp.where(mx == 0, c + early(step), c + n0 - late - early(step)), late))
    mail.wait()
    for s, side in enumerate(near):
        v = merged_in[s]
        a0[0, side.landing(c, n0, 3), 0, own] = v
        a0[2, side.landing(c, n0, 2), 0, own] = pltpu.roll(v, ly - 1, axis=0)
    for step in range(4):
        first, length = span(n0, (4 - step + 1) // 2)
        done = early(step) + late
        if done:
            first = first + jnp.where(mx == 0, done, 0)
        sweep0(step, (first, length - done))
    for j in range(n0):
        w0[j * ly:(j + 1) * ly, :] = residual(r0, black0, rhs0[0], rhs0[1], n0, j, 1.0)
    r = w0[pl.ds(0, n0 * hy, stride=2), :] + w0[pl.ds(1, n0 * hy, stride=2), :]
    source, target = iota((LANES, LANES), 0), iota((LANES, LANES), 1)
    fold = jnp.where(lax.rem(target - left + LANES, hz) == source // 2, 0.125, 0.0)
    r = dot(r, fold)

    own1 = slice(TOP, TOP + hy)
    lane32 = iota((hy, LANES), 1)
    mid = (lane32 >= left) & (lane32 < left + hz)
    chess1 = evens(hy, LANES)
    for j in range(n1):
        one, two = r[2 * j * hy:(2 * j + 1) * hy], r[(2 * j + 1) * hy:(2 * j + 2) * hy]
        red = jnp.where(chess1, one, two)
        black = jnp.where(chess1, two, one)
        tiles_out[j] = jnp.where(mid, red, black)
        a1[0, c + j, 0, own1] = jnp.where(mid, red, 0.0)
        a1[1, c + j, 0, own1] = jnp.where(mid, black, 0.0)

    def pack_edges(read, items, w):
        for d in zdirs:
            first = left + hz - w if d > 0 else left
            packed = jnp.zeros((8, LANES), jnp.float32)
            for t in range(items * groups1):
                here = (lane8 >= w * t) & (lane8 < w * (t + 1))
                packed = jnp.where(here, turn(read(t), w * t - first), packed)
            yield packed

    def post1(mail, out, into, y_in, xy_in, z_out, z_in, corner):
        far_first = list(enumerate([None] + sides1))[::-1]
        for steps in ((1, -1), (0,)):
            for s, side in far_first:
                for zi, dz in enumerate(zdirs):
                    for d in steps:
                        few = corner if d and side is not None else 8
                        rows = pl.ds(8 - few if d > 0 else 0, few)
                        mail.add(z_out.at[zi, rows], z_in.at[zi, s, 1 - d, rows], *to(side, d, dz))
        for s, side in enumerate(sides1):
            for yi, d in enumerate(ydirs):
                src = hy - 8 if d > 0 else 0
                mail.add(out.at[:, pl.ds(src, 8)], xy_in.at[s, yi], *to(side, d, 0))
        for s, side in enumerate(sides1):
            mail.add(out, into.at[s], *to(side, 0, 0))
        for yi, d in enumerate(ydirs):
            src = hy - 8 if d > 0 else 0
            mail.add(out.at[:, pl.ds(src, 8)], y_in.at[yi], *to(None, d, 0))

    def regions1():
        yield from ((None, None, j, c + j) for j in range(n1))
        for s, side in enumerate(sides1):
            for j in range(n1):
                at = side.base(c, n1) + j
                if side.dynamic or 0 <= at < 2 * c + n1:
                    yield (s, side, j, at)

    def row_groups():
        yield 0, groups1 - 1, None, 0
        for g in range(groups1):
            yield 1, g, g, None
        yield 2, 0, None, 1

    lane_l = lane8
    mid8 = (lane_l >= left) & (lane_l < left + hz)

    def edges(z_in, s, which, lo, w):
        at = 0 if s is None else s + 1
        low = turn(z_in[0, at, which], left - w - lo)
        high = turn(z_in[1, at, which], left + hz - lo)
        return jnp.where(lane_l < left, low, high)

    items = 2 * n1
    order1 = [(g, q, j) for g in range(groups1) for j in range(n1) for q in range(2)]
    tile_of = lambda t: a1[order1[t][1], c + order1[t][2], 0, TOP + 8 * order1[t][0]:TOP + 8 * order1[t][0] + 8]
    for zi, packed in enumerate(pack_edges(tile_of, items, RHS1)):
        zout[zi] = packed
    mail = Mail(sems.at[1])
    post1(mail, tiles_out, tiles_in, ysides, xysides, zout, zin, 4)
    for ref in (a1, r1, b1, f1):
        for i in range(ref.shape[-4]):
            halo_pair = i < c or i >= c + n1
            lead = (slice(None),) if len(ref.shape) == 5 else ()
            if halo_pair or ref is not a1:
                at = lead + (i,)
                ref[at] = jnp.zeros(ref[at].shape, jnp.float32)
            else:
                for rows in (slice(0, TOP), slice(TOP + hy, None)):
                    at = lead + (i, slice(None), rows)
                    ref[at] = jnp.zeros(ref[at].shape, jnp.float32)
    for ref in (b2r, b2b, r2, v2, b3r, b3b, r3, v3):
        ref[...] = jnp.zeros_like(ref)
    mail.wait()

    near_lanes = (lane_l >= left - RHS1) & (lane_l < left + hz + RHS1)
    for s, side, j, at in regions1():
        for n, (which, group, rows, yi) in enumerate(row_groups()):
            if rows is None:
                base = ysides[yi, j] if s is None else xysides[s, yi, j]
            elif s is None:
                base = None
            else:
                base = tiles_in[s, j, 8 * rows:8 * rows + 8]
            for q in range(2):
                to_rows = slice(PAD + 8 * n, PAD + 8 * n + 8)
                lo = RHS1 * ((group * n1 + j) * 2 + q)
                if base is None:
                    middle = a1[q, at, 0, to_rows]
                else:
                    middle = base if q == 0 else turn(base, LANES - hz)
                outer = edges(zin, s, which, lo, RHS1)
                a1[q, at, 0, to_rows] = jnp.where(mid8, middle, jnp.where(near_lanes, outer, 0.0))

    rhs1 = [lambda i, g, lo, hi, q=q: a1[q, i, g, lo:hi] for q in (0, 1)]
    first, length = span(n1, 2)
    for j in range(length):
        i = first + j
        value = (a1[0, i, 0, PAD:-PAD] * 4.0) * s1[0]
        factor_x = inside(n1, i)
        r1[i, 0, PAD:-PAD] = value if factor_x is None else value * factor_x
    relax(b1, r1, rhs1[1], s1, n1, 2, False, 4.0)
    relax(r1, b1, rhs1[0], s1, n1, 1, True, 4.0)
    relax(b1, r1, rhs1[1], s1, n1, 1, False, 4.0)

    for j in range(n1):
        w1[j, 0:hy, :] = residual(r1, b1, rhs1[0], rhs1[1], n1, j, 4.0)
    r = jnp.concatenate(
        [w1[j, pl.ds(0, qy, stride=2), :] + w1[j, pl.ds(1, qy, stride=2), :] for j in range(n1)], axis=0
    )
    fold = jnp.where(
        (lax.rem(target, qz) == (source - left) // 2) & (source >= left) & (source < left + hz), 0.125, 0.0
    )
    r = dot(r, fold)
    block = lane8 // qz
    per_colour = qy // 8
    one = two = None
    for h in range(per_colour):
        p, q = r[8 * h:8 * h + 8], r[qy + 8 * h:qy + 8 * h + 8]
        here = lax.rem(block, per_colour) == h
        one = p if one is None else jnp.where(here, p, one)
        two = q if two is None else jnp.where(here, q, two)
    tile = jnp.where(evens(8, LANES) ^ (block >= per_colour), one, two)
    pack[...] = tile

    mine = (mx * gy + my) * gz + mz
    slots[mine] = tile

    dist = (-(-REACH2 // (lx // 4)), -(-REACH2 // qy), -(-REACH2 // qz))

    def coords(k):
        steps = (k // (gy * gz), k // gz % gy, k % gz)
        moved = [at + step for at, step in zip((mx, my, mz), steps)]
        at = tuple(jnp.where(v >= size, v - size, v) for v, size in zip(moved, sizes))
        close = True
        for a, b, size, reach in zip(at, (mx, my, mz), sizes, dist):
            if reach < size - 1:
                close = both(close, (a - b <= reach) & (b - a <= reach))
        return at, close

    def number(at):
        return (at[0] * gy + at[1]) * gz + at[2]

    def flipped(at, k):
        bit = 1
        while bit <= k:
            if k & bit:
                at = at + bit - 2 * bit * lax.rem(lax.div(at, bit), 2)
            bit *= 2
        return at

    def partners():
        own_at = (mx, my, mz)
        flips = [[flipped(at, k) for k in range(size)] for at, size in zip(own_at, sizes)]
        order = [(i, j, k) for i in range(gx) for j in range(gy) for k in range(gz)][1:]
        order.sort(key=lambda f: (-f[0], -min(f[2], 2), -f[1]))
        for f in order:
            at = tuple(flips[axis][k] for axis, k in enumerate(f))
            close = True
            for a, b, k, reach in zip(at, own_at, f, dist):
                if k > reach:
                    close = both(close, (a - b <= reach) & (b - a <= reach))
            yield at, close

    straight = count <= 64 and all(size & (size - 1) == 0 for size in sizes)

    def others(body):
        if straight:
            for place in partners():
                body(place)
        else:
            def step(k, carry):
                body(coords(k))
                return carry

            lax.fori_loop(1, count, step, 0)

    def gather(place, arriving):
        at, close = place
        d = number(at)
        return pltpu.make_async_remote_copy(
            src_ref=pack,
            dst_ref=slots.at[d if arriving else mine],
            send_sem=gather_sems.at[0, d],
            recv_sem=gather_sems.at[1, d if arriving else mine],
            device_id=at,
            device_id_type=MESH,
        ), close

    def gather_start(place):
        copy, close = gather(place, False)
        when(close, copy.start)

    def gather_wait(place):
        copy, close = gather(place, True)

        def done():
            copy.wait_send()
            copy.wait_recv()

        when(close, done)

    others(gather_start)

    red_out = jnp.where(mid, b1[c, 0, own1], turn(b1[c + n1 - 1, 0, own1], LANES - hz))
    n_out[0] = red_out
    order_n = [(g, j) for g in range(groups1) for j in range(n1)]
    tile_n = lambda t: b1[c + order_n[t][1], 0, TOP + 8 * order_n[t][0]:TOP + 8 * order_n[t][0] + 8]
    for zi, packed in enumerate(pack_edges(tile_n, n1, COR1)):
        nz_out[zi] = packed
    mail1 = Mail(sems.at[2])
    post1(mail1, n_out, n_in, ny_in, nxy_in, nz_out, nz_in, 8)

    for zi, d in enumerate(zdirs):
        packed = jnp.zeros((8, LANES), jnp.float32)
        for i in range(n0):
            v = a0[0, c + i, 0, own]
            for g in range(groups0):
                lo = COR0 * (g * n0 + i)
                first = lz - COR0 if d > 0 else 0
                here = (lane8 >= lo) & (lane8 < lo + COR0)
                packed = jnp.where(here, turn(v[8 * g:8 * g + 8], lo - first), packed)
        g_out[zi] = packed
    mail0 = Mail(sems.at[3])
    for side in near:
        src, dst = side.source(c, n0, 2), side.target(c, n0, 2)
        mail0.add(black0.at[pl.ds(src, 2), 0, own], f0.at[pl.ds(dst, 2), 0, own], *to(side, 0, 0))
        for d in ydirs:
            ysrc, ydst = strip(d, ly)
            mail0.add(
                black0.at[pl.ds(src, 2), 0, pl.ds(ysrc, 8)], f0.at[pl.ds(dst, 2), 0, pl.ds(ydst, 8)], *to(side, d, 0)
            )
    for d in ydirs:
        ysrc, ydst = strip(d, ly)
        mail0.add(
            black0.at[pl.ds(c, n0), 0, pl.ds(ysrc, 8)], f0.at[pl.ds(c, n0), 0, pl.ds(ydst, 8)], *to(None, d, 0)
        )
    for zi, dz in enumerate(zdirs):
        for s, side in enumerate([None] + near):
            for yi, d in enumerate((1, 0, -1)):
                mail0.add(g_out.at[zi], g_in.at[zi, s, yi], *to(side, d, dz))

    others(gather_wait)

    per = LANES // qz
    for k in range(gx * gy):
        cx, cy = k // gy, k % gy
        for g in range(gz // per):
            parts = [slots[k * gz + g * per + q] for q in range(per)]
            for h in range(per_colour):
                for colour, ref in ((0, b2r), (1, b2b)):
                    at = colour * per_colour + h
                    v = None
                    for q in range(per):
                        moved = turn(parts[q], (q - at) * qz)
                        here = (lane8 >= q * qz) & (lane8 < (q + 1) * qz)
                        v = moved if v is None else jnp.where(here, moved, v)
                    ref[1 + cx, PAD + cy * qy + 8 * h:PAD + cy * qy + 8 * h + 8, LANES * g:LANES * (g + 1)] = v

    def coarse_total(src, i, red, rows, full):
        width_z = src.shape[2]
        lo, hi = PAD, PAD + rows
        v = src[i, lo:hi]
        low, high = turn(v, 1), turn(v, -1)
        lane = iota(v.shape, 1)
        if full:
            low = jnp.where(lane == 0, 0.0, low)
            high = jnp.where(lane == width_z - 1, 0.0, high)
        chess = evens(rows, width_z)
        prev, nxt = src[i - 1, lo:hi], src[i + 1, lo:hi]
        beside = jnp.where(chess, prev, nxt) if red else jnp.where(chess, nxt, prev)
        total = (v + beside) + (src[i, lo - 1:hi - 1] + src[i, lo + 1:hi + 1])
        return v, total + (low + high)

    def coarse(dst, src, b, pairs, red, factor, rows, scale, full):
        for i in range(1, pairs + 1):
            _, total = coarse_total(src, i, red, rows, full)
            dst[i, PAD:PAD + rows] = (b[i, PAD:PAD + rows] * factor + total) * scale

    def sweep(red, black, red_rhs, black_rhs, pairs, factor, rows, scale, full):
        width_z = black.shape[2]
        lo, hi = PAD, PAD + rows
        lane = iota((rows, width_z), 1)
        chess = evens(rows, width_z)

        def moved(v, k):
            out = turn(v, k)
            if full:
                out = jnp.where(lane < k, 0.0, out) if k > 0 else jnp.where(lane >= width_z + k, 0.0, out)
            return out

        here, before, after = scale
        beside_z = []
        for i in range(1, pairs + 1):
            v = black[i, lo:hi]
            beside = jnp.where(chess, black[i - 1, lo:hi], black[i + 1, lo:hi])
            rest = (red_rhs[i, lo:hi] * factor + (v + beside)) + (black[i, lo - 1:hi - 1] + black[i, lo + 1:hi + 1])
            red[i, lo:hi] = (rest + (moved(v, 1) + moved(v, -1))) * here
            low = (turn(rest, 1) + (moved(v, 2) + v)) * before
            high = (turn(rest, -1) + (v + moved(v, -2))) * after
            beside_z.append(low + high)
        for i in range(1, pairs + 1):
            v = red[i, lo:hi]
            beside = jnp.where(chess, red[i + 1, lo:hi], red[i - 1, lo:hi])
            total = (v + beside) + (red[i, lo - 1:hi - 1] + red[i, lo + 1:hi + 1])
            black[i, lo:hi] = (black_rhs[i, lo:hi] * factor + (total + beside_z[i - 1])) * here

    def scales(rows, width_z, cells):
        lane = iota((rows, width_z), 1)
        return tuple(
            jnp.where((lane - k >= 0) & (lane - k < cells), SIXTH, 0.0) if k or cells < width_z else SIXTH
            for k in (0, 1, -1)
        )

    in2 = slice(PAD, PAD + y2)
    scale2 = scales(y2, z2, z2)
    for i in range(1, p2 + 1):
        r2[i, in2] = (b2r[i, in2] * 16.0) * SIXTH
    coarse(v2, r2, b2b, p2, False, 16.0, y2, SIXTH, True)
    sweep(r2, v2, b2r, b2b, p2, 16.0, y2, scale2, True)

    fold = jnp.where(iota((z2, z3p), 1) == iota((z2, z3p), 0) // 2, 0.125, 0.0)
    parts = []
    for i in range(1, p2 + 1):
        red, from_black = r2[i, in2], coarse_total(v2, i, True, y2, True)[1]
        black, from_red = v2[i, in2], coarse_total(r2, i, False, y2, True)[1]
        r = b2r[i, in2] - (6.0 * red - from_black) * 0.0625
        r = r + (b2b[i, in2] - (6.0 * black - from_red) * 0.0625)
        for g in range(z2 // LANES):
            w2[i - 1, g, 0:y2] = r[:, LANES * g:LANES * (g + 1)]
        parts.append(
            jnp.concatenate(
                [
                    w2[i - 1, g, pl.ds(0, y3, stride=2), :] + w2[i - 1, g, pl.ds(1, y3, stride=2), :]
                    for g in range(z2 // LANES)
                ],
                axis=1,
            )
        )
    r = dot(jnp.concatenate(parts, axis=0), fold)
    chess3 = evens(y3, z3p)
    in3 = slice(PAD, PAD + y3)
    for j in range(p3):
        one, two = r[2 * j * y3:(2 * j + 1) * y3], r[(2 * j + 1) * y3:(2 * j + 2) * y3]
        b3r[1 + j, in3] = jnp.where(chess3, one, two)
        b3b[1 + j, in3] = jnp.where(chess3, two, one)

    full3 = z3 == z3p
    scale3 = scales(y3, z3p, z3)

    def sweep3(_, carry):
        sweep(r3, v3, b3r, b3b, p3, 64.0, y3, scale3, full3)
        return carry

    if p3 == 1:
        for _ in range(CSWEEPS):
            sweep3(0, 0)
    else:
        lax.fori_loop(0, CSWEEPS, sweep3, 0)

    def plane(red, black, chess, odd):
        return jnp.where(chess, black, red) if odd else jnp.where(chess, red, black)

    grow = jnp.where(iota((z3p, z2), 0) == iota((z3p, z2), 1) // 2, 1.0, 0.0)
    v = jnp.concatenate(
        [plane(r3[1 + i // 2, in3], v3[1 + i // 2, in3], chess3, i % 2) for i in range(p2)], axis=0
    )
    v = dot(v, grow)
    for i in range(p2):
        part = v[i * y3:(i + 1) * y3]
        for g in range(z2 // LANES):
            w2[i, g, pl.ds(0, y3, stride=2), :] = part[:, LANES * g:LANES * (g + 1)]
            w2[i, g, pl.ds(1, y3, stride=2), :] = part[:, LANES * g:LANES * (g + 1)]
    for i in range(p2):
        for g in range(z2 // LANES):
            lanes = slice(LANES * g, LANES * (g + 1))
            v2[1 + i, in2, lanes] = v2[1 + i, in2, lanes] + w2[i, g, 0:y2]
    for _ in range(2):
        sweep(r2, v2, b2r, b2b, p2, 16.0, y2, scale2, True)

    mail1.wait()
    grow1 = jnp.where(
        iota((z2, LANES), 0) == mz * qz + (iota((z2, LANES), 1) - left + 2 * LANES) // 2 - LANES, 1.0, 0.0
    )
    rows1 = f1.shape[2]
    half1 = rows1 // 2
    rows2 = pl.ds(pl.multiple_of(my * qy, 8), half1)
    chess2 = evens(half1, z2)
    first, length = span(n1, HALO)
    begin = first - c + mx * n1
    shift = 0 if gx <= 2 else 1
    first_even = begin - shift
    tops = []
    for j in range(length):
        at = j + shift
        index = (first_even + (at - at % 2)) // 2 + 1
        if gx > 2:
            index = jnp.clip(index, 0, p2 + 1)
        tops.append(plane(r2[index, rows2], v2[index, rows2], chess2, at % 2))
    v = dot(jnp.concatenate(tops, axis=0), grow1)
    for j in range(length):
        part = v[j * half1:(j + 1) * half1]
        w1[j, pl.ds(0, half1, stride=2), :] = part
        w1[j, pl.ds(1, half1, stride=2), :] = part

    near_lanes = (lane_l >= left - COR1) & (lane_l < left + hz + COR1)
    for s, side, j, at in regions1():
        for n, (which, group, rows, yi) in enumerate(row_groups()):
            to_rows = slice(PAD + 8 * n, PAD + 8 * n + 8)
            if rows is None:
                base = ny_in[yi, 0] if s is None else nxy_in[s, yi, 0]
            elif s is None:
                base = None
            else:
                base = n_in[s, 0, 8 * rows:8 * rows + 8]
            if base is None:
                middle = b1[at, 0, to_rows]
            else:
                middle = base if j == 0 else turn(base, LANES - hz)
            outer = edges(nz_in, s, which, COR1 * (group * n1 + j), COR1)
            value = jnp.where(mid8, middle, jnp.where(near_lanes, outer, 0.0))
            f1[at, 0, to_rows] = value + w1[at - first, to_rows, :]

    for step in range(4):
        k = (5 - step + 1) // 2
        if step % 2 == 0:
            relax(r1, f1, rhs1[0], s1, n1, k, True, 4.0)
        else:
            relax(f1, r1, rhs1[1], s1, n1, k, False, 4.0)

    mail0.wait()
    grow0 = jnp.where(
        iota((LANES, 2 * LANES), 0) == (left + iota((LANES, 2 * LANES), 1) // 2) % LANES, 1.0, 0.0
    )
    half0 = rows0 // 2
    first, length = span(n0, 2)
    chess_h = evens(half0, LANES)
    tops = []
    for j in range(length):
        index = (first - c + j - j % 2) // 2 + c if gx <= 2 else (first - c + j) // 2 + c
        red, black = r1[index, 0, PAD:PAD + half0], f1[index, 0, PAD:PAD + half0]
        tops.append(plane(red, black, chess_h, j % 2))
    v = dot(jnp.concatenate(tops, axis=0), grow0)
    for j in range(length):
        for g in range(2):
            base = (2 * j + g) * rows0
            part = v[j * half0:(j + 1) * half0, LANES * g:LANES * (g + 1)]
            w0[pl.ds(base, half0, stride=2), :] = part
            w0[pl.ds(base + 1, half0, stride=2), :] = part

    for i in range(n0):
        at = c + i
        j = at - first
        lift = w0[pl.ds(pl.multiple_of(2 * j * rows0, 8) + TOP, ly), :]
        f0[at, 0, own] = black0[at, 0, own] + lift
        for rows in (slice(PAD, TOP), slice(TOP + ly, TOP + ly + 8)):
            lift = w0[pl.ds(pl.multiple_of(2 * j * rows0, 8) + rows.start, 8), :]
            f0[at, 0, rows] = f0[at, 0, rows] + lift
    for side in near:
        for k in (1, 2):
            at = side.landing(c, n0, k)
            j = at - first
            lift = w0[pl.ds(pl.multiple_of(2 * j * rows0, 8) + PAD, rows_h), :]
            f0[at, 0, PAD:PAD + rows_h] = f0[at, 0, PAD:PAD + rows_h] + lift
    for s, side in enumerate([None] + near):
        pairs = range(n0) if side is None else (1, 2)
        for k in pairs:
            if side is None:
                at, far = c + k, k
            else:
                at = side.landing(c, n0, k)
                far = None
            for n in range(groups0 + 2):
                which, group = (0, groups0 - 1) if n == 0 else ((2, 0) if n > groups0 else (1, n - 1))
                tiles = []
                for zi in range(2):
                    t = g_in[zi, s, which]
                    if far is not None:
                        lo = COR0 * (group * n0 + far)
                        tiles.append(turn(t, (LANES - COR0 if zi == 0 else 0) - lo))
                    elif side.dynamic:
                        spot = (LANES - COR0 if zi == 0 else 0)
                        a = turn(t, spot - COR0 * (group * n0 + k - 1))
                        b = turn(t, spot - COR0 * (group * n0 + n0 - k))
                        tiles.append(jnp.where(side.up, a, b))
                    else:
                        far_at = n0 - k if side.up else k - 1
                        tiles.append(turn(t, (LANES - COR0 if zi == 0 else 0) - COR0 * (group * n0 + far_at)))
                low, high = tiles
                value = jnp.where(lane8 >= LANES - COR0, low, jnp.where(lane8 < COR0, high, 0.0))
                j = at - first
                to_rows = slice(PAD + 8 * n, PAD + 8 * n + 8)
                lift = w0[pl.ds(pl.multiple_of((2 * j + 1) * rows0, 8) + PAD + 8 * n, 8), :]
                f0[at, 1, to_rows] = value + lift

    relax(r0, f0, rhs0[0], s0, n0, 2, True, 1.0)
    relax(f0, r0, rhs0[1], s0, n0, 1, False, 1.0)
    relax(r0, f0, rhs0[0], s0, n0, 1, True, 1.0)

    def emit(j, red, black):
        out_ref[2 * j] = jnp.where(even, red, black)
        out_ref[2 * j + 1] = jnp.where(even, black, red)

    relax(None, r0, rhs0[1], s0, n0, 0, False, 1.0, tiles=1, emit=emit)


def local(sizes, right_side, start):
    gx, gy, gz = sizes
    lx, ly, lz = start.shape
    f32 = jnp.float32
    count = gx * gy * gz
    near = {1: 0, 2: 1}.get(gx, 2)
    far = {1: 0, 2: 1}.get(gx, 4)
    n0, n1 = lx // 2, lx // 4
    m0, m1 = n0 + 2 * HALO, n1 + 2 * HALO
    r0, r1 = ly + 2 * TOP, ly // 2 + 2 * TOP
    hy = ly // 2
    y2, z2 = gy * ly // 4, gz * lz // 4
    p2, p3 = gx * lx // 8, gx * lx // 16
    y3, z3 = y2 // 2, z2 // 2
    z3p = -(-z3 // LANES) * LANES
    dx = min(gx - 1, -(-REACH2 // (lx // 4)))
    dy = min(gy - 1, -(-REACH2 // (ly // 4)))
    dz = min(gz - 1, -(-REACH2 // (lz // 4)))
    rounds = max(2, sum(max(0, d - 2) for d in (dx, dy, dz)) - 1)
    near_a, far_a = max(near, 1), max(far, 1)

    def vmem(*shape):
        return pltpu.VMEM(shape, f32)

    messages = 24 if gx <= 2 else 48
    return pl.pallas_call(
        functools.partial(kernel, sizes),
        out_shape=jax.ShapeDtypeStruct(start.shape, f32),
        in_specs=[pl.BlockSpec(memory_space=pl.ANY)] * 2,
        out_specs=pl.BlockSpec(memory_space=pltpu.VMEM),
        scratch_shapes=[
            vmem(lx, ly, lz),
            vmem(lx, ly, lz),
            vmem(3, m0, 2, r0, LANES),
            vmem(m0, 2, r0, LANES),
            vmem(m0, 2, r0, LANES),
            vmem(2, r0 - 2 * PAD, LANES),
            vmem(near_a, ly, LANES),
            vmem(near_a, ly, LANES),
            vmem(2, ly, LANES),
            vmem(2, ly + 16, LANES),
            vmem(near_a, 2, 8, LANES),
            vmem(near_a, 2, 3, 8, LANES),
            vmem(near_a, 2, 16, LANES),
            vmem(near_a, 2, 16, LANES),
            vmem(2, m1, 1, r1, LANES),
            vmem(m1, 1, r1, LANES),
            vmem(m1, 1, r1, LANES),
            vmem(m1, 1, r1, LANES),
            vmem(1, r1 - 2 * PAD, LANES),
            vmem(2 * m0 * r0, LANES),
            vmem(m1, r1, LANES),
            vmem(n1, hy, LANES),
            vmem(far_a, n1, hy, LANES),
            vmem(2, n1, 8, LANES),
            vmem(far_a, 2, n1, 8, LANES),
            vmem(2, 8, LANES),
            vmem(2, far + 1, 3, 8, LANES),
            vmem(1, hy, LANES),
            vmem(far_a, 1, hy, LANES),
            vmem(2, 1, 8, LANES),
            vmem(far_a, 2, 1, 8, LANES),
            vmem(2, 8, LANES),
            vmem(2, far + 1, 3, 8, LANES),
            vmem(2, 8, LANES),
            vmem(2, near + 1, 3, 8, LANES),
            vmem(p2 + 2, y2 + 2 * PAD, z2),
            vmem(p2 + 2, y2 + 2 * PAD, z2),
            vmem(p2 + 2, y2 + 2 * PAD, z2),
            vmem(p2 + 2, y2 + 2 * PAD, z2),
            vmem(8, LANES),
            vmem(count, 8, LANES),
            vmem(p2, z2 // LANES, y2, LANES),
            vmem(p3 + 2, y3 + 2 * PAD, z3p),
            vmem(p3 + 2, y3 + 2 * PAD, z3p),
            vmem(p3 + 2, y3 + 2 * PAD, z3p),
            vmem(p3 + 2, y3 + 2 * PAD, z3p),
            pltpu.SemaphoreType.DMA((2,)),
            pltpu.SemaphoreType.REGULAR((rounds,)),
            pltpu.SemaphoreType.DMA((4, 2, messages)),
            pltpu.SemaphoreType.DMA((2, count)),
        ],
        compiler_params=pltpu.CompilerParams(
            collective_id=0, has_side_effects=True, vmem_limit_bytes=GRANT
        ),
    )(right_side, start)


def solution(mesh):
    sizes = (mesh.shape["gx"], mesh.shape["gy"], mesh.shape["gz"])
    spec = P("gx", "gy", "gz")
    return jax.shard_map(
        functools.partial(local, sizes), mesh=mesh, in_specs=(spec, spec), out_specs=spec, check_vma=False
    )
```

```python
import functools

import jax
import jax.numpy as jnp
from jax import lax
from jax.experimental import pallas as pl
from jax.experimental.pallas import tpu as pltpu
from jax.sharding import PartitionSpec as P

MESH = pl.DeviceIdType.MESH
SIXTH = 1.0 / 6.0
PAD = 8
TOP = 16
LANES = 128
HALO = 3
CSWEEPS = 8
REACH2 = 42
EDGE = ((0, 1, 4), (0, 2, 2), (1, 1, 3), (1, 2, 1), (2, 1, 2))
FACE = 5
RHS1 = 5
COR1 = 6
COR0 = 4
GRANT = 56150000


def dot(a, b):
    high = a.astype(jnp.bfloat16)
    rest = a - high.astype(jnp.float32)
    middle = rest.astype(jnp.bfloat16)
    low = (rest - middle.astype(jnp.float32)).astype(jnp.bfloat16)
    b = b.astype(jnp.bfloat16)
    return jnp.dot(
        jnp.concatenate([high, middle, low], axis=1),
        jnp.concatenate([b, b, b], axis=0),
        preferred_element_type=jnp.float32,
    )


def iota(shape, axis):
    return lax.broadcasted_iota(jnp.int32, shape, axis)


def turn(v, shift):
    shift %= v.shape[1]
    return pltpu.roll(v, shift, axis=1) if shift else v


def evens(rows, lanes, add=0):
    shape = (rows // 8, 8, lanes)
    return ((iota(shape, 1) + iota(shape, 2) + add) & 1).reshape(rows, lanes) == 0


def both(*terms):
    out = True
    for term in terms:
        if term is True:
            continue
        out = term if out is True else out & term
    return out


def when(condition, action):
    if condition is True:
        action()
    else:
        pl.when(condition)(action)


class Side:
    def __init__(self, hop, up, send, recv, peer):
        self.hop, self.up, self.send, self.recv, self.peer = hop, up, send, recv, peer
        self.dynamic = not isinstance(up, bool)

    def pick(self, a, b):
        if self.dynamic:
            return jnp.where(self.up, a, b)
        return a if self.up else b

    def source(self, c, n, count):
        return self.pick(c + n - count, c)

    def target(self, c, n, count):
        return self.pick(c - count, c + n)

    def landing(self, c, n, k):
        if self.dynamic:
            return jnp.where(self.up, c + n + k - 1, c - k)
        return c - k if self.up else c + n + k - 1

    def outward(self, c, n, k):
        return self.pick(c + n - k, c + k - 1)

    def base(self, c, n):
        if self.dynamic:
            return jnp.where(self.up, c + n, c - n)
        return c - self.hop * n if self.up else c + self.hop * n

    def send_shift(self):
        return self.pick(0, 1)

    def recv_shift(self):
        return jnp.where(self.up, 1, 0) if self.dynamic else (0 if self.up else 1)


class Mail:
    def __init__(self, sems):
        self.sems, self.count, self.items = sems, 0, []

    def add(self, src, dst, send, recv, peer, tag=None):
        at = self.count
        self.count += 1
        copy = pltpu.make_async_remote_copy(
            src_ref=src,
            dst_ref=dst,
            send_sem=self.sems.at[0, at],
            recv_sem=self.sems.at[1, at],
            device_id=peer,
            device_id_type=MESH,
        )
        self.items.append((tag, copy, send, recv))
        when(send, copy.start)

    def wait(self, tag=None):
        for item in list(self.items):
            name, copy, send, recv = item
            if tag is None or name == tag:
                when(send, copy.wait_send)
                when(recv, copy.wait_recv)
                self.items.remove(item)


def kernel(
    sizes, rhs_hbm, start_hbm, out_ref,
    rhs, start, a0, r0, f0, s0, merged_out, merged_in, zsend, zrecv, esend, erecv, yedge_out, yedge_in,
    a1, r1, b1, f1, s1, w0, w1, tiles_out, tiles_in, ysides, xysides, zout, zin,
    n_out, n_in, ny_in, nxy_in, nz_out, nz_in, g_out, g_in,
    b2r, b2b, r2, v2, pack, slots, w2, b3r, b3b, r3, v3,
    in_sems, relay, sems, gather_sems,
):
    gx, gy, gz = sizes
    count = gx * gy * gz
    mx, my, mz = lax.axis_index("gx"), lax.axis_index("gy"), lax.axis_index("gz")
    lx, ly, lz = start.shape
    n0, n1 = lx // 2, lx // 4
    hy, hz = ly // 2, lz // 2
    qy, qz = hy // 2, hz // 2
    left = (LANES - hz) // 2
    c = HALO
    y2, z2 = gy * qy, gz * qz
    p2, p3 = gx * lx // 8, gx * lx // 16
    y3, z3 = y2 // 2, z2 // 2
    z3p = r3.shape[2]
    groups0, groups1 = ly // 8, hy // 8

    copies = [
        pltpu.make_async_copy(start_hbm, start, in_sems.at[0]),
        pltpu.make_async_copy(rhs_hbm, rhs, in_sems.at[1]),
    ]
    for copy in copies:
        copy.start()

    if gx == 1:
        near, sides1 = [], []
    elif gx == 2:
        near = sides1 = [Side(1, mx == 0, True, True, 1 - mx)]
    else:
        def side(hop, up):
            if up:
                return Side(hop, True, mx + hop < gx, mx >= hop, mx + hop)
            return Side(hop, False, mx >= hop, mx + hop < gx, mx - hop)

        near = [side(1, True), side(1, False)]
        sides1 = near + [side(2, True), side(2, False)]

    def along(at, size, step):
        if step == 0:
            return True, True, at
        if step > 0:
            return at + 1 < size, at >= 1, at + 1
        return at >= 1, at + 1 < size, at - 1

    def to(side, dy, dz):
        sx, rx, px = (True, True, mx) if side is None else (side.send, side.recv, side.peer)
        sy, ry, py = along(my, gy, dy)
        sz, rz, pz = along(mz, gz, dz)
        return both(sx, sy, sz), both(rx, ry, rz), (px, py, pz)

    faces = [to(s, 0, 0) for s in near]
    faces += [to(None, d, 0) for d in (1, -1)] + [to(None, 0, d) for d in (1, -1)]

    def signal_faces(sem):
        for send, _, peer in faces:
            when(send, lambda peer=peer: pl.semaphore_signal(sem, inc=1, device_id=peer, device_id_type=MESH))

    heard = sum([(1 if recv is True else jnp.where(recv, 1, 0)) for _, recv, _ in faces])

    def clear(*refs):
        for ref in refs:
            ref[...] = jnp.zeros_like(ref)

    rows0 = a0.shape[3]
    own = slice(TOP, TOP + ly)
    outside = [i for i in range(a0.shape[1]) if i < c or i >= c + n0]
    clear(zrecv, erecv, yedge_in)
    for q in range(3):
        for i in range(c, c + n0):
            a0[q, i, 0, PAD:TOP] = jnp.zeros((PAD, LANES), jnp.float32)
            a0[q, i, 0, TOP + ly:TOP + ly + PAD] = jnp.zeros((PAD, LANES), jnp.float32)
        if gx != 2:
            for i in outside:
                a0[q, i, 0, own] = jnp.zeros((ly, LANES), jnp.float32)
    if gx != 2:
        clear(merged_in)
    barrier = pltpu.get_barrier_semaphore()
    signal_faces(barrier)
    clear(slots)

    def mask(shape, row0, lane_of, bounds):
        y = iota(shape, 0) + row0
        z = lane_of(iota(shape, 1))
        inside = (y >= 0) & (y < bounds[0]) & (z >= 0) & (z < bounds[1])
        return jnp.where(inside, SIXTH, 0.0)

    even = evens(ly, LANES)
    for copy in copies:
        copy.wait()
    for i in range(n0):
        a0[0, c + i, 0, own] = jnp.where(even, start[2 * i + 1], start[2 * i])
        a0[1, c + i, 0, own] = jnp.where(even, rhs[2 * i], rhs[2 * i + 1])
        a0[2, c + i, 0, own] = jnp.where(even, rhs[2 * i + 1], rhs[2 * i])
    for s, side in enumerate(near):
        third = a0[0, side.outward(c, n0, 3), 0, own]
        second = a0[2, side.outward(c, n0, 2), 0, own]
        merged_out[s] = jnp.where(evens(ly, LANES, side.send_shift()), third, pltpu.roll(second, 1, axis=0))

    pl.semaphore_wait(barrier, heard)

    lane64 = iota((ly, LANES), 1)
    lane8 = iota((8, LANES), 1)
    ydirs = zdirs = (1, -1)
    mail = Mail(sems.at[0])
    for s, side in enumerate(near):
        where = to(side, 0, 0)
        src, dst = side.source(c, n0, 2), side.target(c, n0, 2)
        mail.add(a0.at[0:2, pl.ds(src, 2), 0, own], a0.at[0:2, pl.ds(dst, 2), 0, own], *where, "x")

    def strip(d, rows):
        return (TOP + rows - 8, TOP - 8) if d > 0 else (TOP, TOP + rows)

    for d in ydirs:
        src, dst = strip(d, ly)
        mail.add(
            a0.at[0:3, pl.ds(c, n0), 0, pl.ds(src, 8)],
            a0.at[0:3, pl.ds(c, n0), 0, pl.ds(dst, 8)],
            *to(None, d, 0), "z",
        )
    signal_faces(relay.at[0])
    clear(ysides, xysides, tiles_in, zin, n_in, ny_in, nxy_in, nz_in, g_in)

    slots0 = [(q, i) for i in range(n0) for q in range(3)]
    for zi, d in enumerate(zdirs):
        packed = jnp.zeros((ly, LANES), jnp.float32)
        for t, (q, i) in enumerate(slots0):
            v = a0[q, c + i, 0, own]
            first = lz - FACE if d > 0 else 0
            here = (lane64 >= FACE * t) & (lane64 < FACE * (t + 1))
            packed = jnp.where(here, turn(v, FACE * t - first), packed)
        zsend[zi] = packed
    for zi, d in enumerate(zdirs):
        mail.add(zsend.at[zi], zrecv.at[zi, pl.ds(8, ly)], *to(None, 0, d), "z")

    width = sum(w for _, _, w in EDGE)
    starts = [sum(w for _, _, w in EDGE[:t]) for t in range(len(EDGE))]
    for s, side in enumerate(near):
        for zi, d in enumerate(zdirs):
            packed = jnp.zeros((8, LANES), jnp.float32)
            for (q, k, w), at in zip(EDGE, starts):
                v = a0[q, side.outward(c, n0, k), 0, own]
                for g in range(groups0):
                    lo = width * g + at
                    first = lz - w if d > 0 else 0
                    here = (lane8 >= lo) & (lane8 < lo + w)
                    packed = jnp.where(here, turn(v[8 * g:8 * g + 8], lo - first), packed)
            esend[s, zi] = packed
        for yi, d in enumerate(ydirs):
            for (q, k, w), at in zip(EDGE, starts):
                first = TOP + ly - w if d > 0 else TOP
                yedge_out[s, yi, at:at + w] = a0[q, side.outward(c, n0, k), 0, first:first + w]
    pl.semaphore_wait(relay.at[0], heard)
    signal_faces(relay.at[1])
    for s, side in enumerate(near):
        for yi, d in enumerate(ydirs):
            filled = pl.ds(0, width)
            mail.add(yedge_out.at[s, yi, filled], yedge_in.at[s, yi, filled], *to(side, d, 0), "y")
    for zi, dz in enumerate(zdirs):
        for d in ydirs:
            src, dst = strip(d, ly)
            mail.add(
                zsend.at[zi, pl.ds(src - TOP, 8)], zrecv.at[zi, pl.ds(dst - 8, 8)], *to(None, d, dz), "z"
            )
        for s, side in enumerate(near):
            mail.add(esend.at[s, zi], erecv.at[s, zi, 1], *to(side, 0, dz), "e")
    rounds = relay.shape[0]
    pl.semaphore_wait(relay.at[1], heard)
    for zi, dz in enumerate(zdirs):
        for s, side in enumerate(near):
            for d in ydirs:
                half = pl.ds(4 if d > 0 else 0, 4)
                mail.add(esend.at[s, zi, half], erecv.at[s, zi, 0 if d > 0 else 2, half], *to(side, d, dz), "e")
    for s, side in enumerate(near):
        where = to(side, 0, 0)
        src, dst = side.source(c, n0, 1), side.target(c, n0, 1)
        mail.add(a0.at[2, pl.ds(src, 1), 0, own], a0.at[2, pl.ds(dst, 1), 0, own], *where)
        mail.add(merged_out.at[s], merged_in.at[s], *where)
    for r in range(2, rounds):
        signal_faces(relay.at[r])
        pl.semaphore_wait(relay.at[r], heard)
    clear(r0, f0)
    for q in range(3):
        for i in range(a0.shape[1]):
            a0[q, i, 1] = jnp.zeros((rows0, LANES), jnp.float32)
            edge = PAD if c <= i < c + n0 else TOP
            a0[q, i, 0, 0:edge] = jnp.zeros((edge, LANES), jnp.float32)
            a0[q, i, 0, rows0 - edge:] = jnp.zeros((edge, LANES), jnp.float32)
    if gx == 2:
        for k in range(1, HALO + 1):
            a0[0, jnp.where(mx == 0, c - k, c + n0 + k - 1), 0, own] = jnp.zeros((ly, LANES), jnp.float32)
    fine = (gy * ly, gz * lz)
    s0[0] = mask(s0.shape[1:], my * ly - PAD, lambda k: mz * lz + k, fine)
    s0[1] = mask(s0.shape[1:], my * ly - PAD, lambda k: mz * lz + jnp.where(k < 64, k + lz, k - LANES), fine)
    s1[0] = mask(s1.shape[1:], my * hy - PAD, lambda k: mz * hz + k - left, (gy * hy, gz * hz))

    mail.wait("z")
    rows_h = ly + 16
    lane_h = iota((rows_h, LANES), 1)
    for t, (q, i) in enumerate(slots0):
        low = turn(zrecv[0], LANES - FACE - FACE * t)
        high = turn(zrecv[1], -FACE * t)
        a0[q, c + i, 1, PAD:PAD + rows_h] = jnp.where(
            lane_h >= LANES - FACE, low, jnp.where(lane_h < FACE, high, 0.0)
        )
    def span(n, k):
        if gx == 1:
            return c, n
        k = min(k, n * (gx - 1), HALO)
        if gx == 2:
            return jnp.where(mx == 0, c, c - k), n + k
        return c - k, n + 2 * k

    def inside(n, i):
        if gx <= 2:
            return None
        at = mx * n + i - c
        return jnp.where((at >= 0) & (at < gx * n), 1.0, 0.0)

    def neighbours(src, i, planes, red, chess, lo, hi, tiles):
        prev, cur, nxt = planes
        low = [turn(t, 1) for t in cur]
        high = [turn(t, -1) for t in cur]
        if len(cur) == 2:
            lane = iota(cur[0].shape, 1)
            low = [jnp.where(lane == 0, low[1 - g], low[g]) for g in range(tiles)]
            high = [jnp.where(lane == LANES - 1, high[1 - g], high[g]) for g in range(tiles)]
        out = []
        for g in range(tiles):
            beside = jnp.where(chess, prev[g], nxt[g]) if red else jnp.where(chess, nxt[g], prev[g])
            total = (cur[g] + beside) + (src[i, g, lo - 1:hi - 1] + src[i, g, lo + 1:hi + 1])
            out.append(total + (low[g] + high[g]))
        return out

    def relax(dst, src, rhs_of, scale, n, k, red, factor, tiles=None, emit=None, part=None):
        first, length = part or span(n, k)
        held = src.shape[1]
        rows = src.shape[2]
        lo, hi = (TOP, rows - TOP) if emit else (PAD, rows - PAD)
        tiles = tiles or held
        chess = evens(hi - lo, LANES)
        planes = [[src[first + j - 1, g, lo:hi] for g in range(held)] for j in range(length + 2)]
        for j in range(length):
            i = first + j
            totals = neighbours(src, i, planes[j:j + 3], red, chess, lo, hi, tiles)
            factor_x = inside(n, i)
            for g in range(tiles):
                b = rhs_of(i, g, lo, hi)
                if factor != 1.0:
                    b = b * factor
                value = (b + totals[g]) * scale[g, lo - PAD:hi - PAD]
                if factor_x is not None:
                    value = value * factor_x
                if emit:
                    emit(j, planes[j + 1][g], value)
                else:
                    dst[i, g, lo:hi] = value

    def residual(red_ref, black_ref, red_rhs, black_rhs, n, j, factor):
        rows = red_ref.shape[2]
        lo, hi = TOP, rows - TOP
        chess = evens(hi - lo, LANES)
        i = c + j
        held = red_ref.shape[1]

        def load(ref):
            return [[ref[i + d, g, lo:hi] for g in range(held if d == 0 else 1)] for d in (-1, 0, 1)]

        red, black = load(red_ref), load(black_ref)
        from_black = neighbours(black_ref, i, black, True, chess, lo, hi, 1)[0]
        from_red = neighbours(red_ref, i, red, False, chess, lo, hi, 1)[0]
        out = red_rhs(i, 0, lo, hi) - (6.0 * red[1][0] - from_black) * (1.0 / factor)
        return out + (black_rhs(i, 0, lo, hi) - (6.0 * black[1][0] - from_red) * (1.0 / factor))

    black0 = a0.at[0]
    rhs0 = [lambda i, g, lo, hi, q=q: a0[q, i, g, lo:hi] for q in (1, 2)]
    def sweep0(step, part):
        if step % 2 == 0:
            relax(r0, black0, rhs0[0], s0, n0, 0, True, 1.0, part=part)
        else:
            relax(black0, r0, rhs0[1], s0, n0, 0, False, 1.0, part=part)

    def early(step):
        return n0 - 1 - step if gx == 2 and n0 >= 4 else 0

    for step in range(4):
        if early(step) > 0:
            sweep0(step, (jnp.where(mx == 0, c, c + n0 - early(step)), early(step)))
    mail.wait("e")
    for s, side in enumerate(near):
        for (q, k, w), at in zip(EDGE, starts):
            pair = side.landing(c, n0, k)
            for g in range(groups0 + 2):
                which, group = (0, groups0 - 1) if g == 0 else ((2, 0) if g > groups0 else (1, g - 1))
                lo = width * group + at
                low = turn(erecv[s, 0, which], LANES - w - lo)
                high = turn(erecv[s, 1, which], -lo)
                a0[q, pair, 1, PAD + 8 * g:PAD + 8 * g + 8] = jnp.where(
                    lane8 >= LANES - w, low, jnp.where(lane8 < w, high, 0.0)
                )

    mail.wait("y")
    for s, side in enumerate(near):
        for yi, d in enumerate(ydirs):
            for (q, k, w), at in zip(EDGE, starts):
                first = TOP - w if d > 0 else TOP + ly
                a0[q, side.landing(c, n0, k), 0, first:first + w] = yedge_in[s, yi, at:at + w]
    late = 2 if gx == 2 and n0 >= 4 else 0
    if late:
        mail.wait("x")
        for step in range(4):
            sweep0(step, (jnp.where(mx == 0, c + early(step), c + n0 - late - early(step)), late))
    mail.wait()
    for s, side in enumerate(near):
        v = merged_in[s]
        a0[0, side.landing(c, n0, 3), 0, own] = v
        a0[2, side.landing(c, n0, 2), 0, own] = pltpu.roll(v, ly - 1, axis=0)
    for step in range(4):
        first, length = span(n0, (4 - step + 1) // 2)
        done = early(step) + late
        if done:
            first = first + jnp.where(mx == 0, done, 0)
        sweep0(step, (first, length - done))
    for j in range(n0):
        w0[j * ly:(j + 1) * ly, :] = residual(r0, black0, rhs0[0], rhs0[1], n0, j, 1.0)
    r = w0[pl.ds(0, n0 * hy, stride=2), :] + w0[pl.ds(1, n0 * hy, stride=2), :]
    source, target = iota((LANES, LANES), 0), iota((LANES, LANES), 1)
    fold = jnp.where(lax.rem(target - left + LANES, hz) == source // 2, 0.125, 0.0)
    r = dot(r, fold)

    own1 = slice(TOP, TOP + hy)
    lane32 = iota((hy, LANES), 1)
    mid = (lane32 >= left) & (lane32 < left + hz)
    chess1 = evens(hy, LANES)
    for j in range(n1):
        one, two = r[2 * j * hy:(2 * j + 1) * hy], r[(2 * j + 1) * hy:(2 * j + 2) * hy]
        red = jnp.where(chess1, one, two)
        black = jnp.where(chess1, two, one)
        tiles_out[j] = jnp.where(mid, red, black)
        a1[0, c + j, 0, own1] = jnp.where(mid, red, 0.0)
        a1[1, c + j, 0, own1] = jnp.where(mid, black, 0.0)

    def pack_edges(read, items, w):
        for d in zdirs:
            first = left + hz - w if d > 0 else left
            packed = jnp.zeros((8, LANES), jnp.float32)
            for t in range(items * groups1):
                here = (lane8 >= w * t) & (lane8 < w * (t + 1))
                packed = jnp.where(here, turn(read(t), w * t - first), packed)
            yield packed

    def post1(mail, out, into, y_in, xy_in, z_out, z_in, corner):
        far_first = list(enumerate([None] + sides1))[::-1]
        for steps in ((1, -1), (0,)):
            for s, side in far_first:
                for zi, dz in enumerate(zdirs):
                    for d in steps:
                        few = corner if d and side is not None else 8
                        rows = pl.ds(8 - few if d > 0 else 0, few)
                        mail.add(z_out.at[zi, rows], z_in.at[zi, s, 1 - d, rows], *to(side, d, dz))
        for s, side in enumerate(sides1):
            for yi, d in enumerate(ydirs):
                src = hy - 8 if d > 0 else 0
                mail.add(out.at[:, pl.ds(src, 8)], xy_in.at[s, yi], *to(side, d, 0))
        for s, side in enumerate(sides1):
            mail.add(out, into.at[s], *to(side, 0, 0))
        for yi, d in enumerate(ydirs):
            src = hy - 8 if d > 0 else 0
            mail.add(out.at[:, pl.ds(src, 8)], y_in.at[yi], *to(None, d, 0))

    def regions1():
        yield from ((None, None, j, c + j) for j in range(n1))
        for s, side in enumerate(sides1):
            for j in range(n1):
                at = side.base(c, n1) + j
                if side.dynamic or 0 <= at < 2 * c + n1:
                    yield (s, side, j, at)

    def row_groups():
        yield 0, groups1 - 1, None, 0
        for g in range(groups1):
            yield 1, g, g, None
        yield 2, 0, None, 1

    lane_l = lane8
    mid8 = (lane_l >= left) & (lane_l < left + hz)

    def edges(z_in, s, which, lo, w):
        at = 0 if s is None else s + 1
        low = turn(z_in[0, at, which], left - w - lo)
        high = turn(z_in[1, at, which], left + hz - lo)
        return jnp.where(lane_l < left, low, high)

    items = 2 * n1
    order1 = [(g, q, j) for g in range(groups1) for j in range(n1) for q in range(2)]
    tile_of = lambda t: a1[order1[t][1], c + order1[t][2], 0, TOP + 8 * order1[t][0]:TOP + 8 * order1[t][0] + 8]
    for zi, packed in enumerate(pack_edges(tile_of, items, RHS1)):
        zout[zi] = packed
    mail = Mail(sems.at[1])
    post1(mail, tiles_out, tiles_in, ysides, xysides, zout, zin, 4)
    for ref in (a1, r1, b1, f1):
        for i in range(ref.shape[-4]):
            halo_pair = i < c or i >= c + n1
            lead = (slice(None),) if len(ref.shape) == 5 else ()
            if halo_pair or ref is not a1:
                at = lead + (i,)
                ref[at] = jnp.zeros(ref[at].shape, jnp.float32)
            else:
                for rows in (slice(0, TOP), slice(TOP + hy, None)):
                    at = lead + (i, slice(None), rows)
                    ref[at] = jnp.zeros(ref[at].shape, jnp.float32)
    for ref in (b2r, b2b, r2, v2, b3r, b3b, r3, v3):
        ref[...] = jnp.zeros_like(ref)
    mail.wait()

    near_lanes = (lane_l >= left - RHS1) & (lane_l < left + hz + RHS1)
    for s, side, j, at in regions1():
        for n, (which, group, rows, yi) in enumerate(row_groups()):
            if rows is None:
                base = ysides[yi, j] if s is None else xysides[s, yi, j]
            elif s is None:
                base = None
            else:
                base = tiles_in[s, j, 8 * rows:8 * rows + 8]
            for q in range(2):
                to_rows = slice(PAD + 8 * n, PAD + 8 * n + 8)
                lo = RHS1 * ((group * n1 + j) * 2 + q)
                if base is None:
                    middle = a1[q, at, 0, to_rows]
                else:
                    middle = base if q == 0 else turn(base, LANES - hz)
                outer = edges(zin, s, which, lo, RHS1)
                a1[q, at, 0, to_rows] = jnp.where(mid8, middle, jnp.where(near_lanes, outer, 0.0))

    rhs1 = [lambda i, g, lo, hi, q=q: a1[q, i, g, lo:hi] for q in (0, 1)]
    first, length = span(n1, 2)
    for j in range(length):
        i = first + j
        value = (a1[0, i, 0, PAD:-PAD] * 4.0) * s1[0]
        factor_x = inside(n1, i)
        r1[i, 0, PAD:-PAD] = value if factor_x is None else value * factor_x
    relax(b1, r1, rhs1[1], s1, n1, 2, False, 4.0)
    relax(r1, b1, rhs1[0], s1, n1, 1, True, 4.0)
    relax(b1, r1, rhs1[1], s1, n1, 1, False, 4.0)

    for j in range(n1):
        w1[j, 0:hy, :] = residual(r1, b1, rhs1[0], rhs1[1], n1, j, 4.0)
    r = jnp.concatenate(
        [w1[j, pl.ds(0, qy, stride=2), :] + w1[j, pl.ds(1, qy, stride=2), :] for j in range(n1)], axis=0
    )
    fold = jnp.where(
        (lax.rem(target, qz) == (source - left) // 2) & (source >= left) & (source < left + hz), 0.125, 0.0
    )
    r = dot(r, fold)
    block = lane8 // qz
    per_colour = qy // 8
    one = two = None
    for h in range(per_colour):
        p, q = r[8 * h:8 * h + 8], r[qy + 8 * h:qy + 8 * h + 8]
        here = lax.rem(block, per_colour) == h
        one = p if one is None else jnp.where(here, p, one)
        two = q if two is None else jnp.where(here, q, two)
    tile = jnp.where(evens(8, LANES) ^ (block >= per_colour), one, two)
    pack[...] = tile

    mine = (mx * gy + my) * gz + mz
    slots[mine] = tile

    dist = (-(-REACH2 // (lx // 4)), -(-REACH2 // qy), -(-REACH2 // qz))

    def coords(k):
        steps = (k // (gy * gz), k // gz % gy, k % gz)
        moved = [at + step for at, step in zip((mx, my, mz), steps)]
        at = tuple(jnp.where(v >= size, v - size, v) for v, size in zip(moved, sizes))
        close = True
        for a, b, size, reach in zip(at, (mx, my, mz), sizes, dist):
            if reach < size - 1:
                close = both(close, (a - b <= reach) & (b - a <= reach))
        return at, close

    def number(at):
        return (at[0] * gy + at[1]) * gz + at[2]

    def flipped(at, k):
        bit = 1
        while bit <= k:
            if k & bit:
                at = at + bit - 2 * bit * lax.rem(lax.div(at, bit), 2)
            bit *= 2
        return at

    def partners():
        own_at = (mx, my, mz)
        flips = [[flipped(at, k) for k in range(size)] for at, size in zip(own_at, sizes)]
        order = [(i, j, k) for i in range(gx) for j in range(gy) for k in range(gz)][1:]
        order.sort(key=lambda f: (-f[0], -min(f[2], 2), -f[1]))
        for f in order:
            at = tuple(flips[axis][k] for axis, k in enumerate(f))
            close = True
            for a, b, k, reach in zip(at, own_at, f, dist):
                if k > reach:
                    close = both(close, (a - b <= reach) & (b - a <= reach))
            yield at, close

    straight = count <= 64 and all(size & (size - 1) == 0 for size in sizes)

    def others(body):
        if straight:
            for place in partners():
                body(place)
        else:
            def step(k, carry):
                body(coords(k))
                return carry

            lax.fori_loop(1, count, step, 0)

    def gather(place, arriving):
        at, close = place
        d = number(at)
        return pltpu.make_async_remote_copy(
            src_ref=pack,
            dst_ref=slots.at[d if arriving else mine],
            send_sem=gather_sems.at[0, d],
            recv_sem=gather_sems.at[1, d if arriving else mine],
            device_id=at,
            device_id_type=MESH,
        ), close

    def gather_start(place):
        copy, close = gather(place, False)
        when(close, copy.start)

    def gather_wait(place):
        copy, close = gather(place, True)

        def done():
            copy.wait_send()
            copy.wait_recv()

        when(close, done)

    others(gather_start)

    red_out = jnp.where(mid, b1[c, 0, own1], turn(b1[c + n1 - 1, 0, own1], LANES - hz))
    n_out[0] = red_out
    order_n = [(g, j) for g in range(groups1) for j in range(n1)]
    tile_n = lambda t: b1[c + order_n[t][1], 0, TOP + 8 * order_n[t][0]:TOP + 8 * order_n[t][0] + 8]
    for zi, packed in enumerate(pack_edges(tile_n, n1, COR1)):
        nz_out[zi] = packed
    mail1 = Mail(sems.at[2])
    post1(mail1, n_out, n_in, ny_in, nxy_in, nz_out, nz_in, 8)

    for zi, d in enumerate(zdirs):
        packed = jnp.zeros((8, LANES), jnp.float32)
        for i in range(n0):
            v = a0[0, c + i, 0, own]
            for g in range(groups0):
                lo = COR0 * (g * n0 + i)
                first = lz - COR0 if d > 0 else 0
                here = (lane8 >= lo) & (lane8 < lo + COR0)
                packed = jnp.where(here, turn(v[8 * g:8 * g + 8], lo - first), packed)
        g_out[zi] = packed
    mail0 = Mail(sems.at[3])
    for d in ydirs:
        ysrc, ydst = strip(d, ly)
        mail0.add(
            black0.at[pl.ds(c, n0), 0, pl.ds(ysrc, 8)], f0.at[pl.ds(c, n0), 0, pl.ds(ydst, 8)], *to(None, d, 0)
        )
    for zi, dz in enumerate(zdirs):
        for s, side in enumerate([None] + near):
            for yi, d in enumerate((1, 0, -1)):
                mail0.add(g_out.at[zi], g_in.at[zi, s, yi], *to(side, d, dz))
    for side in near:
        src, dst = side.source(c, n0, 2), side.target(c, n0, 2)
        mail0.add(black0.at[pl.ds(src, 2), 0, own], f0.at[pl.ds(dst, 2), 0, own], *to(side, 0, 0))
        for d in ydirs:
            ysrc, ydst = strip(d, ly)
            mail0.add(
                black0.at[pl.ds(src, 2), 0, pl.ds(ysrc, 8)], f0.at[pl.ds(dst, 2), 0, pl.ds(ydst, 8)], *to(side, d, 0)
            )

    others(gather_wait)

    per = LANES // qz
    for k in range(gx * gy):
        cx, cy = k // gy, k % gy
        for g in range(gz // per):
            parts = [slots[k * gz + g * per + q] for q in range(per)]
            for h in range(per_colour):
                for colour, ref in ((0, b2r), (1, b2b)):
                    at = colour * per_colour + h
                    v = None
                    for q in range(per):
                        moved = turn(parts[q], (q - at) * qz)
                        here = (lane8 >= q * qz) & (lane8 < (q + 1) * qz)
                        v = moved if v is None else jnp.where(here, moved, v)
                    ref[1 + cx, PAD + cy * qy + 8 * h:PAD + cy * qy + 8 * h + 8, LANES * g:LANES * (g + 1)] = v

    def coarse_total(src, i, red, rows, full):
        width_z = src.shape[2]
        lo, hi = PAD, PAD + rows
        v = src[i, lo:hi]
        low, high = turn(v, 1), turn(v, -1)
        lane = iota(v.shape, 1)
        if full:
            low = jnp.where(lane == 0, 0.0, low)
            high = jnp.where(lane == width_z - 1, 0.0, high)
        chess = evens(rows, width_z)
        prev, nxt = src[i - 1, lo:hi], src[i + 1, lo:hi]
        beside = jnp.where(chess, prev, nxt) if red else jnp.where(chess, nxt, prev)
        total = (v + beside) + (src[i, lo - 1:hi - 1] + src[i, lo + 1:hi + 1])
        return v, total + (low + high)

    def coarse(dst, src, b, pairs, red, factor, rows, scale, full):
        for i in range(1, pairs + 1):
            _, total = coarse_total(src, i, red, rows, full)
            dst[i, PAD:PAD + rows] = (b[i, PAD:PAD + rows] * factor + total) * scale

    def sweep(red, black, red_rhs, black_rhs, pairs, factor, rows, scale, full):
        width_z = black.shape[2]
        lo, hi = PAD, PAD + rows
        lane = iota((rows, width_z), 1)
        chess = evens(rows, width_z)

        def moved(v, k):
            out = turn(v, k)
            if full:
                out = jnp.where(lane < k, 0.0, out) if k > 0 else jnp.where(lane >= width_z + k, 0.0, out)
            return out

        here, before, after = scale
        beside_z = []
        for i in range(1, pairs + 1):
            v = black[i, lo:hi]
            beside = jnp.where(chess, black[i - 1, lo:hi], black[i + 1, lo:hi])
            rest = (red_rhs[i, lo:hi] * factor + (v + beside)) + (black[i, lo - 1:hi - 1] + black[i, lo + 1:hi + 1])
            red[i, lo:hi] = (rest + (moved(v, 1) + moved(v, -1))) * here
            low = (turn(rest, 1) + (moved(v, 2) + v)) * before
            high = (turn(rest, -1) + (v + moved(v, -2))) * after
            beside_z.append(low + high)
        for i in range(1, pairs + 1):
            v = red[i, lo:hi]
            beside = jnp.where(chess, red[i + 1, lo:hi], red[i - 1, lo:hi])
            total = (v + beside) + (red[i, lo - 1:hi - 1] + red[i, lo + 1:hi + 1])
            black[i, lo:hi] = (black_rhs[i, lo:hi] * factor + (total + beside_z[i - 1])) * here

    def scales(rows, width_z, cells):
        lane = iota((rows, width_z), 1)
        return tuple(
            jnp.where((lane - k >= 0) & (lane - k < cells), SIXTH, 0.0) if k or cells < width_z else SIXTH
            for k in (0, 1, -1)
        )

    in2 = slice(PAD, PAD + y2)
    scale2 = scales(y2, z2, z2)
    for i in range(1, p2 + 1):
        r2[i, in2] = (b2r[i, in2] * 16.0) * SIXTH
    coarse(v2, r2, b2b, p2, False, 16.0, y2, SIXTH, True)
    sweep(r2, v2, b2r, b2b, p2, 16.0, y2, scale2, True)

    fold = jnp.where(iota((z2, z3p), 1) == iota((z2, z3p), 0) // 2, 0.125, 0.0)
    parts = []
    for i in range(1, p2 + 1):
        red, from_black = r2[i, in2], coarse_total(v2, i, True, y2, True)[1]
        black, from_red = v2[i, in2], coarse_total(r2, i, False, y2, True)[1]
        r = b2r[i, in2] - (6.0 * red - from_black) * 0.0625
        r = r + (b2b[i, in2] - (6.0 * black - from_red) * 0.0625)
        for g in range(z2 // LANES):
            w2[i - 1, g, 0:y2] = r[:, LANES * g:LANES * (g + 1)]
        parts.append(
            jnp.concatenate(
                [
                    w2[i - 1, g, pl.ds(0, y3, stride=2), :] + w2[i - 1, g, pl.ds(1, y3, stride=2), :]
                    for g in range(z2 // LANES)
                ],
                axis=1,
            )
        )
    r = dot(jnp.concatenate(parts, axis=0), fold)
    chess3 = evens(y3, z3p)
    in3 = slice(PAD, PAD + y3)
    for j in range(p3):
        one, two = r[2 * j * y3:(2 * j + 1) * y3], r[(2 * j + 1) * y3:(2 * j + 2) * y3]
        b3r[1 + j, in3] = jnp.where(chess3, one, two)
        b3b[1 + j, in3] = jnp.where(chess3, two, one)

    full3 = z3 == z3p
    scale3 = scales(y3, z3p, z3)

    def sweep3(_, carry):
        sweep(r3, v3, b3r, b3b, p3, 64.0, y3, scale3, full3)
        return carry

    if p3 == 1:
        for _ in range(CSWEEPS):
            sweep3(0, 0)
    else:
        lax.fori_loop(0, CSWEEPS, sweep3, 0)

    def plane(red, black, chess, odd):
        return jnp.where(chess, black, red) if odd else jnp.where(chess, red, black)

    grow = jnp.where(iota((z3p, z2), 0) == iota((z3p, z2), 1) // 2, 1.0, 0.0)
    v = jnp.concatenate(
        [plane(r3[1 + i // 2, in3], v3[1 + i // 2, in3], chess3, i % 2) for i in range(p2)], axis=0
    )
    v = dot(v, grow)
    for i in range(p2):
        part = v[i * y3:(i + 1) * y3]
        for g in range(z2 // LANES):
            w2[i, g, pl.ds(0, y3, stride=2), :] = part[:, LANES * g:LANES * (g + 1)]
            w2[i, g, pl.ds(1, y3, stride=2), :] = part[:, LANES * g:LANES * (g + 1)]
    for i in range(p2):
        for g in range(z2 // LANES):
            lanes = slice(LANES * g, LANES * (g + 1))
            v2[1 + i, in2, lanes] = v2[1 + i, in2, lanes] + w2[i, g, 0:y2]
    for _ in range(2):
        sweep(r2, v2, b2r, b2b, p2, 16.0, y2, scale2, True)

    mail1.wait()
    grow1 = jnp.where(
        iota((z2, LANES), 0) == mz * qz + (iota((z2, LANES), 1) - left + 2 * LANES) // 2 - LANES, 1.0, 0.0
    )
    rows1 = f1.shape[2]
    half1 = rows1 // 2
    rows2 = pl.ds(pl.multiple_of(my * qy, 8), half1)
    chess2 = evens(half1, z2)
    first, length = span(n1, HALO)
    begin = first - c + mx * n1
    shift = 0 if gx <= 2 else 1
    first_even = begin - shift
    tops = []
    for j in range(length):
        at = j + shift
        index = (first_even + (at - at % 2)) // 2 + 1
        if gx > 2:
            index = jnp.clip(index, 0, p2 + 1)
        tops.append(plane(r2[index, rows2], v2[index, rows2], chess2, at % 2))
    v = dot(jnp.concatenate(tops, axis=0), grow1)
    for j in range(length):
        part = v[j * half1:(j + 1) * half1]
        w1[j, pl.ds(0, half1, stride=2), :] = part
        w1[j, pl.ds(1, half1, stride=2), :] = part

    near_lanes = (lane_l >= left - COR1) & (lane_l < left + hz + COR1)
    for s, side, j, at in regions1():
        for n, (which, group, rows, yi) in enumerate(row_groups()):
            to_rows = slice(PAD + 8 * n, PAD + 8 * n + 8)
            if rows is None:
                base = ny_in[yi, 0] if s is None else nxy_in[s, yi, 0]
            elif s is None:
                base = None
            else:
                base = n_in[s, 0, 8 * rows:8 * rows + 8]
            if base is None:
                middle = b1[at, 0, to_rows]
            else:
                middle = base if j == 0 else turn(base, LANES - hz)
            outer = edges(nz_in, s, which, COR1 * (group * n1 + j), COR1)
            value = jnp.where(mid8, middle, jnp.where(near_lanes, outer, 0.0))
            f1[at, 0, to_rows] = value + w1[at - first, to_rows, :]

    for step in range(4):
        k = (5 - step + 1) // 2
        if step % 2 == 0:
            relax(r1, f1, rhs1[0], s1, n1, k, True, 4.0)
        else:
            relax(f1, r1, rhs1[1], s1, n1, k, False, 4.0)

    mail0.wait()
    grow0 = jnp.where(
        iota((LANES, 2 * LANES), 0) == (left + iota((LANES, 2 * LANES), 1) // 2) % LANES, 1.0, 0.0
    )
    half0 = rows0 // 2
    first, length = span(n0, 2)
    chess_h = evens(half0, LANES)
    tops = []
    for j in range(length):
        index = (first - c + j - j % 2) // 2 + c if gx <= 2 else (first - c + j) // 2 + c
        red, black = r1[index, 0, PAD:PAD + half0], f1[index, 0, PAD:PAD + half0]
        tops.append(plane(red, black, chess_h, j % 2))
    v = dot(jnp.concatenate(tops, axis=0), grow0)
    for j in range(length):
        for g in range(2):
            base = (2 * j + g) * rows0
            part = v[j * half0:(j + 1) * half0, LANES * g:LANES * (g + 1)]
            w0[pl.ds(base, half0, stride=2), :] = part
            w0[pl.ds(base + 1, half0, stride=2), :] = part

    for i in range(n0):
        at = c + i
        j = at - first
        lift = w0[pl.ds(pl.multiple_of(2 * j * rows0, 8) + TOP, ly), :]
        f0[at, 0, own] = black0[at, 0, own] + lift
        for rows in (slice(PAD, TOP), slice(TOP + ly, TOP + ly + 8)):
            lift = w0[pl.ds(pl.multiple_of(2 * j * rows0, 8) + rows.start, 8), :]
            f0[at, 0, rows] = f0[at, 0, rows] + lift
    for side in near:
        for k in (1, 2):
            at = side.landing(c, n0, k)
            j = at - first
            lift = w0[pl.ds(pl.multiple_of(2 * j * rows0, 8) + PAD, rows_h), :]
            f0[at, 0, PAD:PAD + rows_h] = f0[at, 0, PAD:PAD + rows_h] + lift
    for s, side in enumerate([None] + near):
        pairs = range(n0) if side is None else (1, 2)
        for k in pairs:
            if side is None:
                at, far = c + k, k
            else:
                at = side.landing(c, n0, k)
                far = None
            for n in range(groups0 + 2):
                which, group = (0, groups0 - 1) if n == 0 else ((2, 0) if n > groups0 else (1, n - 1))
                tiles = []
                for zi in range(2):
                    t = g_in[zi, s, which]
                    if far is not None:
                        lo = COR0 * (group * n0 + far)
                        tiles.append(turn(t, (LANES - COR0 if zi == 0 else 0) - lo))
                    elif side.dynamic:
                        spot = (LANES - COR0 if zi == 0 else 0)
                        a = turn(t, spot - COR0 * (group * n0 + k - 1))
                        b = turn(t, spot - COR0 * (group * n0 + n0 - k))
                        tiles.append(jnp.where(side.up, a, b))
                    else:
                        far_at = n0 - k if side.up else k - 1
                        tiles.append(turn(t, (LANES - COR0 if zi == 0 else 0) - COR0 * (group * n0 + far_at)))
                low, high = tiles
                value = jnp.where(lane8 >= LANES - COR0, low, jnp.where(lane8 < COR0, high, 0.0))
                j = at - first
                to_rows = slice(PAD + 8 * n, PAD + 8 * n + 8)
                lift = w0[pl.ds(pl.multiple_of((2 * j + 1) * rows0, 8) + PAD + 8 * n, 8), :]
                f0[at, 1, to_rows] = value + lift

    relax(r0, f0, rhs0[0], s0, n0, 2, True, 1.0)
    relax(f0, r0, rhs0[1], s0, n0, 1, False, 1.0)
    relax(r0, f0, rhs0[0], s0, n0, 1, True, 1.0)

    def emit(j, red, black):
        out_ref[2 * j] = jnp.where(even, red, black)
        out_ref[2 * j + 1] = jnp.where(even, black, red)

    relax(None, r0, rhs0[1], s0, n0, 0, False, 1.0, tiles=1, emit=emit)


def local(sizes, right_side, start):
    gx, gy, gz = sizes
    lx, ly, lz = start.shape
    f32 = jnp.float32
    count = gx * gy * gz
    near = {1: 0, 2: 1}.get(gx, 2)
    far = {1: 0, 2: 1}.get(gx, 4)
    n0, n1 = lx // 2, lx // 4
    m0, m1 = n0 + 2 * HALO, n1 + 2 * HALO
    r0, r1 = ly + 2 * TOP, ly // 2 + 2 * TOP
    hy = ly // 2
    y2, z2 = gy * ly // 4, gz * lz // 4
    p2, p3 = gx * lx // 8, gx * lx // 16
    y3, z3 = y2 // 2, z2 // 2
    z3p = -(-z3 // LANES) * LANES
    dx = min(gx - 1, -(-REACH2 // (lx // 4)))
    dy = min(gy - 1, -(-REACH2 // (ly // 4)))
    dz = min(gz - 1, -(-REACH2 // (lz // 4)))
    rounds = max(2, sum(max(0, d - 2) for d in (dx, dy, dz)) - 1)
    near_a, far_a = max(near, 1), max(far, 1)

    def vmem(*shape):
        return pltpu.VMEM(shape, f32)

    messages = 24 if gx <= 2 else 48
    return pl.pallas_call(
        functools.partial(kernel, sizes),
        out_shape=jax.ShapeDtypeStruct(start.shape, f32),
        in_specs=[pl.BlockSpec(memory_space=pl.ANY)] * 2,
        out_specs=pl.BlockSpec(memory_space=pltpu.VMEM),
        scratch_shapes=[
            vmem(lx, ly, lz),
            vmem(lx, ly, lz),
            vmem(3, m0, 2, r0, LANES),
            vmem(m0, 2, r0, LANES),
            vmem(m0, 2, r0, LANES),
            vmem(2, r0 - 2 * PAD, LANES),
            vmem(near_a, ly, LANES),
            vmem(near_a, ly, LANES),
            vmem(2, ly, LANES),
            vmem(2, ly + 16, LANES),
            vmem(near_a, 2, 8, LANES),
            vmem(near_a, 2, 3, 8, LANES),
            vmem(near_a, 2, 16, LANES),
            vmem(near_a, 2, 16, LANES),
            vmem(2, m1, 1, r1, LANES),
            vmem(m1, 1, r1, LANES),
            vmem(m1, 1, r1, LANES),
            vmem(m1, 1, r1, LANES),
            vmem(1, r1 - 2 * PAD, LANES),
            vmem(2 * m0 * r0, LANES),
            vmem(m1, r1, LANES),
            vmem(n1, hy, LANES),
            vmem(far_a, n1, hy, LANES),
            vmem(2, n1, 8, LANES),
            vmem(far_a, 2, n1, 8, LANES),
            vmem(2, 8, LANES),
            vmem(2, far + 1, 3, 8, LANES),
            vmem(1, hy, LANES),
            vmem(far_a, 1, hy, LANES),
            vmem(2, 1, 8, LANES),
            vmem(far_a, 2, 1, 8, LANES),
            vmem(2, 8, LANES),
            vmem(2, far + 1, 3, 8, LANES),
            vmem(2, 8, LANES),
            vmem(2, near + 1, 3, 8, LANES),
            vmem(p2 + 2, y2 + 2 * PAD, z2),
            vmem(p2 + 2, y2 + 2 * PAD, z2),
            vmem(p2 + 2, y2 + 2 * PAD, z2),
            vmem(p2 + 2, y2 + 2 * PAD, z2),
            vmem(8, LANES),
            vmem(count, 8, LANES),
            vmem(p2, z2 // LANES, y2, LANES),
            vmem(p3 + 2, y3 + 2 * PAD, z3p),
            vmem(p3 + 2, y3 + 2 * PAD, z3p),
            vmem(p3 + 2, y3 + 2 * PAD, z3p),
            vmem(p3 + 2, y3 + 2 * PAD, z3p),
            pltpu.SemaphoreType.DMA((2,)),
            pltpu.SemaphoreType.REGULAR((rounds,)),
            pltpu.SemaphoreType.DMA((4, 2, messages)),
            pltpu.SemaphoreType.DMA((2, count)),
        ],
        compiler_params=pltpu.CompilerParams(
            collective_id=0, has_side_effects=True, vmem_limit_bytes=GRANT
        ),
    )(right_side, start)


def solution(mesh):
    sizes = (mesh.shape["gx"], mesh.shape["gy"], mesh.shape["gz"])
    spec = P("gx", "gy", "gz")
    return jax.shard_map(
        functools.partial(local, sizes), mesh=mesh, in_specs=(spec, spec), out_specs=spec, check_vma=False
    )
```
